256 devices in a mesh: row: 32 (over y, x, core), gz: 8 (over z).
Axes of the slice: x: 4, y: 4, z: 8, core: 2. Of those that a mesh axis runs over, the one named last changes fastest.
Arguments:
- velocity_x: bfloat16 [2, 32, 1024, 1024], P(None, None, 'row', 'gz'), may hold values from -6 to 6
- velocity_y: bfloat16 [2, 32, 1024, 1024], P(None, None, 'row', 'gz'), may hold values from -6 to 6
- velocity_z: bfloat16 [2, 32, 1024, 1024], P(None, None, 'row', 'gz'), may hold values from -6 to 6
- spacing: float32 [64], replicated, may hold values from 0.5 to 2
- level_index: int32 [1024], replicated, may hold values from 0 to 63
- plane_index: int32 [32], replicated, may hold values from 4 to 128
Outputs:
- pressure: float32 [2, 32, 1024, 1024], P(None, None, 'row', 'gz')
The draws below stay inside these ranges and needn't reach their ends.
All inputs are finite; a program needn't handle non-finite values.
Results may differ from the reference program's by a relative error of at most 0.002.
The reference program's roundings to bfloat16 on the way count: a program that leaves them out, or rounds other values in their place, can miss the bound.
Values may be sent and summed in bfloat16 or wider, within the bound.
A program may use at most 64 MiB of HBM per device.

```python
import math
import jax
import jax.numpy as jnp
from jax import lax

NX = 1024
NZ = 1024
NLEV = 64
P_SIZE = 32


def plant(values, rng, low, largest):
    dims = values.shape
    spot = [jax.random.randint(jax.random.fold_in(rng, axis), (), 0, dims[axis]) for axis in range(len(dims))]
    values = values.at[tuple(spot)].set(low)
    longest = dims.index(max(dims))
    spot[longest] = (spot[longest] + 1) % dims[longest]
    return values.at[tuple(spot)].set(largest)


def shard_levels(own_key, shape, cuts, low, high):
    factor_of, own = 1.0, jax.random.fold_in(own_key, 6)
    for position, shards_of in cuts:
        heights = jnp.exp(jax.random.uniform(jax.random.fold_in(own, position), (shards_of,), jnp.float32, low / len(cuts), high / len(cuts)))
        factor_of = factor_of * jnp.repeat(heights, shape[position] // shards_of).reshape([-1 if axis == position else 1 for axis in range(len(shape))])
    return factor_of


def centred(key, dims, deviation, limit, split=(), kind=jnp.bfloat16):
    level = shard_levels(key, dims, split, -0.22, 0.18) if split else 1.0
    array = jax.random.normal(key, dims, jnp.float32) * deviation * level
    return jnp.minimum(jnp.maximum(array, -limit), limit).astype(kind)


def setup_inputs(seed: int = 0) -> dict:
    key_of = jax.random.split(jax.random.key(seed), 7)
    velocity_x = centred(key_of[0], (2, P_SIZE, NX, NZ), 1.0, 6.0, ((2, 32), (3, 8)))
    velocity_y = centred(key_of[1], (2, P_SIZE, NX, NZ), 1.0, 6.0, ((2, 32), (3, 8)))
    velocity_z = centred(key_of[2], (2, P_SIZE, NX, NZ), 1.0, 6.0, ((2, 32), (3, 8)))
    spacing = jnp.clip(jnp.exp(jax.random.uniform(key_of[3], (NLEV,), jnp.float32, math.log(0.5), math.log(2.0))), 0.5, 2.0)
    level_index = plant(jax.random.randint(key_of[4], (NZ,), 0, NLEV), jax.random.fold_in(key_of[4], 1), 0, NLEV - 1).astype(jnp.int32)
    plane_index = plant(jax.random.randint(key_of[5], (P_SIZE,), 4, 129), jax.random.fold_in(key_of[5], 1), 4, 128).astype(jnp.int32)
    return {"velocity_x": velocity_x, "velocity_y": velocity_y, "velocity_z": velocity_z, "spacing": spacing, "level_index": level_index, "plane_index": plane_index}


full_turn = 2.0 * math.pi
wave_unit = 2.0 * math.pi / 2048.0


def band_coefficients(cell_width):
    length = cell_width.shape[0]
    index = jnp.arange(length, dtype=jnp.int32)
    previous = jnp.concatenate([cell_width[:1], cell_width[:-1]])
    following = jnp.concatenate([cell_width[1:], cell_width[-1:]])
    lower_band = jnp.where(index > 0, 1.0 / (0.5 * (previous + cell_width) * cell_width), 0.0)
    upper_band = jnp.where(index < length - 1, 1.0 / (0.5 * (cell_width + following) * cell_width), 0.0)
    return lower_band, upper_band


def thomas(lower_band, diagonal, upper_band, right_real, right_imag):
    rows = (lower_band, upper_band, diagonal.T, right_real.T, right_imag.T)

    def sweep(carry, row):
        ratio_prev, real_prev, imag_prev = carry
        low_coef, up_coef, diag_col, real_in, imag_in = row
        pivot = diag_col - low_coef * ratio_prev
        ratio = up_coef / pivot
        real_now = (real_in - low_coef * real_prev) / pivot
        imag_now = (imag_in - low_coef * imag_prev) / pivot
        return (ratio, real_now, imag_now), (ratio, real_now, imag_now)

    zeros = jnp.zeros((diagonal.shape[0],), diagonal.dtype)
    unused, (ratios, reals, imags) = lax.scan(sweep, (zeros, zeros, zeros), rows)

    def back(carry, row):
        next_real, next_imag = carry
        ratio, real_now, imag_now = row
        value_real = real_now - ratio * next_real
        value_imag = imag_now - ratio * next_imag
        return (value_real, value_imag), (value_real, value_imag)

    unused, (sol_real, sol_imag) = lax.scan(back, (zeros, zeros), (ratios, reals, imags), reverse=True)
    return sol_real.T, sol_imag.T


def reference(velocity_x, velocity_y, velocity_z, spacing, level_index, plane_index):
    cell_width = spacing[level_index]
    lower_band, upper_band = band_coefficients(cell_width)
    modes = jnp.arange(NX, dtype=jnp.int32)
    signed = jnp.where(modes >= NX // 2, modes - NX, modes)
    wave_x = signed.astype(jnp.float32) * (full_turn / NX)

    def one_plane(item):
        along, across, upward, index_y = item
        wave_y = index_y.astype(jnp.float32) * wave_unit
        up_real = upward[0].astype(jnp.float32)
        up_imag = upward[1].astype(jnp.float32)
        zero_col = jnp.zeros((NX, 1), jnp.float32)
        below_real = jnp.concatenate([zero_col, up_real[:, :-1]], axis=1)
        below_imag = jnp.concatenate([zero_col, up_imag[:, :-1]], axis=1)
        across_real = across[0].astype(jnp.float32)
        across_imag = across[1].astype(jnp.float32)
        source_real = (-wave_y * across_imag + (up_real - below_real) / cell_width).astype(jnp.bfloat16)
        source_imag = (wave_y * across_real + (up_imag - below_imag) / cell_width).astype(jnp.bfloat16)
        source_real, source_imag = lax.optimization_barrier((source_real, source_imag))
        source_hat = jnp.fft.fft(source_real.astype(jnp.float32) + 1j * source_imag.astype(jnp.float32), axis=0)
        along_hat = jnp.fft.fft(along[0].astype(jnp.float32) + 1j * along[1].astype(jnp.float32), axis=0)
        right_hat = source_hat + 1j * wave_x[:, None] * along_hat
        wave_sq = wave_x * wave_x + wave_y * wave_y
        diagonal = -(lower_band + upper_band)[None, :] - wave_sq[:, None]
        sol_real, sol_imag = thomas(lower_band, diagonal, upper_band, jnp.real(right_hat), jnp.imag(right_hat))
        field = jnp.fft.ifft(sol_real + 1j * sol_imag, axis=0)
        return jnp.stack([jnp.real(field), jnp.imag(field)]).astype(jnp.float32)

    stacked = lax.map(one_plane, (jnp.moveaxis(velocity_x, 1, 0), jnp.moveaxis(velocity_y, 1, 0), jnp.moveaxis(velocity_z, 1, 0), plane_index))
    return jnp.moveaxis(stacked, 0, 1)
```

```python
import math

import jax
import jax.numpy as jnp
import numpy as np
from jax import lax
from jax.experimental import pallas as pl
from jax.experimental.pallas import tpu as pltpu
from jax.sharding import PartitionSpec as P

MESH = pl.DeviceIdType.MESH
f32 = jnp.float32
bf16 = jnp.bfloat16
full_turn = 2.0 * math.pi
wave_unit = 2.0 * math.pi / 2048.0
ROW = 32
GZ = 8
DEPTH = 128
RADIX = 8
HALF = DEPTH // 2
ROOT_HALF = math.sqrt(0.5)


def tables():
    idx = np.arange(128)
    angle = 2.0 * np.pi / 128.0 * ((idx[:, None] * idx[None, :]) % 128)
    c, s = np.cos(angle), np.sin(angle)
    w = np.block([[c, -s], [s, c]]).astype(np.float32)
    hi = w.astype(jnp.bfloat16)
    lo = (w - hi.astype(np.float32)).astype(jnp.bfloat16)
    weights = np.concatenate([hi, hi, lo], axis=0)
    twist = 2.0 * np.pi / 1024.0 * (np.arange(8)[:, None] * idx[None, :])
    twiddle = np.concatenate([np.cos(twist), np.sin(twist)], axis=0).astype(np.float32)
    return weights, twiddle


def butterfly(xr, xi):
    def add(p, q):
        return (p[0] + q[0], p[1] + q[1])

    def sub(p, q):
        return (p[0] - q[0], p[1] - q[1])

    def turn(p):
        return (p[1], -p[0])

    x = list(zip(xr, xi))
    a0, a1 = add(x[0], x[4]), sub(x[0], x[4])
    a2, a3 = add(x[2], x[6]), turn(sub(x[2], x[6]))
    b0, b1 = add(x[1], x[5]), sub(x[1], x[5])
    b2, b3 = add(x[3], x[7]), turn(sub(x[3], x[7]))
    e = [add(a0, a2), add(a1, a3), sub(a0, a2), sub(a1, a3)]
    o = [add(b0, b2), add(b1, b3), sub(b0, b2), sub(b1, b3)]
    o1 = ((o[1][0] + o[1][1]) * ROOT_HALF, (o[1][1] - o[1][0]) * ROOT_HALF)
    o2 = turn(o[2])
    o3 = ((o[3][1] - o[3][0]) * ROOT_HALF, -(o[3][0] + o[3][1]) * ROOT_HALF)
    odd = [o[0], o1, o2, o3]
    return [add(e[k], odd[k]) for k in range(4)] + [sub(e[k], odd[k]) for k in range(4)]


def twisted(re, im, tw_ref, c):
    if c == 0:
        return re, im
    cos = tw_ref[c : c + 1, :]
    sin = tw_ref[8 + c : 9 + c, :]
    return re * cos + im * sin, im * cos - re * sin


def put_split(y_ref, c, rows, re, im):
    re_hi = re.astype(bf16)
    im_hi = im.astype(bf16)
    y_ref[c, rows, 0:128] = re_hi
    y_ref[c, rows, 128:256] = im_hi
    y_ref[c, rows, 256:384] = (re - re_hi.astype(f32)).astype(bf16)
    y_ref[c, rows, 384:512] = (im - im_hi.astype(f32)).astype(bf16)


def kernel(
    u_hbm, v_hbm, w_hbm, spacing_ref, level_ref, plane_ref, weights_ref, tw_ref,
    out_ref,
    u_v, v_v, w_v, s_v, recv_u, recv_s, out_v, halo_out, halo_in, halo_cols, band, bmat,
    inv_s, fe_s, bc_s, vs_s, ws_s, vt_s, wt_s, yt_s, rhs, part, q_t, y_s, kx_s,
    sp_all, ex_all, sp_send, ex_send, red, edge,
    lsem, bar_send, bar_recv,
):
    me = lax.axis_index("row")
    g = lax.axis_index("gz")
    barrier = pltpu.get_barrier_semaphore()
    loads = [
        pltpu.make_async_copy(w_hbm, w_v, lsem.at[0]),
        pltpu.make_async_copy(u_hbm, u_v, lsem.at[1]),
        pltpu.make_async_copy(v_hbm, v_v, lsem.at[2]),
    ]
    for load in loads:
        load.start()

    def greet_row(d, carry):
        pl.semaphore_signal(
            barrier, inc=1, device_id={"row": lax.rem(me + d, ROW)}, device_id_type=MESH
        )
        return carry

    def greet_gz(d, carry):
        pl.semaphore_signal(
            barrier, inc=1, device_id={"gz": lax.rem(g + d, GZ)}, device_id_type=MESH
        )
        return carry

    lax.fori_loop(1, ROW, greet_row, 0)
    lax.fori_loop(1, GZ, greet_gz, 0)

    def row_send(src, dst, k, t):
        return pltpu.make_async_remote_copy(
            src, dst, bar_send.at[k], bar_recv.at[k], device_id={"row": t}, device_id_type=MESH
        )

    def gz_send(src, dst, k, t):
        return pltpu.make_async_remote_copy(
            src, dst, bar_send.at[k], bar_recv.at[k], device_id={"gz": t}, device_id_type=MESH
        )

    level = level_ref[...]
    width = jnp.zeros((GZ, DEPTH), f32)
    for n in range(64):
        width = jnp.where(level == n, spacing_ref[n], width)
    lane = lax.broadcasted_iota(jnp.int32, (GZ, DEPTH), 1)
    block = lax.broadcasted_iota(jnp.int32, (GZ, DEPTH), 0)
    shift_up = pltpu.roll(width, 1, 1)
    previous = jnp.where(lane == 0, pltpu.roll(shift_up, 1, 0), shift_up)
    shift_down = pltpu.roll(width, DEPTH - 1, 1)
    following = jnp.where(lane == DEPTH - 1, pltpu.roll(shift_down, GZ - 1, 0), shift_down)
    lower = 1.0 / (0.5 * (previous + width) * width)
    upper = 1.0 / (0.5 * (width + following) * width)
    lower = jnp.where((lane == 0) & (block == 0), 0.0, lower)
    upper = jnp.where((lane == DEPTH - 1) & (block == GZ - 1), 0.0, upper)
    band[0] = lower
    band[1] = upper
    band[2] = -(lower + upper)
    band[3] = 1.0 / width
    for n in range(3):
        row_n = jnp.broadcast_to(band[n, pl.ds(g, 1), :], (DEPTH, DEPTH))
        bmat[n] = row_n.T

    loads[0].wait()
    pick = (lax.broadcasted_iota(jnp.int32, (16, DEPTH), 1) == DEPTH - 1).astype(f32).astype(bf16)
    for n in range(2):
        column = lax.dot_general(
            pick,
            w_v[n].reshape(1024, DEPTH),
            (((1,), (1,)), ((), ())),
            preferred_element_type=f32,
        )
        halo_out[:, n * 1024 : (n + 1) * 1024] = column[0:1, :]
    loads[1].wait()
    loads[2].wait()
    pl.semaphore_wait(barrier, ROW - 1 + GZ - 1)

    above = lax.rem(g + 1, GZ)
    halo_copy = gz_send(halo_out, halo_in, 0, above)
    halo_copy.start()

    def send_u(d, carry):
        t = lax.rem(me + d, ROW)
        row_send(u_v.at[:, t], recv_u.at[:, me], 1, t).start()
        return carry

    lax.fori_loop(1, ROW, send_u, 0)
    recv_u[:, pl.ds(me, 1)] = u_v[:, pl.ds(me, 1)]

    halo_copy.wait()
    has_below = jnp.where(g > 0, 1.0, 0.0)
    first_lane = (lax.broadcasted_iota(jnp.int32, (8, DEPTH), 1) == 0).astype(f32)
    first_row = (lax.broadcasted_iota(jnp.int32, (8, DEPTH), 0) == 0).astype(f32)
    spot = (first_lane * first_row * has_below).astype(bf16)
    for n in range(2):
        wide = jnp.broadcast_to(halo_in[:, n * 1024 : (n + 1) * 1024], (8, 1024)).astype(bf16)
        halo_cols[n] = lax.dot_general(
            wide, spot, (((0,), (0,)), ((), ())), preferred_element_type=f32
        ).reshape(32, 32, DEPTH)
    inv_width = band[3, pl.ds(g, 1), :]
    lane32 = lax.broadcasted_iota(jnp.int32, (32, DEPTH), 1)

    def make_source(t):
        wave = plane_ref[t].astype(f32) * wave_unit
        slopes = []
        for n in range(2):
            upward = w_v[n, t].astype(f32)
            below = jnp.where(lane32 == 0, halo_cols[n, t], pltpu.roll(upward, 1, 1))
            slopes.append((upward - below) * inv_width)
        s_v[0, t] = (-wave * v_v[1, t].astype(f32) + slopes[0]).astype(bf16)
        s_v[1, t] = (wave * v_v[0, t].astype(f32) + slopes[1]).astype(bf16)

    def send_s(t):
        row_send(s_v.at[:, t], recv_s.at[:, me], 2, t).start()

    make_source(lax.rem(me + 1, ROW))

    def source_step(d, carry):
        make_source(lax.rem(me + d, ROW))
        send_s(lax.rem(me + d - 1, ROW))
        return carry

    lax.fori_loop(2, ROW, source_step, 0)
    make_source(me)
    send_s(lax.rem(me + ROW - 1, ROW))
    recv_s[:, pl.ds(me, 1)] = s_v[:, pl.ds(me, 1)]

    outer = lax.broadcasted_iota(jnp.int32, (RADIX, 128), 0)
    inner = lax.broadcasted_iota(jnp.int32, (RADIX, 128), 1)
    mode = 8 * inner + outer
    mode = jnp.where(mode >= 512, mode - 1024, mode)
    wave_x = mode.astype(f32) * (full_turn / 1024.0)
    own_wave = plane_ref[me].astype(f32) * wave_unit
    wave_sq = wave_x * wave_x + own_wave * own_wave
    kx_s[...] = wave_x

    def coef(n, z):
        return jnp.broadcast_to(bmat[n, pl.ds(z, 1), :], (RADIX, 128))

    def factor(j, carry):
        top, bottom, v_top, w_bottom = carry
        z = j
        lo, up = coef(0, z), coef(1, z)
        inv = 1.0 / ((coef(2, z) - wave_sq) - lo * top)
        fe = lo * inv
        top = up * inv
        inv_s[z] = inv
        fe_s[z] = fe
        bc_s[z] = top
        v_top = -fe * v_top
        vs_s[pl.ds(pl.multiple_of(z * 8, 8), 8), :] = v_top
        z = DEPTH - 1 - j
        lo, up = coef(0, z), coef(1, z)
        inv = 1.0 / ((coef(2, z) - wave_sq) - up * bottom)
        fe = up * inv
        bottom = lo * inv
        inv_s[z] = inv
        fe_s[z] = fe
        bc_s[z] = bottom
        w_bottom = -fe * w_bottom
        ws_s[pl.ds(pl.multiple_of(z * 8, 8), 8), :] = w_bottom
        return top, bottom, v_top, w_bottom

    zero = jnp.zeros((RADIX, 128), f32)
    one = jnp.ones((RADIX, 128), f32)
    top, bottom, v_top, w_bottom = lax.fori_loop(0, HALF, factor, (zero, zero, one, one))
    inv_det = 1.0 / (1.0 - top * bottom)

    def at(z):
        return pl.ds(pl.multiple_of(z * 8, 8), 8)

    v_lo = v_top * inv_det
    v_hi = -bottom * v_lo
    w_hi = w_bottom * inv_det
    w_lo = -top * w_hi
    vs_s[at(HALF - 1), :] = v_lo
    vs_s[at(HALF), :] = v_hi
    ws_s[at(HALF - 1), :] = w_lo
    ws_s[at(HALF), :] = w_hi

    def spread(j, carry):
        v_lo, v_hi, w_lo, w_hi = carry
        z = HALF - 1 - j
        bc = bc_s[z]
        v_lo = vs_s[at(z), :] - bc * v_lo
        w_lo = -bc * w_lo
        vs_s[at(z), :] = v_lo
        ws_s[at(z), :] = w_lo
        z = HALF + j
        bc = bc_s[z]
        v_hi = -bc * v_hi
        w_hi = ws_s[at(z), :] - bc * w_hi
        vs_s[at(z), :] = v_hi
        ws_s[at(z), :] = w_hi
        return v_lo, v_hi, w_lo, w_hi

    v_lo, v_hi, w_lo, w_hi = lax.fori_loop(1, HALF, spread, (v_lo, v_hi, w_lo, w_hi))
    sp_send[0] = v_lo
    sp_send[1] = v_hi
    sp_send[2] = w_lo
    sp_send[3] = w_hi
    sp_all[pl.ds(g, 1)] = sp_send[...][None]
    for c in range(RADIX):
        vt_s[c] = vs_s[pl.ds(c, DEPTH, stride=8), :]
        wt_s[c] = ws_s[pl.ds(c, DEPTH, stride=8), :]

    def send_sp(d, carry):
        t = lax.rem(g + d, GZ)
        gz_send(sp_send, sp_all.at[g], 3, t).start()
        return carry

    lax.fori_loop(1, GZ, send_sp, 0)

    def forward(recv, finish):
        def flip(a, carry):
            for n in range(2):
                q_t[n, a] = recv[n, pl.ds(4 * a, 4)].reshape(128, 128).T
            return carry

        lax.fori_loop(0, RADIX, flip, 0)

        def mix(i, carry):
            rows = pl.ds(pl.multiple_of(16 * i, 16), 16)
            xr = [q_t[0, a, rows, :].astype(f32) for a in range(RADIX)]
            xi = [q_t[1, a, rows, :].astype(f32) for a in range(RADIX)]
            for c, (re, im) in enumerate(butterfly(xr, xi)):
                re, im = twisted(re, im, tw_ref, c)
                put_split(y_s, c, rows, re, im)
            return carry

        lax.fori_loop(0, DEPTH // 16, mix, 0)
        for c in range(0, RADIX, 2):
            finish(c, product(c))

    def product(c):
        rows = y_s[c : c + 2].reshape(2 * DEPTH, 512)
        return jnp.dot(rows, weights_ref[0:512, :], preferred_element_type=f32) + jnp.dot(
            rows[:, 0:256], weights_ref[512:768, :], preferred_element_type=f32
        )

    def keep_along(c, acc):
        for n in range(2):
            kx = kx_s[c + n : c + n + 1, :]
            own = acc[n * DEPTH : (n + 1) * DEPTH]
            part[c + n, :, 0:128] = -kx * own[:, 128:256]
            part[c + n, :, 128:256] = kx * own[:, 0:128]

    def keep_rhs(c, acc):
        for n in range(2):
            total = acc[n * DEPTH : (n + 1) * DEPTH] + part[c + n]
            rhs[0, pl.ds(c + n, DEPTH, stride=8), :] = total[:, 0:128]
            rhs[1, pl.ds(c + n, DEPTH, stride=8), :] = total[:, 128:256]

    def row_wait(ref, k):
        row_send(ref.at[:, 0 : ROW - 1], ref.at[:, 0 : ROW - 1], k, me).wait_recv()

    row_wait(recv_u, 1)
    forward(recv_u, keep_along)

    gz_send(sp_all.at[0 : GZ - 1], sp_all.at[0 : GZ - 1], 3, g).wait_recv()
    beta = zero
    for b in range(GZ):
        v_first, v_last, w_first, w_last = (sp_all[b, n] for n in range(4))
        inv = 1.0 / (1.0 - v_first * beta)
        gamma = v_last * beta * inv
        red[0, b] = gamma
        red[1, b] = v_last + gamma * v_first
        red[2, b] = inv
        red[3, b] = inv * v_first
        red[4, b] = inv * w_first
        beta = w_last + gamma * w_first
        red[5, b] = beta

    row_wait(recv_s, 2)
    forward(recv_s, keep_rhs)

    def down(j, carry):
        out = []
        for z, pair in ((j, carry[0:2]), (DEPTH - 1 - j, carry[2:4])):
            inv, fe = inv_s[z], fe_s[z]
            for n in range(2):
                value = rhs[n, at(z), :] * inv - fe * pair[n]
                rhs[n, at(z), :] = value
                out.append(value)
        return tuple(out)

    low_re, low_im, high_re, high_im = lax.fori_loop(0, HALF, down, (zero,) * 4)
    bc_low, bc_high = bc_s[HALF - 1], bc_s[HALF]
    inv_det = 1.0 / (1.0 - bc_low * bc_high)
    low_re = (low_re - bc_low * high_re) * inv_det
    low_im = (low_im - bc_low * high_im) * inv_det
    high_re = high_re - bc_high * low_re
    high_im = high_im - bc_high * low_im
    rhs[0, at(HALF - 1), :] = low_re
    rhs[1, at(HALF - 1), :] = low_im
    rhs[0, at(HALF), :] = high_re
    rhs[1, at(HALF), :] = high_im

    def up_again(j, carry):
        out = []
        for z, pair in ((HALF - 1 - j, carry[0:2]), (HALF + j, carry[2:4])):
            bc = bc_s[z]
            for n in range(2):
                value = rhs[n, at(z), :] - bc * pair[n]
                rhs[n, at(z), :] = value
                out.append(value)
        return tuple(out)

    low_re, low_im, high_re, high_im = lax.fori_loop(
        1, HALF, up_again, (low_re, low_im, high_re, high_im)
    )
    ex_send[0] = low_re
    ex_send[1] = low_im
    ex_send[2] = high_re
    ex_send[3] = high_im
    ex_all[pl.ds(g, 1)] = ex_send[...][None]

    def send_ex(d, carry):
        t = lax.rem(g + d, GZ)
        gz_send(ex_send, ex_all.at[g], 4, t).start()
        return carry

    lax.fori_loop(1, GZ, send_ex, 0)
    for c in range(RADIX):
        for n in range(2):
            yt_s[n, c] = rhs[n, pl.ds(c, DEPTH, stride=8), :]
    gz_send(ex_all.at[0 : GZ - 1], ex_all.at[0 : GZ - 1], 4, g).wait_recv()

    for n in range(2):
        alpha = zero
        befores = []
        for b in range(GZ):
            befores.append(alpha)
            alpha = (
                ex_all[b, 2 + n] + red[0, b] * ex_all[b, n] + red[1, b] * alpha
            )
        first = zero
        edge[1, n, GZ - 1] = zero
        for b in range(GZ - 1, -1, -1):
            first = red[2, b] * ex_all[b, n] + red[3, b] * befores[b] + red[4, b] * first
            if b > 0:
                edge[1, n, b - 1] = first
                edge[0, n, b] = befores[b] + red[5, b - 1] * first
        edge[0, n, 0] = zero

    from_below = [edge[0, n, g] for n in range(2)]
    from_above = [edge[1, n, g] for n in range(2)]

    def correct(i, carry):
        rows = pl.ds(pl.multiple_of(16 * i, 16), 16)
        for c in range(RADIX):
            v_c, w_c = vt_s[c, rows, :], wt_s[c, rows, :]
            full = [
                yt_s[n, c, rows, :]
                + v_c * from_below[n][c : c + 1, :]
                + w_c * from_above[n][c : c + 1, :]
                for n in range(2)
            ]
            put_split(y_s, c, rows, full[1], full[0])
        return carry

    lax.fori_loop(0, DEPTH // 16, correct, 0)
    for c in range(0, RADIX, 2):
        part[c : c + 2] = product(c).reshape(2, DEPTH, 256)

    def unmix(i, carry):
        rows = pl.ds(pl.multiple_of(16 * i, 16), 16)
        turned = [
            twisted(part[c, rows, 0:128], part[c, rows, 128:256], tw_ref, c) for c in range(RADIX)
        ]
        mixed = butterfly([t[0] for t in turned], [t[1] for t in turned])
        for j, (first, second) in enumerate(mixed):
            q_t[0, j, rows, :] = second.astype(bf16)
            q_t[1, j, rows, :] = first.astype(bf16)
        return carry

    lax.fori_loop(0, DEPTH // 16, unmix, 0)

    start = me // 4

    def give(jj, carry):
        j = lax.rem(start + jj, RADIX)
        for n in range(2):
            out_v[n, pl.ds(4 * j, 4)] = q_t[n, j].T.reshape(4, 32, DEPTH)
        return carry

    def give_send(jj, carry):
        j = lax.rem(start + jj, RADIX)
        for n in range(4):
            t = 4 * j + n

            @pl.when(t != me)
            def _():
                row_send(out_v.at[:, t], out_ref.at[:, me], 5, t).start()

        return carry

    give(0, 0)

    def give_step(jj, carry):
        give(jj, carry)
        give_send(jj - 1, carry)
        return carry

    lax.fori_loop(1, RADIX, give_step, 0)
    own = pltpu.make_async_copy(out_v.at[:, me], out_ref.at[:, me], lsem.at[0])
    own.start()
    give_send(RADIX - 1, 0)
    own.wait()
    row_wait(out_ref, 5)
    for k, ref in ((1, u_v), (2, s_v), (5, out_v)):
        row_send(ref.at[:, 0 : ROW - 1], ref.at[:, 0 : ROW - 1], k, me).wait_send()
    for k, ref in ((3, sp_all), (4, ex_all)):
        gz_send(ref.at[0 : GZ - 1], ref.at[0 : GZ - 1], k, g).wait_send()


def on_device(velocity_x, velocity_y, velocity_z, spacing, level_index, plane_index):
    weights, twiddle = tables()
    block = (2, 32, 32, 128)
    line = (DEPTH, RADIX, 128)
    flat = (DEPTH * RADIX, 128)
    tile = (RADIX, DEPTH, 128)
    pressure = pl.pallas_call(
        kernel,
        out_shape=jax.ShapeDtypeStruct(block, bf16),
        in_specs=[
            pl.BlockSpec(memory_space=pl.ANY),
            pl.BlockSpec(memory_space=pl.ANY),
            pl.BlockSpec(memory_space=pl.ANY),
            pl.BlockSpec(memory_space=pltpu.SMEM),
            pl.BlockSpec(memory_space=pltpu.VMEM),
            pl.BlockSpec(memory_space=pltpu.SMEM),
            pl.BlockSpec(memory_space=pltpu.VMEM),
            pl.BlockSpec(memory_space=pltpu.VMEM),
        ],
        out_specs=pl.BlockSpec(memory_space=pl.ANY),
        scratch_shapes=[
            pltpu.VMEM(block, bf16),
            pltpu.VMEM(block, bf16),
            pltpu.VMEM(block, bf16),
            pltpu.VMEM(block, bf16),
            pltpu.VMEM(block, bf16),
            pltpu.VMEM(block, bf16),
            pltpu.VMEM(block, bf16),
            pltpu.VMEM((1, 2048), f32),
            pltpu.VMEM((1, 2048), f32),
            pltpu.VMEM(block, f32),
            pltpu.VMEM((4, 8, 128), f32),
            pltpu.VMEM((3, 128, 128), f32),
            pltpu.VMEM(line, f32),
            pltpu.VMEM(line, f32),
            pltpu.VMEM(line, f32),
            pltpu.VMEM(flat, f32),
            pltpu.VMEM(flat, f32),
            pltpu.VMEM(tile, f32),
            pltpu.VMEM(tile, f32),
            pltpu.VMEM((2,) + tile, f32),
            pltpu.VMEM((2,) + flat, f32),
            pltpu.VMEM((RADIX, DEPTH, 256), f32),
            pltpu.VMEM((2, RADIX, 128, 128), bf16),
            pltpu.VMEM((RADIX, DEPTH, 512), bf16),
            pltpu.VMEM((RADIX, 128), f32),
            pltpu.VMEM((GZ, 4, RADIX, 128), f32),
            pltpu.VMEM((GZ, 4, RADIX, 128), f32),
            pltpu.VMEM((4, RADIX, 128), f32),
            pltpu.VMEM((4, RADIX, 128), f32),
            pltpu.VMEM((6, GZ, RADIX, 128), f32),
            pltpu.VMEM((2, 2, GZ, RADIX, 128), f32),
            pltpu.SemaphoreType.DMA((3,)),
            pltpu.SemaphoreType.DMA((6,)),
            pltpu.SemaphoreType.DMA((6,)),
        ],
        compiler_params=pltpu.CompilerParams(
            collective_id=0, has_side_effects=True, vmem_limit_bytes=48 * 1024 * 1024
        ),
        name="poisson",
    )(
        velocity_x,
        velocity_y,
        velocity_z,
        spacing,
        level_index.reshape(8, 128),
        plane_index,
        jnp.asarray(weights),
        jnp.asarray(twiddle),
    )
    return pressure.astype(f32) * (1.0 / 1024.0)


def solution(mesh):
    placed = (
        P(None, None, "row", "gz"),
        P(None, None, "row", "gz"),
        P(None, None, "row", "gz"),
        P(),
        P(),
        P(),
    )
    return jax.shard_map(
        on_device, mesh=mesh, in_specs=placed, out_specs=P(None, None, "row", "gz"), check_vma=False
    )
```

```python
import math

import jax
import jax.numpy as jnp
import numpy as np
from jax import lax
from jax.experimental import pallas as pl
from jax.experimental.pallas import tpu as pltpu
from jax.sharding import PartitionSpec as P

MESH = pl.DeviceIdType.MESH
f32 = jnp.float32
bf16 = jnp.bfloat16
full_turn = 2.0 * math.pi
wave_unit = 2.0 * math.pi / 2048.0
ROW = 32
GZ = 8
DEPTH = 128
RADIX = 8
HALF = DEPTH // 2
ROOT_HALF = math.sqrt(0.5)


def tables():
    idx = np.arange(128)
    angle = 2.0 * np.pi / 128.0 * ((idx[:, None] * idx[None, :]) % 128)
    c, s = np.cos(angle), np.sin(angle)
    w = np.block([[c, -s], [s, c]]).astype(np.float32)
    hi = w.astype(jnp.bfloat16)
    lo = (w - hi.astype(np.float32)).astype(jnp.bfloat16)
    weights = np.concatenate([hi, hi, lo], axis=0)
    twist = 2.0 * np.pi / 1024.0 * (np.arange(8)[:, None] * idx[None, :])
    twiddle = np.concatenate([np.cos(twist), np.sin(twist)], axis=0).astype(np.float32)
    return weights, twiddle


def butterfly(xr, xi):
    def add(p, q):
        return (p[0] + q[0], p[1] + q[1])

    def sub(p, q):
        return (p[0] - q[0], p[1] - q[1])

    def turn(p):
        return (p[1], -p[0])

    x = list(zip(xr, xi))
    a0, a1 = add(x[0], x[4]), sub(x[0], x[4])
    a2, a3 = add(x[2], x[6]), turn(sub(x[2], x[6]))
    b0, b1 = add(x[1], x[5]), sub(x[1], x[5])
    b2, b3 = add(x[3], x[7]), turn(sub(x[3], x[7]))
    e = [add(a0, a2), add(a1, a3), sub(a0, a2), sub(a1, a3)]
    o = [add(b0, b2), add(b1, b3), sub(b0, b2), sub(b1, b3)]
    o1 = ((o[1][0] + o[1][1]) * ROOT_HALF, (o[1][1] - o[1][0]) * ROOT_HALF)
    o2 = turn(o[2])
    o3 = ((o[3][1] - o[3][0]) * ROOT_HALF, -(o[3][0] + o[3][1]) * ROOT_HALF)
    odd = [o[0], o1, o2, o3]
    return [add(e[k], odd[k]) for k in range(4)] + [sub(e[k], odd[k]) for k in range(4)]


def twisted(re, im, tw_ref, c):
    if c == 0:
        return re, im
    cos = tw_ref[c : c + 1, :]
    sin = tw_ref[8 + c : 9 + c, :]
    return re * cos + im * sin, im * cos - re * sin


def put_split(y_ref, c, rows, re, im):
    re_hi = re.astype(bf16)
    im_hi = im.astype(bf16)
    y_ref[c, rows, 0:128] = re_hi
    y_ref[c, rows, 128:256] = im_hi
    y_ref[c, rows, 256:384] = (re - re_hi.astype(f32)).astype(bf16)
    y_ref[c, rows, 384:512] = (im - im_hi.astype(f32)).astype(bf16)


def kernel(
    u_hbm, v_hbm, w_hbm, spacing_hbm, level_hbm, plane_hbm, weights_hbm, tw_hbm,
    out_ref,
    spacing_ref, level_ref, plane_ref, weights_ref, tw_ref,
    u_v, v_v, w_v, s_v, recv_u, recv_s, out_v, halo_out, halo_in, halo_cols, band, bmat,
    inv_s, fe_s, bc_s, vs_s, ws_s, vt_s, wt_s, yt_s, rhs, part, q_t, y_s, kx_s,
    sp_all, ex_all, sp_send, ex_send, red, edge,
    lsem, bar_send, bar_recv,
):
    me = lax.axis_index("row")
    g = lax.axis_index("gz")
    barrier = pltpu.get_barrier_semaphore()
    loads = [
        pltpu.make_async_copy(w_hbm, w_v, lsem.at[0]),
        pltpu.make_async_copy(u_hbm, u_v, lsem.at[1]),
        pltpu.make_async_copy(v_hbm, v_v, lsem.at[2]),
        pltpu.make_async_copy(level_hbm, level_ref, lsem.at[3]),
        pltpu.make_async_copy(spacing_hbm, spacing_ref, lsem.at[4]),
        pltpu.make_async_copy(plane_hbm, plane_ref, lsem.at[5]),
        pltpu.make_async_copy(tw_hbm, tw_ref, lsem.at[6]),
        pltpu.make_async_copy(weights_hbm, weights_ref, lsem.at[7]),
    ]
    for load in loads:
        load.start()

    def greet_row(d, carry):
        pl.semaphore_signal(
            barrier, inc=1, device_id={"row": lax.rem(me + d, ROW)}, device_id_type=MESH
        )
        return carry

    def greet_gz(d, carry):
        pl.semaphore_signal(
            barrier, inc=1, device_id={"gz": lax.rem(g + d, GZ)}, device_id_type=MESH
        )
        return carry

    lax.fori_loop(1, ROW, greet_row, 0)
    lax.fori_loop(1, GZ, greet_gz, 0)

    def row_send(src, dst, k, t):
        return pltpu.make_async_remote_copy(
            src, dst, bar_send.at[k], bar_recv.at[k], device_id={"row": t}, device_id_type=MESH
        )

    def gz_send(src, dst, k, t):
        return pltpu.make_async_remote_copy(
            src, dst, bar_send.at[k], bar_recv.at[k], device_id={"gz": t}, device_id_type=MESH
        )

    for load in loads[3:]:
        load.wait()

    level = level_ref[...]
    width = jnp.zeros((GZ, DEPTH), f32)
    for n in range(64):
        width = jnp.where(level == n, spacing_ref[n], width)
    lane = lax.broadcasted_iota(jnp.int32, (GZ, DEPTH), 1)
    block = lax.broadcasted_iota(jnp.int32, (GZ, DEPTH), 0)
    shift_up = pltpu.roll(width, 1, 1)
    previous = jnp.where(lane == 0, pltpu.roll(shift_up, 1, 0), shift_up)
    shift_down = pltpu.roll(width, DEPTH - 1, 1)
    following = jnp.where(lane == DEPTH - 1, pltpu.roll(shift_down, GZ - 1, 0), shift_down)
    lower = 1.0 / (0.5 * (previous + width) * width)
    upper = 1.0 / (0.5 * (width + following) * width)
    lower = jnp.where((lane == 0) & (block == 0), 0.0, lower)
    upper = jnp.where((lane == DEPTH - 1) & (block == GZ - 1), 0.0, upper)
    band[0] = lower
    band[1] = upper
    band[2] = -(lower + upper)
    band[3] = 1.0 / width
    for n in range(3):
        row_n = jnp.broadcast_to(band[n, pl.ds(g, 1), :], (DEPTH, DEPTH))
        bmat[n] = row_n.T

    loads[0].wait()
    pick = (lax.broadcasted_iota(jnp.int32, (16, DEPTH), 1) == DEPTH - 1).astype(f32).astype(bf16)
    for n in range(2):
        column = lax.dot_general(
            pick,
            w_v[n].reshape(1024, DEPTH),
            (((1,), (1,)), ((), ())),
            preferred_element_type=f32,
        )
        halo_out[:, n * 1024 : (n + 1) * 1024] = column[0:1, :]
    loads[1].wait()
    loads[2].wait()
    pl.semaphore_wait(barrier, ROW - 1 + GZ - 1)

    above = lax.rem(g + 1, GZ)
    halo_copy = gz_send(halo_out, halo_in, 0, above)
    halo_copy.start()

    def send_u(d, carry):
        t = lax.rem(me + d, ROW)
        row_send(u_v.at[:, t], recv_u.at[:, me], 1, t).start()
        return carry

    lax.fori_loop(1, ROW, send_u, 0)
    recv_u[:, pl.ds(me, 1)] = u_v[:, pl.ds(me, 1)]

    halo_copy.wait()
    has_below = jnp.where(g > 0, 1.0, 0.0)
    first_lane = (lax.broadcasted_iota(jnp.int32, (8, DEPTH), 1) == 0).astype(f32)
    first_row = (lax.broadcasted_iota(jnp.int32, (8, DEPTH), 0) == 0).astype(f32)
    spot = (first_lane * first_row * has_below).astype(bf16)
    for n in range(2):
        wide = jnp.broadcast_to(halo_in[:, n * 1024 : (n + 1) * 1024], (8, 1024)).astype(bf16)
        halo_cols[n] = lax.dot_general(
            wide, spot, (((0,), (0,)), ((), ())), preferred_element_type=f32
        ).reshape(32, 32, DEPTH)
    inv_width = band[3, pl.ds(g, 1), :]
    lane32 = lax.broadcasted_iota(jnp.int32, (32, DEPTH), 1)

    def make_source(t):
        wave = plane_ref[t].astype(f32) * wave_unit
        slopes = []
        for n in range(2):
            upward = w_v[n, t].astype(f32)
            below = jnp.where(lane32 == 0, halo_cols[n, t], pltpu.roll(upward, 1, 1))
            slopes.append((upward - below) * inv_width)
        s_v[0, t] = (-wave * v_v[1, t].astype(f32) + slopes[0]).astype(bf16)
        s_v[1, t] = (wave * v_v[0, t].astype(f32) + slopes[1]).astype(bf16)

    def send_s(t):
        row_send(s_v.at[:, t], recv_s.at[:, me], 2, t).start()

    make_source(lax.rem(me + 1, ROW))

    def source_step(d, carry):
        make_source(lax.rem(me + d, ROW))
        send_s(lax.rem(me + d - 1, ROW))
        return carry

    lax.fori_loop(2, ROW, source_step, 0)
    make_source(me)
    send_s(lax.rem(me + ROW - 1, ROW))
    recv_s[:, pl.ds(me, 1)] = s_v[:, pl.ds(me, 1)]

    outer = lax.broadcasted_iota(jnp.int32, (RADIX, 128), 0)
    inner = lax.broadcasted_iota(jnp.int32, (RADIX, 128), 1)
    mode = 8 * inner + outer
    mode = jnp.where(mode >= 512, mode - 1024, mode)
    wave_x = mode.astype(f32) * (full_turn / 1024.0)
    own_wave = plane_ref[me].astype(f32) * wave_unit
    wave_sq = wave_x * wave_x + own_wave * own_wave
    kx_s[...] = wave_x

    def coef(n, z):
        return jnp.broadcast_to(bmat[n, pl.ds(z, 1), :], (RADIX, 128))

    def factor(j, carry):
        top, bottom, v_top, w_bottom = carry
        z = j
        lo, up = coef(0, z), coef(1, z)
        inv = 1.0 / ((coef(2, z) - wave_sq) - lo * top)
        fe = lo * inv
        top = up * inv
        inv_s[z] = inv
        fe_s[z] = fe
        bc_s[z] = top
        v_top = -fe * v_top
        vs_s[pl.ds(pl.multiple_of(z * 8, 8), 8), :] = v_top
        z = DEPTH - 1 - j
        lo, up = coef(0, z), coef(1, z)
        inv = 1.0 / ((coef(2, z) - wave_sq) - up * bottom)
        fe = up * inv
        bottom = lo * inv
        inv_s[z] = inv
        fe_s[z] = fe
        bc_s[z] = bottom
        w_bottom = -fe * w_bottom
        ws_s[pl.ds(pl.multiple_of(z * 8, 8), 8), :] = w_bottom
        return top, bottom, v_top, w_bottom

    zero = jnp.zeros((RADIX, 128), f32)
    one = jnp.ones((RADIX, 128), f32)
    top, bottom, v_top, w_bottom = lax.fori_loop(0, HALF, factor, (zero, zero, one, one))
    inv_det = 1.0 / (1.0 - top * bottom)

    def at(z):
        return pl.ds(pl.multiple_of(z * 8, 8), 8)

    v_lo = v_top * inv_det
    v_hi = -bottom * v_lo
    w_hi = w_bottom * inv_det
    w_lo = -top * w_hi
    vs_s[at(HALF - 1), :] = v_lo
    vs_s[at(HALF), :] = v_hi
    ws_s[at(HALF - 1), :] = w_lo
    ws_s[at(HALF), :] = w_hi

    def spread(j, carry):
        v_lo, v_hi, w_lo, w_hi = carry
        z = HALF - 1 - j
        bc = bc_s[z]
        v_lo = vs_s[at(z), :] - bc * v_lo
        w_lo = -bc * w_lo
        vs_s[at(z), :] = v_lo
        ws_s[at(z), :] = w_lo
        z = HALF + j
        bc = bc_s[z]
        v_hi = -bc * v_hi
        w_hi = ws_s[at(z), :] - bc * w_hi
        vs_s[at(z), :] = v_hi
        ws_s[at(z), :] = w_hi
        return v_lo, v_hi, w_lo, w_hi

    v_lo, v_hi, w_lo, w_hi = lax.fori_loop(1, HALF, spread, (v_lo, v_hi, w_lo, w_hi))
    sp_send[0] = v_lo
    sp_send[1] = v_hi
    sp_send[2] = w_lo
    sp_send[3] = w_hi
    sp_all[pl.ds(g, 1)] = sp_send[...][None]
    for c in range(RADIX):
        vt_s[c] = vs_s[pl.ds(c, DEPTH, stride=8), :]
        wt_s[c] = ws_s[pl.ds(c, DEPTH, stride=8), :]

    def send_sp(d, carry):
        t = lax.rem(g + d, GZ)
        gz_send(sp_send, sp_all.at[g], 3, t).start()
        return carry

    lax.fori_loop(1, GZ, send_sp, 0)

    def forward(recv, finish):
        def flip(a, carry):
            for n in range(2):
                q_t[n, a] = recv[n, pl.ds(4 * a, 4)].reshape(128, 128).T
            return carry

        lax.fori_loop(0, RADIX, flip, 0)

        def mix(i, carry):
            rows = pl.ds(pl.multiple_of(16 * i, 16), 16)
            xr = [q_t[0, a, rows, :].astype(f32) for a in range(RADIX)]
            xi = [q_t[1, a, rows, :].astype(f32) for a in range(RADIX)]
            for c, (re, im) in enumerate(butterfly(xr, xi)):
                re, im = twisted(re, im, tw_ref, c)
                put_split(y_s, c, rows, re, im)
            return carry

        lax.fori_loop(0, DEPTH // 16, mix, 0)
        for c in range(0, RADIX, 2):
            finish(c, product(c))

    def product(c):
        rows = y_s[c : c + 2].reshape(2 * DEPTH, 512)
        return jnp.dot(rows, weights_ref[0:512, :], preferred_element_type=f32) + jnp.dot(
            rows[:, 0:256], weights_ref[512:768, :], preferred_element_type=f32
        )

    def keep_along(c, acc):
        for n in range(2):
            kx = kx_s[c + n : c + n + 1, :]
            own = acc[n * DEPTH : (n + 1) * DEPTH]
            part[c + n, :, 0:128] = -kx * own[:, 128:256]
            part[c + n, :, 128:256] = kx * own[:, 0:128]

    def keep_rhs(c, acc):
        for n in range(2):
            total = acc[n * DEPTH : (n + 1) * DEPTH] + part[c + n]
            rhs[0, pl.ds(c + n, DEPTH, stride=8), :] = total[:, 0:128]
            rhs[1, pl.ds(c + n, DEPTH, stride=8), :] = total[:, 128:256]

    def row_wait(ref, k):
        row_send(ref.at[:, 0 : ROW - 1], ref.at[:, 0 : ROW - 1], k, me).wait_recv()

    row_wait(recv_u, 1)
    forward(recv_u, keep_along)

    gz_send(sp_all.at[0 : GZ - 1], sp_all.at[0 : GZ - 1], 3, g).wait_recv()
    beta = zero
    for b in range(GZ):
        v_first, v_last, w_first, w_last = (sp_all[b, n] for n in range(4))
        inv = 1.0 / (1.0 - v_first * beta)
        gamma = v_last * beta * inv
        red[0, b] = gamma
        red[1, b] = v_last + gamma * v_first
        red[2, b] = inv
        red[3, b] = inv * v_first
        red[4, b] = inv * w_first
        beta = w_last + gamma * w_first
        red[5, b] = beta

    row_wait(recv_s, 2)
    forward(recv_s, keep_rhs)

    def down(j, carry):
        out = []
        for z, pair in ((j, carry[0:2]), (DEPTH - 1 - j, carry[2:4])):
            inv, fe = inv_s[z], fe_s[z]
            for n in range(2):
                value = rhs[n, at(z), :] * inv - fe * pair[n]
                rhs[n, at(z), :] = value
                out.append(value)
        return tuple(out)

    low_re, low_im, high_re, high_im = lax.fori_loop(0, HALF, down, (zero,) * 4)
    bc_low, bc_high = bc_s[HALF - 1], bc_s[HALF]
    inv_det = 1.0 / (1.0 - bc_low * bc_high)
    low_re = (low_re - bc_low * high_re) * inv_det
    low_im = (low_im - bc_low * high_im) * inv_det
    high_re = high_re - bc_high * low_re
    high_im = high_im - bc_high * low_im
    rhs[0, at(HALF - 1), :] = low_re
    rhs[1, at(HALF - 1), :] = low_im
    rhs[0, at(HALF), :] = high_re
    rhs[1, at(HALF), :] = high_im

    def up_again(j, carry):
        out = []
        for z, pair in ((HALF - 1 - j, carry[0:2]), (HALF + j, carry[2:4])):
            bc = bc_s[z]
            for n in range(2):
                value = rhs[n, at(z), :] - bc * pair[n]
                rhs[n, at(z), :] = value
                out.append(value)
        return tuple(out)

    low_re, low_im, high_re, high_im = lax.fori_loop(
        1, HALF, up_again, (low_re, low_im, high_re, high_im)
    )
    ex_send[0] = low_re
    ex_send[1] = low_im
    ex_send[2] = high_re
    ex_send[3] = high_im
    ex_all[pl.ds(g, 1)] = ex_send[...][None]

    def send_ex(d, carry):
        t = lax.rem(g + d, GZ)
        gz_send(ex_send, ex_all.at[g], 4, t).start()
        return carry

    lax.fori_loop(1, GZ, send_ex, 0)
    for c in range(RADIX):
        for n in range(2):
            yt_s[n, c] = rhs[n, pl.ds(c, DEPTH, stride=8), :]
    gz_send(ex_all.at[0 : GZ - 1], ex_all.at[0 : GZ - 1], 4, g).wait_recv()

    for n in range(2):
        alpha = zero
        befores = []
        for b in range(GZ):
            befores.append(alpha)
            alpha = (
                ex_all[b, 2 + n] + red[0, b] * ex_all[b, n] + red[1, b] * alpha
            )
        first = zero
        edge[1, n, GZ - 1] = zero
        for b in range(GZ - 1, -1, -1):
            first = red[2, b] * ex_all[b, n] + red[3, b] * befores[b] + red[4, b] * first
            if b > 0:
                edge[1, n, b - 1] = first
                edge[0, n, b] = befores[b] + red[5, b - 1] * first
        edge[0, n, 0] = zero

    from_below = [edge[0, n, g] for n in range(2)]
    from_above = [edge[1, n, g] for n in range(2)]

    def correct(i, carry):
        rows = pl.ds(pl.multiple_of(16 * i, 16), 16)
        for c in range(RADIX):
            v_c, w_c = vt_s[c, rows, :], wt_s[c, rows, :]
            full = [
                yt_s[n, c, rows, :]
                + v_c * from_below[n][c : c + 1, :]
                + w_c * from_above[n][c : c + 1, :]
                for n in range(2)
            ]
            put_split(y_s, c, rows, full[1], full[0])
        return carry

    lax.fori_loop(0, DEPTH // 16, correct, 0)
    for c in range(0, RADIX, 2):
        part[c : c + 2] = product(c).reshape(2, DEPTH, 256)

    def unmix(i, carry):
        rows = pl.ds(pl.multiple_of(16 * i, 16), 16)
        turned = [
            twisted(part[c, rows, 0:128], part[c, rows, 128:256], tw_ref, c) for c in range(RADIX)
        ]
        mixed = butterfly([t[0] for t in turned], [t[1] for t in turned])
        for j, (first, second) in enumerate(mixed):
            q_t[0, j, rows, :] = second.astype(bf16)
            q_t[1, j, rows, :] = first.astype(bf16)
        return carry

    lax.fori_loop(0, DEPTH // 16, unmix, 0)

    start = me // 4

    def give(jj, carry):
        j = lax.rem(start + jj, RADIX)
        for n in range(2):
            out_v[n, pl.ds(4 * j, 4)] = q_t[n, j].T.reshape(4, 32, DEPTH)
        return carry

    def give_send(jj, carry):
        j = lax.rem(start + jj, RADIX)
        for n in range(4):
            t = 4 * j + n

            @pl.when(t != me)
            def _():
                row_send(out_v.at[:, t], out_ref.at[:, me], 5, t).start()

        return carry

    give(0, 0)

    def give_step(jj, carry):
        give(jj, carry)
        give_send(jj - 1, carry)
        return carry

    lax.fori_loop(1, RADIX, give_step, 0)
    own = pltpu.make_async_copy(out_v.at[:, me], out_ref.at[:, me], lsem.at[0])
    own.start()
    give_send(RADIX - 1, 0)
    own.wait()
    row_wait(out_ref, 5)
    for k, ref in ((1, u_v), (2, s_v), (5, out_v)):
        row_send(ref.at[:, 0 : ROW - 1], ref.at[:, 0 : ROW - 1], k, me).wait_send()
    for k, ref in ((3, sp_all), (4, ex_all)):
        gz_send(ref.at[0 : GZ - 1], ref.at[0 : GZ - 1], k, g).wait_send()


def on_device(velocity_x, velocity_y, velocity_z, spacing, level_index, plane_index):
    weights, twiddle = tables()
    block = (2, 32, 32, 128)
    line = (DEPTH, RADIX, 128)
    flat = (DEPTH * RADIX, 128)
    tile = (RADIX, DEPTH, 128)
    pressure = pl.pallas_call(
        kernel,
        out_shape=jax.ShapeDtypeStruct(block, bf16),
        in_specs=[
            pl.BlockSpec(memory_space=pltpu.HBM),
        ]
        * 8,
        out_specs=pl.BlockSpec(memory_space=pltpu.HBM),
        scratch_shapes=[
            pltpu.SMEM((64,), f32),
            pltpu.VMEM((8, 128), jnp.int32),
            pltpu.SMEM((32,), jnp.int32),
            pltpu.VMEM((768, 256), bf16),
            pltpu.VMEM((16, 128), f32),
            pltpu.VMEM(block, bf16),
            pltpu.VMEM(block, bf16),
            pltpu.VMEM(block, bf16),
            pltpu.VMEM(block, bf16),
            pltpu.VMEM(block, bf16),
            pltpu.VMEM(block, bf16),
            pltpu.VMEM(block, bf16),
            pltpu.VMEM((1, 2048), f32),
            pltpu.VMEM((1, 2048), f32),
            pltpu.VMEM(block, f32),
            pltpu.VMEM((4, 8, 128), f32),
            pltpu.VMEM((3, 128, 128), f32),
            pltpu.VMEM(line, f32),
            pltpu.VMEM(line, f32),
            pltpu.VMEM(line, f32),
            pltpu.VMEM(flat, f32),
            pltpu.VMEM(flat, f32),
            pltpu.VMEM(tile, f32),
            pltpu.VMEM(tile, f32),
            pltpu.VMEM((2,) + tile, f32),
            pltpu.VMEM((2,) + flat, f32),
            pltpu.VMEM((RADIX, DEPTH, 256), f32),
            pltpu.VMEM((2, RADIX, 128, 128), bf16),
            pltpu.VMEM((RADIX, DEPTH, 512), bf16),
            pltpu.VMEM((RADIX, 128), f32),
            pltpu.VMEM((GZ, 4, RADIX, 128), f32),
            pltpu.VMEM((GZ, 4, RADIX, 128), f32),
            pltpu.VMEM((4, RADIX, 128), f32),
            pltpu.VMEM((4, RADIX, 128), f32),
            pltpu.VMEM((6, GZ, RADIX, 128), f32),
            pltpu.VMEM((2, 2, GZ, RADIX, 128), f32),
            pltpu.SemaphoreType.DMA((8,)),
            pltpu.SemaphoreType.DMA((6,)),
            pltpu.SemaphoreType.DMA((6,)),
        ],
        compiler_params=pltpu.CompilerParams(
            collective_id=0, has_side_effects=True, vmem_limit_bytes=67043328
        ),
        name="poisson",
    )(
        velocity_x,
        velocity_y,
        velocity_z,
        spacing,
        level_index.reshape(8, 128),
        plane_index,
        jnp.asarray(weights),
        jnp.asarray(twiddle),
    )
    return pressure.astype(f32) * (1.0 / 1024.0)


def solution(mesh):
    placed = (
        P(None, None, "row", "gz"),
        P(None, None, "row", "gz"),
        P(None, None, "row", "gz"),
        P(),
        P(),
        P(),
    )
    return jax.shard_map(
        on_device, mesh=mesh, in_specs=placed, out_specs=P(None, None, "row", "gz"), check_vma=False
    )
```

```python
import math

import jax
import jax.numpy as jnp
import numpy as np
from jax import lax
from jax.experimental import pallas as pl
from jax.experimental.pallas import tpu as pltpu
from jax.sharding import PartitionSpec as P

MESH = pl.DeviceIdType.MESH
f32 = jnp.float32
bf16 = jnp.bfloat16
full_turn = 2.0 * math.pi
wave_unit = 2.0 * math.pi / 2048.0
ROW = 32
GZ = 8
DEPTH = 128
RADIX = 8
HALF = DEPTH // 2
ROOT_HALF = math.sqrt(0.5)


def tables():
    idx = np.arange(128)
    angle = 2.0 * np.pi / 128.0 * ((idx[:, None] * idx[None, :]) % 128)
    c, s = np.cos(angle), np.sin(angle)
    w = np.block([[c, -s], [s, c]]).astype(np.float32)
    hi = w.astype(jnp.bfloat16)
    lo = (w - hi.astype(np.float32)).astype(jnp.bfloat16)
    weights = np.concatenate([hi, hi, lo], axis=0)
    twist = 2.0 * np.pi / 1024.0 * (np.arange(8)[:, None] * idx[None, :])
    twiddle = np.concatenate([np.cos(twist), np.sin(twist)], axis=0).astype(np.float32)
    return weights, twiddle


def butterfly(xr, xi):
    def add(p, q):
        return (p[0] + q[0], p[1] + q[1])

    def sub(p, q):
        return (p[0] - q[0], p[1] - q[1])

    def turn(p):
        return (p[1], -p[0])

    x = list(zip(xr, xi))
    a0, a1 = add(x[0], x[4]), sub(x[0], x[4])
    a2, a3 = add(x[2], x[6]), turn(sub(x[2], x[6]))
    b0, b1 = add(x[1], x[5]), sub(x[1], x[5])
    b2, b3 = add(x[3], x[7]), turn(sub(x[3], x[7]))
    e = [add(a0, a2), add(a1, a3), sub(a0, a2), sub(a1, a3)]
    o = [add(b0, b2), add(b1, b3), sub(b0, b2), sub(b1, b3)]
    o1 = ((o[1][0] + o[1][1]) * ROOT_HALF, (o[1][1] - o[1][0]) * ROOT_HALF)
    o2 = turn(o[2])
    o3 = ((o[3][1] - o[3][0]) * ROOT_HALF, -(o[3][0] + o[3][1]) * ROOT_HALF)
    odd = [o[0], o1, o2, o3]
    return [add(e[k], odd[k]) for k in range(4)] + [sub(e[k], odd[k]) for k in range(4)]


def twisted(re, im, tw_ref, c):
    if c == 0:
        return re, im
    cos = tw_ref[c : c + 1, :]
    sin = tw_ref[8 + c : 9 + c, :]
    return re * cos + im * sin, im * cos - re * sin


def put_split(y_ref, c, rows, re, im):
    re_hi = re.astype(bf16)
    im_hi = im.astype(bf16)
    y_ref[c, rows, 0:128] = re_hi
    y_ref[c, rows, 128:256] = im_hi
    y_ref[c, rows, 256:384] = (re - re_hi.astype(f32)).astype(bf16)
    y_ref[c, rows, 384:512] = (im - im_hi.astype(f32)).astype(bf16)


def far_first(i):
    return lax.rem(2 + i + (i // 2) * (1 + 2 * lax.rem(i, 2)), 4)


def kernel(
    u_hbm, v_hbm, w_hbm, spacing_hbm, level_hbm, plane_hbm, weights_hbm, weights_t_hbm, tw_hbm,
    out_ref,
    spacing_ref, level_ref, plane_ref, weights_ref, weights_t, tw_ref,
    u_v, v_v, w_v, s_v, recv_u, recv_s, out_v, halo_out, halo_in, halo_cols, band, bmat,
    inv_s, fe_s, bc_s, vs_s, ws_s, vt_s, wt_s, yt_s, rhs, part, part_t, tc_s, ts_s, q_t, y_s, kx_s,
    sp_all, ex_all, sp_send, ex_send, red, edge,
    lsem, bar_send, bar_recv, s_recv,
):
    me = lax.axis_index("row")
    g = lax.axis_index("gz")
    barrier = pltpu.get_barrier_semaphore()
    loads = [
        pltpu.make_async_copy(w_hbm, w_v, lsem.at[0]),
        pltpu.make_async_copy(u_hbm, u_v, lsem.at[1]),
        pltpu.make_async_copy(v_hbm, v_v, lsem.at[2]),
        pltpu.make_async_copy(level_hbm, level_ref, lsem.at[3]),
        pltpu.make_async_copy(spacing_hbm, spacing_ref, lsem.at[4]),
        pltpu.make_async_copy(plane_hbm, plane_ref, lsem.at[5]),
        pltpu.make_async_copy(tw_hbm, tw_ref, lsem.at[6]),
        pltpu.make_async_copy(weights_hbm, weights_ref, lsem.at[7]),
        pltpu.make_async_copy(weights_t_hbm, weights_t, lsem.at[8]),
    ]
    for load in loads:
        load.start()

    def greet_row(d, carry):
        pl.semaphore_signal(
            barrier, inc=1, device_id={"row": lax.rem(me + d, ROW)}, device_id_type=MESH
        )
        return carry

    def greet_gz(d, carry):
        pl.semaphore_signal(
            barrier, inc=1, device_id={"gz": lax.rem(g + d, GZ)}, device_id_type=MESH
        )
        return carry

    lax.fori_loop(1, ROW, greet_row, 0)
    lax.fori_loop(1, GZ, greet_gz, 0)

    def row_send(src, dst, k, t):
        return pltpu.make_async_remote_copy(
            src, dst, bar_send.at[k], bar_recv.at[k], device_id={"row": t}, device_id_type=MESH
        )

    def gz_send(src, dst, k, t):
        return pltpu.make_async_remote_copy(
            src, dst, bar_send.at[k], bar_recv.at[k], device_id={"gz": t}, device_id_type=MESH
        )

    for load in loads[3:]:
        load.wait()

    my_y, my_x, my_core = me // 8, lax.rem(me // 2, 4), lax.rem(me, 2)

    def partner(i):
        y = lax.rem(my_y + far_first(i // 8), 4)
        x = lax.rem(my_x + far_first(lax.rem(i // 2, 4)), 4)
        core = lax.rem(my_core + 1 + lax.rem(i, 2), 2)
        return (y * 4 + x) * 2 + core

    level = level_ref[...]
    width = jnp.zeros((GZ, DEPTH), f32)
    for n in range(64):
        width = jnp.where(level == n, spacing_ref[n], width)
    lane = lax.broadcasted_iota(jnp.int32, (GZ, DEPTH), 1)
    block = lax.broadcasted_iota(jnp.int32, (GZ, DEPTH), 0)
    shift_up = pltpu.roll(width, 1, 1)
    previous = jnp.where(lane == 0, pltpu.roll(shift_up, 1, 0), shift_up)
    shift_down = pltpu.roll(width, DEPTH - 1, 1)
    following = jnp.where(lane == DEPTH - 1, pltpu.roll(shift_down, GZ - 1, 0), shift_down)
    lower = 1.0 / (0.5 * (previous + width) * width)
    upper = 1.0 / (0.5 * (width + following) * width)
    lower = jnp.where((lane == 0) & (block == 0), 0.0, lower)
    upper = jnp.where((lane == DEPTH - 1) & (block == GZ - 1), 0.0, upper)
    band[0] = lower
    band[1] = upper
    band[2] = -(lower + upper)
    band[3] = 1.0 / width
    for n in range(3):
        row_n = jnp.broadcast_to(band[n, pl.ds(g, 1), :], (DEPTH, DEPTH))
        bmat[n] = row_n.T

    loads[0].wait()
    pick = (lax.broadcasted_iota(jnp.int32, (16, DEPTH), 1) == DEPTH - 1).astype(f32).astype(bf16)
    for n in range(2):
        column = lax.dot_general(
            pick,
            w_v[n].reshape(1024, DEPTH),
            (((1,), (1,)), ((), ())),
            preferred_element_type=f32,
        )
        halo_out[:, n * 1024 : (n + 1) * 1024] = column[0:1, :]
    loads[1].wait()
    loads[2].wait()
    pl.semaphore_wait(barrier, ROW - 1 + GZ - 1)

    above = lax.rem(g + 1, GZ)
    halo_copy = gz_send(halo_out, halo_in, 0, above)
    halo_copy.start()

    def send_u(i, carry):
        t = partner(i)
        row_send(u_v.at[:, t], recv_u.at[:, me], 1, t).start()
        return carry

    lax.fori_loop(0, ROW - 1, send_u, 0)
    recv_u[:, pl.ds(me, 1)] = u_v[:, pl.ds(me, 1)]

    halo_copy.wait()
    has_below = jnp.where(g > 0, 1.0, 0.0)
    first_lane = (lax.broadcasted_iota(jnp.int32, (8, DEPTH), 1) == 0).astype(f32)
    first_row = (lax.broadcasted_iota(jnp.int32, (8, DEPTH), 0) == 0).astype(f32)
    spot = (first_lane * first_row * has_below).astype(bf16)
    for n in range(2):
        wide = jnp.broadcast_to(halo_in[:, n * 1024 : (n + 1) * 1024], (8, 1024)).astype(bf16)
        halo_cols[n] = lax.dot_general(
            wide, spot, (((0,), (0,)), ((), ())), preferred_element_type=f32
        ).reshape(32, 32, DEPTH)
    inv_width = band[3, pl.ds(g, 1), :]
    lane32 = lax.broadcasted_iota(jnp.int32, (32, DEPTH), 1)

    def make_source(t):
        wave = plane_ref[t].astype(f32) * wave_unit
        slopes = []
        for n in range(2):
            upward = w_v[n, t].astype(f32)
            below = jnp.where(lane32 == 0, halo_cols[n, t], pltpu.roll(upward, 1, 1))
            slopes.append((upward - below) * inv_width)
        s_v[0, t] = (-wave * v_v[1, t].astype(f32) + slopes[0]).astype(bf16)
        s_v[1, t] = (wave * v_v[0, t].astype(f32) + slopes[1]).astype(bf16)

    def send_s(t):
        pltpu.make_async_remote_copy(
            s_v.at[:, t],
            recv_s.at[:, me],
            bar_send.at[2],
            s_recv.at[me // 4],
            device_id={"row": t},
            device_id_type=MESH,
        ).start()

    make_source(partner(0))

    def source_step(i, carry):
        make_source(partner(i))
        send_s(partner(i - 1))
        return carry

    lax.fori_loop(1, ROW - 1, source_step, 0)
    make_source(me)
    send_s(partner(ROW - 2))
    recv_s[:, pl.ds(me, 1)] = s_v[:, pl.ds(me, 1)]

    outer = lax.broadcasted_iota(jnp.int32, (RADIX, 128), 0)
    inner = lax.broadcasted_iota(jnp.int32, (RADIX, 128), 1)
    mode = 8 * inner + outer
    mode = jnp.where(mode >= 512, mode - 1024, mode)
    wave_x = mode.astype(f32) * (full_turn / 1024.0)
    own_wave = plane_ref[me].astype(f32) * wave_unit
    wave_sq = wave_x * wave_x + own_wave * own_wave
    kx_s[...] = wave_x

    def coef(n, z):
        return jnp.broadcast_to(bmat[n, pl.ds(z, 1), :], (RADIX, 128))

    def factor(j, carry):
        top, bottom, v_top, w_bottom = carry
        z = j
        lo, up = coef(0, z), coef(1, z)
        inv = 1.0 / ((coef(2, z) - wave_sq) - lo * top)
        fe = lo * inv
        top = up * inv
        inv_s[z] = inv
        fe_s[z] = fe
        bc_s[z] = top
        v_top = -fe * v_top
        vs_s[pl.ds(pl.multiple_of(z * 8, 8), 8), :] = v_top
        z = DEPTH - 1 - j
        lo, up = coef(0, z), coef(1, z)
        inv = 1.0 / ((coef(2, z) - wave_sq) - up * bottom)
        fe = up * inv
        bottom = lo * inv
        inv_s[z] = inv
        fe_s[z] = fe
        bc_s[z] = bottom
        w_bottom = -fe * w_bottom
        ws_s[pl.ds(pl.multiple_of(z * 8, 8), 8), :] = w_bottom
        return top, bottom, v_top, w_bottom

    zero = jnp.zeros((RADIX, 128), f32)
    one = jnp.ones((RADIX, 128), f32)
    top, bottom, v_top, w_bottom = lax.fori_loop(0, HALF, factor, (zero, zero, one, one))
    inv_det = 1.0 / (1.0 - top * bottom)

    def at(z):
        return pl.ds(pl.multiple_of(z * 8, 8), 8)

    v_lo = v_top * inv_det
    v_hi = -bottom * v_lo
    w_hi = w_bottom * inv_det
    w_lo = -top * w_hi
    vs_s[at(HALF - 1), :] = v_lo
    vs_s[at(HALF), :] = v_hi
    ws_s[at(HALF - 1), :] = w_lo
    ws_s[at(HALF), :] = w_hi

    def spread(j, carry):
        v_lo, v_hi, w_lo, w_hi = carry
        z = HALF - 1 - j
        bc = bc_s[z]
        v_lo = vs_s[at(z), :] - bc * v_lo
        w_lo = -bc * w_lo
        vs_s[at(z), :] = v_lo
        ws_s[at(z), :] = w_lo
        z = HALF + j
        bc = bc_s[z]
        v_hi = -bc * v_hi
        w_hi = ws_s[at(z), :] - bc * w_hi
        vs_s[at(z), :] = v_hi
        ws_s[at(z), :] = w_hi
        return v_lo, v_hi, w_lo, w_hi

    v_lo, v_hi, w_lo, w_hi = lax.fori_loop(1, HALF, spread, (v_lo, v_hi, w_lo, w_hi))
    sp_send[0] = v_lo
    sp_send[1] = v_hi
    sp_send[2] = w_lo
    sp_send[3] = w_hi
    sp_all[pl.ds(g, 1)] = sp_send[...][None]
    for c in range(RADIX):
        vt_s[c] = vs_s[pl.ds(c, DEPTH, stride=8), :]
        wt_s[c] = ws_s[pl.ds(c, DEPTH, stride=8), :]

    def send_sp(d, carry):
        t = lax.rem(g + d, GZ)
        gz_send(sp_send, sp_all.at[g], 3, t).start()
        return carry

    lax.fori_loop(1, GZ, send_sp, 0)

    def forward(recv, ready, finish):
        def flip(i, carry):
            y = lax.rem(my_y + 4 - far_first(i), 4)
            for n in range(2):
                ready(2 * y + n)
            for n in range(2):
                for h in range(2):
                    a = 2 * y + h
                    q_t[n, a] = recv[n, pl.ds(4 * a, 4)].reshape(128, 128).T
            return carry

        lax.fori_loop(0, 4, flip, 0)

        def mix(i, carry):
            rows = pl.ds(pl.multiple_of(16 * i, 16), 16)
            xr = [q_t[0, a, rows, :].astype(f32) for a in range(RADIX)]
            xi = [q_t[1, a, rows, :].astype(f32) for a in range(RADIX)]
            for c, (re, im) in enumerate(butterfly(xr, xi)):
                re, im = twisted(re, im, tw_ref, c)
                put_split(y_s, c, rows, re, im)
            return carry

        lax.fori_loop(0, DEPTH // 16, mix, 0)
        for c in range(0, RADIX, 2):
            finish(c, product(c))

    def product(c):
        rows = y_s[c : c + 2].reshape(2 * DEPTH, 512)
        return jnp.dot(rows, weights_ref[0:512, :], preferred_element_type=f32) + jnp.dot(
            rows[:, 0:256], weights_ref[512:768, :], preferred_element_type=f32
        )

    def keep_along(c, acc):
        for n in range(2):
            kx = kx_s[c + n : c + n + 1, :]
            own = acc[n * DEPTH : (n + 1) * DEPTH]
            part[c + n, :, 0:128] = -kx * own[:, 128:256]
            part[c + n, :, 128:256] = kx * own[:, 0:128]

    def keep_rhs(c, acc):
        for n in range(2):
            total = acc[n * DEPTH : (n + 1) * DEPTH] + part[c + n]
            rhs[0, pl.ds(c + n, DEPTH, stride=8), :] = total[:, 0:128]
            rhs[1, pl.ds(c + n, DEPTH, stride=8), :] = total[:, 128:256]

    def row_wait(ref, k):
        row_send(ref.at[:, 0 : ROW - 1], ref.at[:, 0 : ROW - 1], k, me).wait_recv()

    def turn_table(c, carry):
        tc_s[c] = jnp.broadcast_to(tw_ref[pl.ds(c, 1), :], (128, 128)).T
        ts_s[c] = jnp.broadcast_to(tw_ref[pl.ds(8 + c, 1), :], (128, 128)).T
        return carry

    lax.fori_loop(1, RADIX, turn_table, 0)
    row_wait(recv_u, 1)
    forward(recv_u, lambda a: None, keep_along)

    gz_send(sp_all.at[0 : GZ - 1], sp_all.at[0 : GZ - 1], 3, g).wait_recv()
    beta = zero
    for b in range(GZ):
        v_first, v_last, w_first, w_last = (sp_all[b, n] for n in range(4))
        inv = 1.0 / (1.0 - v_first * beta)
        gamma = v_last * beta * inv
        red[0, b] = gamma
        red[1, b] = v_last + gamma * v_first
        red[2, b] = inv
        red[3, b] = inv * v_first
        red[4, b] = inv * w_first
        beta = w_last + gamma * w_first
        red[5, b] = beta

    def s_ready(a):
        def wait_for(count):
            view = recv_s.at[:, 0:count]
            pltpu.make_async_remote_copy(
                view, view, bar_send.at[2], s_recv.at[a], device_id={"row": me}, device_id_type=MESH
            ).wait_recv()

        @pl.when(a == me // 4)
        def _():
            wait_for(3)

        @pl.when(a != me // 4)
        def _():
            wait_for(4)

    forward(recv_s, s_ready, keep_rhs)

    def down(i, carry):
        for h in range(8):
            j = 8 * i + h
            out = []
            for z, pair in ((j, carry[0:2]), (DEPTH - 1 - j, carry[2:4])):
                inv, fe = inv_s[z], fe_s[z]
                for n in range(2):
                    value = rhs[n, at(z), :] * inv - fe * pair[n]
                    rhs[n, at(z), :] = value
                    out.append(value)
            carry = tuple(out)
        return carry

    low_re, low_im, high_re, high_im = lax.fori_loop(0, HALF // 8, down, (zero,) * 4)
    bc_low, bc_high = bc_s[HALF - 1], bc_s[HALF]
    inv_det = 1.0 / (1.0 - bc_low * bc_high)
    low_re = (low_re - bc_low * high_re) * inv_det
    low_im = (low_im - bc_low * high_im) * inv_det
    high_re = high_re - bc_high * low_re
    high_im = high_im - bc_high * low_im
    rhs[0, at(HALF - 1), :] = low_re
    rhs[1, at(HALF - 1), :] = low_im
    rhs[0, at(HALF), :] = high_re
    rhs[1, at(HALF), :] = high_im

    def up_again(i, carry):
        for h in range(7):
            j = 7 * i + h + 1
            out = []
            for z, pair in ((HALF - 1 - j, carry[0:2]), (HALF + j, carry[2:4])):
                bc = bc_s[z]
                for n in range(2):
                    value = rhs[n, at(z), :] - bc * pair[n]
                    rhs[n, at(z), :] = value
                    out.append(value)
            carry = tuple(out)
        return carry

    low_re, low_im, high_re, high_im = lax.fori_loop(
        0, (HALF - 1) // 7, up_again, (low_re, low_im, high_re, high_im)
    )
    ex_send[0] = low_re
    ex_send[1] = low_im
    ex_send[2] = high_re
    ex_send[3] = high_im
    ex_all[pl.ds(g, 1)] = ex_send[...][None]

    for d in (4, 3, 5, 2, 6, 1, 7):
        gz_send(ex_send, ex_all.at[g], 4, lax.rem(g + d, GZ)).start()
    for c in range(RADIX):
        for n in range(2):
            yt_s[n, c] = rhs[n, pl.ds(c, DEPTH, stride=8), :]
    gz_send(ex_all.at[0 : GZ - 1], ex_all.at[0 : GZ - 1], 4, g).wait_recv()

    for n in range(2):
        alpha = zero
        befores = []
        for b in range(GZ):
            befores.append(alpha)
            alpha = (
                ex_all[b, 2 + n] + red[0, b] * ex_all[b, n] + red[1, b] * alpha
            )
        first = zero
        edge[1, n, GZ - 1] = zero
        for b in range(GZ - 1, -1, -1):
            first = red[2, b] * ex_all[b, n] + red[3, b] * befores[b] + red[4, b] * first
            if b > 0:
                edge[1, n, b - 1] = first
                edge[0, n, b] = befores[b] + red[5, b - 1] * first
        edge[0, n, 0] = zero

    from_below = [edge[0, n, g] for n in range(2)]
    from_above = [edge[1, n, g] for n in range(2)]

    def correct(i, carry):
        rows = pl.ds(pl.multiple_of(16 * i, 16), 16)
        for c in range(RADIX):
            v_c, w_c = vt_s[c, rows, :], wt_s[c, rows, :]
            full = [
                yt_s[n, c, rows, :]
                + v_c * from_below[n][c : c + 1, :]
                + w_c * from_above[n][c : c + 1, :]
                for n in range(2)
            ]
            put_split(y_s, c, rows, full[1], full[0])
        return carry

    lax.fori_loop(0, DEPTH // 16, correct, 0)
    for c in range(0, RADIX, 2):
        rows = y_s[c : c + 2].reshape(2 * DEPTH, 512)
        across = (((1,), (1,)), ((), ()))
        acc = lax.dot_general(
            weights_t[:, 0:512], rows, across, preferred_element_type=f32
        ) + lax.dot_general(
            weights_t[:, 512:768], rows[:, 0:256], across, preferred_element_type=f32
        )
        for n in range(2):
            for h in range(2):
                part_t[n, c + h] = acc[n * 128 : (n + 1) * 128, h * DEPTH : (h + 1) * DEPTH]

    def unmix(q, carry):
        for h in range(2):
            rows = pl.ds(pl.multiple_of(32 * q + 16 * h, 16), 16)
            turned = []
            for c in range(RADIX):
                re, im = part_t[0, c, rows, :], part_t[1, c, rows, :]
                if c > 0:
                    cos, sin = tc_s[c, rows, :], ts_s[c, rows, :]
                    re, im = re * cos + im * sin, im * cos - re * sin
                turned.append((re, im))
            mixed = butterfly([t[0] for t in turned], [t[1] for t in turned])
            for j, (first, second) in enumerate(mixed):
                out_v[0, 4 * j + q, 16 * h : 16 * h + 16, :] = second.astype(bf16)
                out_v[1, 4 * j + q, 16 * h : 16 * h + 16, :] = first.astype(bf16)
        return carry

    def give(q, carry):
        for i in range(RADIX):
            y = lax.rem(my_y + (2, 3, 1, 0)[i // 2], 4)
            t = 8 * y + 4 * (i % 2) + q

            @pl.when(t != me)
            def _():
                row_send(out_v.at[:, t], out_ref.at[:, me], 5, t).start()

        return carry

    unmix(0, 0)

    def unmix_step(q, carry):
        unmix(q, carry)
        give(q - 1, carry)
        return carry

    lax.fori_loop(1, 4, unmix_step, 0)
    own = pltpu.make_async_copy(out_v.at[:, me], out_ref.at[:, me], lsem.at[0])
    own.start()
    give(3, 0)
    own.wait()
    row_wait(out_ref, 5)
    for k, ref in ((1, u_v), (2, s_v), (5, out_v)):
        row_send(ref.at[:, 0 : ROW - 1], ref.at[:, 0 : ROW - 1], k, me).wait_send()
    for k, ref in ((3, sp_all), (4, ex_all)):
        gz_send(ref.at[0 : GZ - 1], ref.at[0 : GZ - 1], k, g).wait_send()


def on_device(velocity_x, velocity_y, velocity_z, spacing, level_index, plane_index):
    weights, twiddle = tables()
    block = (2, 32, 32, 128)
    line = (DEPTH, RADIX, 128)
    flat = (DEPTH * RADIX, 128)
    tile = (RADIX, DEPTH, 128)
    pressure = pl.pallas_call(
        kernel,
        out_shape=jax.ShapeDtypeStruct(block, bf16),
        in_specs=[
            pl.BlockSpec(memory_space=pltpu.HBM),
        ]
        * 9,
        out_specs=pl.BlockSpec(memory_space=pltpu.HBM),
        scratch_shapes=[
            pltpu.SMEM((64,), f32),
            pltpu.VMEM((8, 128), jnp.int32),
            pltpu.SMEM((32,), jnp.int32),
            pltpu.VMEM((768, 256), bf16),
            pltpu.VMEM((256, 768), bf16),
            pltpu.VMEM((16, 128), f32),
            pltpu.VMEM(block, bf16),
            pltpu.VMEM(block, bf16),
            pltpu.VMEM(block, bf16),
            pltpu.VMEM(block, bf16),
            pltpu.VMEM(block, bf16),
            pltpu.VMEM(block, bf16),
            pltpu.VMEM(block, bf16),
            pltpu.VMEM((1, 2048), f32),
            pltpu.VMEM((1, 2048), f32),
            pltpu.VMEM(block, f32),
            pltpu.VMEM((4, 8, 128), f32),
            pltpu.VMEM((3, 128, 128), f32),
            pltpu.VMEM(line, f32),
            pltpu.VMEM(line, f32),
            pltpu.VMEM(line, f32),
            pltpu.VMEM(flat, f32),
            pltpu.VMEM(flat, f32),
            pltpu.VMEM(tile, f32),
            pltpu.VMEM(tile, f32),
            pltpu.VMEM((2,) + tile, f32),
            pltpu.VMEM((2,) + flat, f32),
            pltpu.VMEM((RADIX, DEPTH, 256), f32),
            pltpu.VMEM((2,) + tile, f32),
            pltpu.VMEM(tile, f32),
            pltpu.VMEM(tile, f32),
            pltpu.VMEM((2, RADIX, 128, 128), bf16),
            pltpu.VMEM((RADIX, DEPTH, 512), bf16),
            pltpu.VMEM((RADIX, 128), f32),
            pltpu.VMEM((GZ, 4, RADIX, 128), f32),
            pltpu.VMEM((GZ, 4, RADIX, 128), f32),
            pltpu.VMEM((4, RADIX, 128), f32),
            pltpu.VMEM((4, RADIX, 128), f32),
            pltpu.VMEM((6, GZ, RADIX, 128), f32),
            pltpu.VMEM((2, 2, GZ, RADIX, 128), f32),
            pltpu.SemaphoreType.DMA((9,)),
            pltpu.SemaphoreType.DMA((6,)),
            pltpu.SemaphoreType.DMA((6,)),
            pltpu.SemaphoreType.DMA((8,)),
        ],
        compiler_params=pltpu.CompilerParams(
            collective_id=0, has_side_effects=True, vmem_limit_bytes=67043328
        ),
        name="poisson",
    )(
        velocity_x,
        velocity_y,
        velocity_z,
        spacing,
        level_index.reshape(8, 128),
        plane_index,
        jnp.asarray(weights),
        jnp.asarray(weights.T),
        jnp.asarray(twiddle),
    )
    return pressure.astype(f32) * (1.0 / 1024.0)


def solution(mesh):
    placed = (
        P(None, None, "row", "gz"),
        P(None, None, "row", "gz"),
        P(None, None, "row", "gz"),
        P(),
        P(),
        P(),
    )
    return jax.shard_map(
        on_device, mesh=mesh, in_specs=placed, out_specs=P(None, None, "row", "gz"), check_vma=False
    )
```

```python
import math

import jax
import jax.numpy as jnp
import numpy as np
from jax import lax
from jax.experimental import pallas as pl
from jax.experimental.pallas import tpu as pltpu
from jax.sharding import PartitionSpec as P

MESH = pl.DeviceIdType.MESH
f32 = jnp.float32
bf16 = jnp.bfloat16
full_turn = 2.0 * math.pi
wave_unit = 2.0 * math.pi / 2048.0
ROW = 32
GZ = 8
DEPTH = 128
RADIX = 8
HALF = DEPTH // 2
ROOT_HALF = math.sqrt(0.5)


def tables():
    idx = np.arange(128)
    angle = 2.0 * np.pi / 128.0 * ((idx[:, None] * idx[None, :]) % 128)
    c, s = np.cos(angle), np.sin(angle)
    w = np.block([[c, -s], [s, c]]).astype(np.float32)
    hi = w.astype(jnp.bfloat16)
    lo = (w - hi.astype(np.float32)).astype(jnp.bfloat16)
    weights = np.concatenate([hi, hi, lo], axis=0)
    twist = 2.0 * np.pi / 1024.0 * (np.arange(8)[:, None] * idx[None, :])
    twiddle = np.concatenate([np.cos(twist), np.sin(twist)], axis=0).astype(np.float32)
    return weights, twiddle


def butterfly(xr, xi):
    def add(p, q):
        return (p[0] + q[0], p[1] + q[1])

    def sub(p, q):
        return (p[0] - q[0], p[1] - q[1])

    def turn(p):
        return (p[1], -p[0])

    x = list(zip(xr, xi))
    a0, a1 = add(x[0], x[4]), sub(x[0], x[4])
    a2, a3 = add(x[2], x[6]), turn(sub(x[2], x[6]))
    b0, b1 = add(x[1], x[5]), sub(x[1], x[5])
    b2, b3 = add(x[3], x[7]), turn(sub(x[3], x[7]))
    e = [add(a0, a2), add(a1, a3), sub(a0, a2), sub(a1, a3)]
    o = [add(b0, b2), add(b1, b3), sub(b0, b2), sub(b1, b3)]
    o1 = ((o[1][0] + o[1][1]) * ROOT_HALF, (o[1][1] - o[1][0]) * ROOT_HALF)
    o2 = turn(o[2])
    o3 = ((o[3][1] - o[3][0]) * ROOT_HALF, -(o[3][0] + o[3][1]) * ROOT_HALF)
    odd = [o[0], o1, o2, o3]
    return [add(e[k], odd[k]) for k in range(4)] + [sub(e[k], odd[k]) for k in range(4)]


def twisted(re, im, tw_ref, c):
    if c == 0:
        return re, im
    cos = tw_ref[c : c + 1, :]
    sin = tw_ref[8 + c : 9 + c, :]
    return re * cos + im * sin, im * cos - re * sin


def put_split(y_ref, c, rows, re, im):
    re_hi = re.astype(bf16)
    im_hi = im.astype(bf16)
    y_ref[c, rows, 0:128] = re_hi
    y_ref[c, rows, 128:256] = im_hi
    y_ref[c, rows, 256:384] = (re - re_hi.astype(f32)).astype(bf16)
    y_ref[c, rows, 384:512] = (im - im_hi.astype(f32)).astype(bf16)


FAR_FIRST = (2, 3, 1, 0)


def kernel(
    u_hbm, v_hbm, w_hbm, spacing_hbm, level_hbm, plane_hbm, weights_hbm, weights_t_hbm, tw_hbm,
    out_ref,
    spacing_ref, level_ref, plane_ref, weights_ref, weights_t, tw_ref,
    u_v, v_v, w_v, s_v, recv_u, recv_s, out_v, halo_out, halo_in, halo_cols, band, bmat,
    inv_s, fe_s, bc_s, vs_s, ws_s, vt_s, wt_s, yt_s, rhs, part, part_t, tc_s, ts_s, q_t, y_s, kx_s,
    sp_all, ex_all, sp_send, ex_send, red, edge,
    lsem, bar_send, bar_recv, s_recv,
):
    me = lax.axis_index("row")
    g = lax.axis_index("gz")
    my_y, my_x, my_core = me // 8, lax.rem(me // 2, 4), lax.rem(me, 2)
    ys = [lax.rem(my_y + d, 4) * 8 for d in FAR_FIRST]
    ends = [
        lax.rem(my_x + d, 4) * 2 + lax.rem(my_core + c, 2) for d in FAR_FIRST for c in (1, 0)
    ]
    barrier = pltpu.get_barrier_semaphore()

    def greet(device):
        pl.semaphore_signal(barrier, inc=1, device_id=device, device_id_type=MESH)

    for d in (4, 3, 5):
        greet({"gz": lax.rem(g + d, GZ)})
    for i in range(ROW - 1):
        greet({"row": ys[i // 8] + ends[i % 8]})
    for d in (2, 6, 1, 7):
        greet({"gz": lax.rem(g + d, GZ)})
    loads = [
        pltpu.make_async_copy(w_hbm, w_v, lsem.at[0]),
        pltpu.make_async_copy(u_hbm, u_v, lsem.at[1]),
        pltpu.make_async_copy(v_hbm, v_v, lsem.at[2]),
        pltpu.make_async_copy(level_hbm, level_ref, lsem.at[3]),
        pltpu.make_async_copy(spacing_hbm, spacing_ref, lsem.at[4]),
        pltpu.make_async_copy(plane_hbm, plane_ref, lsem.at[5]),
        pltpu.make_async_copy(tw_hbm, tw_ref, lsem.at[6]),
        pltpu.make_async_copy(weights_hbm, weights_ref, lsem.at[7]),
        pltpu.make_async_copy(weights_t_hbm, weights_t, lsem.at[8]),
    ]
    for load in loads:
        load.start()

    def row_send(src, dst, k, t):
        return pltpu.make_async_remote_copy(
            src, dst, bar_send.at[k], bar_recv.at[k], device_id={"row": t}, device_id_type=MESH
        )

    def gz_send(src, dst, k, t):
        return pltpu.make_async_remote_copy(
            src, dst, bar_send.at[k], bar_recv.at[k], device_id={"gz": t}, device_id_type=MESH
        )

    for load in loads[3:]:
        load.wait()

    level = level_ref[...]
    width = jnp.zeros((GZ, DEPTH), f32)
    for n in range(64):
        width = jnp.where(level == n, spacing_ref[n], width)
    lane = lax.broadcasted_iota(jnp.int32, (GZ, DEPTH), 1)
    block = lax.broadcasted_iota(jnp.int32, (GZ, DEPTH), 0)
    shift_up = pltpu.roll(width, 1, 1)
    previous = jnp.where(lane == 0, pltpu.roll(shift_up, 1, 0), shift_up)
    shift_down = pltpu.roll(width, DEPTH - 1, 1)
    following = jnp.where(lane == DEPTH - 1, pltpu.roll(shift_down, GZ - 1, 0), shift_down)
    lower = 1.0 / (0.5 * (previous + width) * width)
    upper = 1.0 / (0.5 * (width + following) * width)
    lower = jnp.where((lane == 0) & (block == 0), 0.0, lower)
    upper = jnp.where((lane == DEPTH - 1) & (block == GZ - 1), 0.0, upper)
    band[0] = lower
    band[1] = upper
    band[2] = -(lower + upper)
    band[3] = 1.0 / width
    for n in range(3):
        row_n = jnp.broadcast_to(band[n, pl.ds(g, 1), :], (DEPTH, DEPTH))
        bmat[n] = row_n.T

    loads[0].wait()
    pick = (lax.broadcasted_iota(jnp.int32, (16, DEPTH), 1) == DEPTH - 1).astype(f32).astype(bf16)
    for n in range(2):
        column = lax.dot_general(
            pick,
            w_v[n].reshape(1024, DEPTH),
            (((1,), (1,)), ((), ())),
            preferred_element_type=f32,
        )
        halo_out[:, n * 1024 : (n + 1) * 1024] = column[0:1, :]
    loads[1].wait()
    loads[2].wait()
    pl.semaphore_wait(barrier, ROW - 1 + GZ - 1)

    above = lax.rem(g + 1, GZ)
    halo_copy = gz_send(halo_out, halo_in, 0, above)
    halo_copy.start()

    for i in range(ROW - 1):
        t = ys[i // 8] + ends[i % 8]
        row_send(u_v.at[:, t], recv_u.at[:, me], 1, t).start()
    recv_u[:, pl.ds(me, 1)] = u_v[:, pl.ds(me, 1)]

    halo_copy.wait()
    has_below = jnp.where(g > 0, 1.0, 0.0)
    first_lane = (lax.broadcasted_iota(jnp.int32, (8, DEPTH), 1) == 0).astype(f32)
    first_row = (lax.broadcasted_iota(jnp.int32, (8, DEPTH), 0) == 0).astype(f32)
    spot = (first_lane * first_row * has_below).astype(bf16)
    for n in range(2):
        wide = jnp.broadcast_to(halo_in[:, n * 1024 : (n + 1) * 1024], (8, 1024)).astype(bf16)
        halo_cols[n] = lax.dot_general(
            wide, spot, (((0,), (0,)), ((), ())), preferred_element_type=f32
        ).reshape(32, 32, DEPTH)
    inv_width = band[3, pl.ds(g, 1), :]
    lane32 = lax.broadcasted_iota(jnp.int32, (32, DEPTH), 1)

    def make_source(t):
        wave = plane_ref[t].astype(f32) * wave_unit
        slopes = []
        for n in range(2):
            upward = w_v[n, t].astype(f32)
            below = jnp.where(lane32 == 0, halo_cols[n, t], pltpu.roll(upward, 1, 1))
            slopes.append((upward - below) * inv_width)
        s_v[0, t] = (-wave * v_v[1, t].astype(f32) + slopes[0]).astype(bf16)
        s_v[1, t] = (wave * v_v[0, t].astype(f32) + slopes[1]).astype(bf16)

    def send_s(t):
        pltpu.make_async_remote_copy(
            s_v.at[:, t],
            recv_s.at[:, me],
            bar_send.at[2],
            s_recv.at[me // 4],
            device_id={"row": t},
            device_id_type=MESH,
        ).start()

    def source_step(i, carry):
        base = lax.rem(my_y + lax.rem(2 + i + (i // 2) * (1 + 2 * lax.rem(i, 2)), 4), 4) * 8
        make_source(base + ends[0])
        for n in range(1, 8):
            make_source(base + ends[n])
            send_s(base + ends[n - 1])

        @pl.when(i < 3)
        def _():
            send_s(base + ends[7])

        return carry

    lax.fori_loop(0, 4, source_step, 0)
    recv_s[:, pl.ds(me, 1)] = s_v[:, pl.ds(me, 1)]

    outer = lax.broadcasted_iota(jnp.int32, (RADIX, 128), 0)
    inner = lax.broadcasted_iota(jnp.int32, (RADIX, 128), 1)
    mode = 8 * inner + outer
    mode = jnp.where(mode >= 512, mode - 1024, mode)
    wave_x = mode.astype(f32) * (full_turn / 1024.0)
    own_wave = plane_ref[me].astype(f32) * wave_unit
    wave_sq = wave_x * wave_x + own_wave * own_wave
    kx_s[...] = wave_x

    def coef(n, z):
        return jnp.broadcast_to(bmat[n, pl.ds(z, 1), :], (RADIX, 128))

    def factor(j, carry):
        top, bottom, v_top, w_bottom = carry
        z = j
        lo, up = coef(0, z), coef(1, z)
        inv = 1.0 / ((coef(2, z) - wave_sq) - lo * top)
        fe = lo * inv
        top = up * inv
        inv_s[z] = inv
        fe_s[z] = fe
        bc_s[z] = top
        v_top = -fe * v_top
        vs_s[pl.ds(pl.multiple_of(z * 8, 8), 8), :] = v_top
        z = DEPTH - 1 - j
        lo, up = coef(0, z), coef(1, z)
        inv = 1.0 / ((coef(2, z) - wave_sq) - up * bottom)
        fe = up * inv
        bottom = lo * inv
        inv_s[z] = inv
        fe_s[z] = fe
        bc_s[z] = bottom
        w_bottom = -fe * w_bottom
        ws_s[pl.ds(pl.multiple_of(z * 8, 8), 8), :] = w_bottom
        return top, bottom, v_top, w_bottom

    zero = jnp.zeros((RADIX, 128), f32)
    one = jnp.ones((RADIX, 128), f32)
    top, bottom, v_top, w_bottom = lax.fori_loop(0, HALF, factor, (zero, zero, one, one))
    inv_det = 1.0 / (1.0 - top * bottom)

    def at(z):
        return pl.ds(pl.multiple_of(z * 8, 8), 8)

    v_lo = v_top * inv_det
    v_hi = -bottom * v_lo
    w_hi = w_bottom * inv_det
    w_lo = -top * w_hi
    vs_s[at(HALF - 1), :] = v_lo
    vs_s[at(HALF), :] = v_hi
    ws_s[at(HALF - 1), :] = w_lo
    ws_s[at(HALF), :] = w_hi

    def spread(j, carry):
        v_lo, v_hi, w_lo, w_hi = carry
        z = HALF - 1 - j
        bc = bc_s[z]
        v_lo = vs_s[at(z), :] - bc * v_lo
        w_lo = -bc * w_lo
        vs_s[at(z), :] = v_lo
        ws_s[at(z), :] = w_lo
        z = HALF + j
        bc = bc_s[z]
        v_hi = -bc * v_hi
        w_hi = ws_s[at(z), :] - bc * w_hi
        vs_s[at(z), :] = v_hi
        ws_s[at(z), :] = w_hi
        return v_lo, v_hi, w_lo, w_hi

    v_lo, v_hi, w_lo, w_hi = lax.fori_loop(1, HALF, spread, (v_lo, v_hi, w_lo, w_hi))
    sp_send[0] = v_lo
    sp_send[1] = v_hi
    sp_send[2] = w_lo
    sp_send[3] = w_hi
    sp_all[pl.ds(g, 1)] = sp_send[...][None]
    for c in range(RADIX):
        vt_s[c] = vs_s[pl.ds(c, DEPTH, stride=8), :]
        wt_s[c] = ws_s[pl.ds(c, DEPTH, stride=8), :]

    def send_sp(d, carry):
        t = lax.rem(g + d, GZ)
        gz_send(sp_send, sp_all.at[g], 3, t).start()
        return carry

    lax.fori_loop(1, GZ, send_sp, 0)

    def forward(recv, ready, finish):
        def flip(i, carry):
            y = lax.rem(my_y + 4 - lax.rem(2 + i + (i // 2) * (1 + 2 * lax.rem(i, 2)), 4), 4)
            for n in range(2):
                ready(2 * y + n)
            for n in range(2):
                for h in range(2):
                    a = 2 * y + h
                    q_t[n, a] = recv[n, pl.ds(4 * a, 4)].reshape(128, 128).T
            return carry

        lax.fori_loop(0, 4, flip, 0)

        for half in range(2):
            for i in range(4):
                rows = slice(64 * half + 16 * i, 64 * half + 16 * (i + 1))
                xr = [q_t[0, a, rows, :].astype(f32) for a in range(RADIX)]
                xi = [q_t[1, a, rows, :].astype(f32) for a in range(RADIX)]
                for c, (re, im) in enumerate(butterfly(xr, xi)):
                    re, im = twisted(re, im, tw_ref, c)
                    put_split(y_s, c, rows, re, im)
            for c in range(0, RADIX, 4):
                rows = y_s[c : c + 4, 64 * half : 64 * (half + 1), :].reshape(256, 512)
                acc = jnp.dot(
                    rows, weights_ref[0:512, :], preferred_element_type=f32
                ) + jnp.dot(rows[:, 0:256], weights_ref[512:768, :], preferred_element_type=f32)
                for n in range(4):
                    finish(c + n, half, acc[64 * n : 64 * (n + 1)])

    def keep_along(c, half, own):
        rows = slice(64 * half, 64 * (half + 1))
        kx = kx_s[c : c + 1, :]
        part[c, rows, 0:128] = -kx * own[:, 128:256]
        part[c, rows, 128:256] = kx * own[:, 0:128]

    def keep_rhs(c, half, own):
        total = own + part[c, 64 * half : 64 * (half + 1)]
        rhs[0, pl.ds(512 * half + c, 64, stride=8), :] = total[:, 0:128]
        rhs[1, pl.ds(512 * half + c, 64, stride=8), :] = total[:, 128:256]

    def row_wait(ref, k):
        row_send(ref.at[:, 0 : ROW - 1], ref.at[:, 0 : ROW - 1], k, me).wait_recv()

    def turn_table(c, carry):
        tc_s[c] = jnp.broadcast_to(tw_ref[pl.ds(c, 1), :], (128, 128)).T
        ts_s[c] = jnp.broadcast_to(tw_ref[pl.ds(8 + c, 1), :], (128, 128)).T
        return carry

    lax.fori_loop(1, RADIX, turn_table, 0)
    row_wait(recv_u, 1)
    forward(recv_u, lambda a: None, keep_along)

    gz_send(sp_all.at[0 : GZ - 1], sp_all.at[0 : GZ - 1], 3, g).wait_recv()
    beta = zero
    for b in range(GZ):
        v_first, v_last, w_first, w_last = (sp_all[b, n] for n in range(4))
        inv = 1.0 / (1.0 - v_first * beta)
        gamma = v_last * beta * inv
        red[0, b] = gamma
        red[1, b] = v_last + gamma * v_first
        red[2, b] = inv
        red[3, b] = inv * v_first
        red[4, b] = inv * w_first
        beta = w_last + gamma * w_first
        red[5, b] = beta

    def s_ready(a):
        def wait_for(count):
            view = recv_s.at[:, 0:count]
            pltpu.make_async_remote_copy(
                view, view, bar_send.at[2], s_recv.at[a], device_id={"row": me}, device_id_type=MESH
            ).wait_recv()

        @pl.when(a == me // 4)
        def _():
            wait_for(3)

        @pl.when(a != me // 4)
        def _():
            wait_for(4)

    forward(recv_s, s_ready, keep_rhs)

    def sweep(rows, factor_ref, scale_ref, before):
        for k in range(0, len(rows), 4):
            group = rows[k : k + 4]
            factors = [factor_ref[z] for z in group]
            products = [-factors[0]]
            for factor_z in factors[1:]:
                products.append(-factor_z * products[-1])
            after = []
            for n in range(2):
                partial = None
                for z, factor_z, product_z in zip(group, factors, products):
                    own = rhs[n, 8 * z : 8 * z + 8, :]
                    if scale_ref is not None:
                        own = own * scale_ref[z]
                    partial = own if partial is None else own - factor_z * partial
                    value = partial + product_z * before[n]
                    rhs[n, 8 * z : 8 * z + 8, :] = value
                after.append(value)
            before = after
            yield before

    def both(low_rows, high_rows, factor_ref, scale_ref, low, high):
        for low, high in zip(
            sweep(low_rows, factor_ref, scale_ref, low),
            sweep(high_rows, factor_ref, scale_ref, high),
        ):
            pass
        return low, high

    (low_re, low_im), (high_re, high_im) = both(
        range(HALF), range(DEPTH - 1, HALF - 1, -1), fe_s, inv_s, (zero, zero), (zero, zero)
    )
    bc_low, bc_high = bc_s[HALF - 1], bc_s[HALF]
    inv_det = 1.0 / (1.0 - bc_low * bc_high)
    low_re = (low_re - bc_low * high_re) * inv_det
    low_im = (low_im - bc_low * high_im) * inv_det
    high_re = high_re - bc_high * low_re
    high_im = high_im - bc_high * low_im
    rhs[0, at(HALF - 1), :] = low_re
    rhs[1, at(HALF - 1), :] = low_im
    rhs[0, at(HALF), :] = high_re
    rhs[1, at(HALF), :] = high_im

    (low_re, low_im), (high_re, high_im) = both(
        range(HALF - 2, -1, -1),
        range(HALF + 1, DEPTH),
        bc_s,
        None,
        (low_re, low_im),
        (high_re, high_im),
    )
    ex_send[0] = low_re
    ex_send[1] = low_im
    ex_send[2] = high_re
    ex_send[3] = high_im
    ex_all[pl.ds(g, 1)] = ex_send[...][None]

    for d in (4, 3, 5, 2, 6, 1, 7):
        gz_send(ex_send, ex_all.at[g], 4, lax.rem(g + d, GZ)).start()
    for c in range(RADIX):
        for n in range(2):
            yt_s[n, c] = rhs[n, pl.ds(c, DEPTH, stride=8), :]
    gz_send(ex_all.at[0 : GZ - 1], ex_all.at[0 : GZ - 1], 4, g).wait_recv()

    for n in range(2):
        alpha = zero
        befores = []
        for b in range(GZ):
            befores.append(alpha)
            alpha = (
                ex_all[b, 2 + n] + red[0, b] * ex_all[b, n] + red[1, b] * alpha
            )
        first = zero
        edge[1, n, GZ - 1] = zero
        for b in range(GZ - 1, -1, -1):
            first = red[2, b] * ex_all[b, n] + red[3, b] * befores[b] + red[4, b] * first
            if b > 0:
                edge[1, n, b - 1] = first
                edge[0, n, b] = befores[b] + red[5, b - 1] * first
        edge[0, n, 0] = zero

    from_below = [edge[0, n, g] for n in range(2)]
    from_above = [edge[1, n, g] for n in range(2)]

    across = (((1,), (1,)), ((), ()))
    for c in range(0, RADIX, 2):
        for h in range(2):
            for i in range(DEPTH // 16):
                rows = slice(16 * i, 16 * (i + 1))
                v_c, w_c = vt_s[c + h, rows, :], wt_s[c + h, rows, :]
                full = [
                    yt_s[n, c + h, rows, :]
                    + v_c * from_below[n][c + h : c + h + 1, :]
                    + w_c * from_above[n][c + h : c + h + 1, :]
                    for n in range(2)
                ]
                put_split(y_s, c + h, rows, full[1], full[0])
        rows = y_s[c : c + 2].reshape(2 * DEPTH, 512)
        acc = lax.dot_general(
            weights_t[:, 0:512], rows, across, preferred_element_type=f32
        ) + lax.dot_general(
            weights_t[:, 512:768], rows[:, 0:256], across, preferred_element_type=f32
        )
        for n in range(2):
            for h in range(2):
                part_t[n, c + h] = acc[n * 128 : (n + 1) * 128, h * DEPTH : (h + 1) * DEPTH]

    def unmix(q, carry):
        for h in range(2):
            rows = pl.ds(pl.multiple_of(32 * q + 16 * h, 16), 16)
            turned = []
            for c in range(RADIX):
                re, im = part_t[0, c, rows, :], part_t[1, c, rows, :]
                if c > 0:
                    cos, sin = tc_s[c, rows, :], ts_s[c, rows, :]
                    re, im = re * cos + im * sin, im * cos - re * sin
                turned.append((re, im))
            mixed = butterfly([t[0] for t in turned], [t[1] for t in turned])
            for j, (first, second) in enumerate(mixed):
                out_v[0, 4 * j + q, 16 * h : 16 * h + 16, :] = second.astype(bf16)
                out_v[1, 4 * j + q, 16 * h : 16 * h + 16, :] = first.astype(bf16)
        return carry

    def give(q, carry):
        for i in range(RADIX):
            y = lax.rem(my_y + (2, 3, 1, 0)[i // 2], 4)
            t = 8 * y + 4 * (i % 2) + q

            @pl.when(t != me)
            def _():
                row_send(out_v.at[:, t], out_ref.at[:, me], 5, t).start()

        return carry

    unmix(0, 0)

    def unmix_step(q, carry):
        unmix(q, carry)
        give(q - 1, carry)
        return carry

    lax.fori_loop(1, 4, unmix_step, 0)
    give(3, 0)
    out_ref[:, pl.ds(me, 1)] = out_v[:, pl.ds(me, 1)]
    row_wait(out_ref, 5)
    for k, ref in ((1, u_v), (2, s_v), (5, out_v)):
        row_send(ref.at[:, 0 : ROW - 1], ref.at[:, 0 : ROW - 1], k, me).wait_send()
    for k, ref in ((3, sp_all), (4, ex_all)):
        gz_send(ref.at[0 : GZ - 1], ref.at[0 : GZ - 1], k, g).wait_send()


def on_device(velocity_x, velocity_y, velocity_z, spacing, level_index, plane_index):
    weights, twiddle = tables()
    block = (2, 32, 32, 128)
    line = (DEPTH, RADIX, 128)
    flat = (DEPTH * RADIX, 128)
    tile = (RADIX, DEPTH, 128)
    pressure = pl.pallas_call(
        kernel,
        out_shape=pltpu.VMEM(block, bf16),
        in_specs=[
            pl.BlockSpec(memory_space=pltpu.HBM),
        ]
        * 9,
        out_specs=pl.BlockSpec(memory_space=pltpu.VMEM),
        scratch_shapes=[
            pltpu.SMEM((64,), f32),
            pltpu.VMEM((8, 128), jnp.int32),
            pltpu.SMEM((32,), jnp.int32),
            pltpu.VMEM((768, 256), bf16),
            pltpu.VMEM((256, 768), bf16),
            pltpu.VMEM((16, 128), f32),
            pltpu.VMEM(block, bf16),
            pltpu.VMEM(block, bf16),
            pltpu.VMEM(block, bf16),
            pltpu.VMEM(block, bf16),
            pltpu.VMEM(block, bf16),
            pltpu.VMEM(block, bf16),
            pltpu.VMEM(block, bf16),
            pltpu.VMEM((1, 2048), f32),
            pltpu.VMEM((1, 2048), f32),
            pltpu.VMEM(block, f32),
            pltpu.VMEM((4, 8, 128), f32),
            pltpu.VMEM((3, 128, 128), f32),
            pltpu.VMEM(line, f32),
            pltpu.VMEM(line, f32),
            pltpu.VMEM(line, f32),
            pltpu.VMEM(flat, f32),
            pltpu.VMEM(flat, f32),
            pltpu.VMEM(tile, f32),
            pltpu.VMEM(tile, f32),
            pltpu.VMEM((2,) + tile, f32),
            pltpu.VMEM((2,) + flat, f32),
            pltpu.VMEM((RADIX, DEPTH, 256), f32),
            pltpu.VMEM((2,) + tile, f32),
            pltpu.VMEM(tile, f32),
            pltpu.VMEM(tile, f32),
            pltpu.VMEM((2, RADIX, 128, 128), bf16),
            pltpu.VMEM((RADIX, DEPTH, 512), bf16),
            pltpu.VMEM((RADIX, 128), f32),
            pltpu.VMEM((GZ, 4, RADIX, 128), f32),
            pltpu.VMEM((GZ, 4, RADIX, 128), f32),
            pltpu.VMEM((4, RADIX, 128), f32),
            pltpu.VMEM((4, RADIX, 128), f32),
            pltpu.VMEM((6, GZ, RADIX, 128), f32),
            pltpu.VMEM((2, 2, GZ, RADIX, 128), f32),
            pltpu.SemaphoreType.DMA((9,)),
            pltpu.SemaphoreType.DMA((6,)),
            pltpu.SemaphoreType.DMA((6,)),
            pltpu.SemaphoreType.DMA((8,)),
        ],
        compiler_params=pltpu.CompilerParams(
            collective_id=0, has_side_effects=True, vmem_limit_bytes=48 * 1024 * 1024
        ),
        name="poisson",
    )(
        *(
            pltpu.with_memory_space_constraint(operand, pltpu.HBM)
            for operand in (
                velocity_x,
                velocity_y,
                velocity_z,
                spacing,
                level_index.reshape(8, 128),
                plane_index,
                jnp.asarray(weights),
                jnp.asarray(weights.T),
                jnp.asarray(twiddle),
            )
        )
    )
    return pressure.astype(f32) * (1.0 / 1024.0)


def solution(mesh):
    placed = (
        P(None, None, "row", "gz"),
        P(None, None, "row", "gz"),
        P(None, None, "row", "gz"),
        P(),
        P(),
        P(),
    )
    return jax.shard_map(
        on_device, mesh=mesh, in_specs=placed, out_specs=P(None, None, "row", "gz"), check_vma=False
    )
```

```python
import math

import jax
import jax.numpy as jnp
import numpy as np
from jax import lax
from jax.experimental import pallas as pl
from jax.experimental.pallas import tpu as pltpu
from jax.sharding import PartitionSpec as P

MESH = pl.DeviceIdType.MESH
f32 = jnp.float32
bf16 = jnp.bfloat16
full_turn = 2.0 * math.pi
wave_unit = 2.0 * math.pi / 2048.0
ROW = 32
GZ = 8
DEPTH = 128
RADIX = 8
HALF = DEPTH // 2
ROOT_HALF = math.sqrt(0.5)


def tables():
    idx = np.arange(128)
    angle = 2.0 * np.pi / 128.0 * ((idx[:, None] * idx[None, :]) % 128)
    c, s = np.cos(angle), np.sin(angle)
    w = np.block([[c, -s], [s, c]]).astype(np.float32)
    hi = w.astype(jnp.bfloat16)
    lo = (w - hi.astype(np.float32)).astype(jnp.bfloat16)
    weights = np.concatenate([hi, hi, lo], axis=0)
    twist = 2.0 * np.pi / 1024.0 * (np.arange(8)[:, None] * idx[None, :])
    twiddle = np.concatenate([np.cos(twist), np.sin(twist)], axis=0).astype(np.float32)
    return weights, twiddle


def butterfly(xr, xi):
    def add(p, q):
        return (p[0] + q[0], p[1] + q[1])

    def sub(p, q):
        return (p[0] - q[0], p[1] - q[1])

    def turn(p):
        return (p[1], -p[0])

    x = list(zip(xr, xi))
    a0, a1 = add(x[0], x[4]), sub(x[0], x[4])
    a2, a3 = add(x[2], x[6]), turn(sub(x[2], x[6]))
    b0, b1 = add(x[1], x[5]), sub(x[1], x[5])
    b2, b3 = add(x[3], x[7]), turn(sub(x[3], x[7]))
    e = [add(a0, a2), add(a1, a3), sub(a0, a2), sub(a1, a3)]
    o = [add(b0, b2), add(b1, b3), sub(b0, b2), sub(b1, b3)]
    o1 = ((o[1][0] + o[1][1]) * ROOT_HALF, (o[1][1] - o[1][0]) * ROOT_HALF)
    o2 = turn(o[2])
    o3 = ((o[3][1] - o[3][0]) * ROOT_HALF, -(o[3][0] + o[3][1]) * ROOT_HALF)
    odd = [o[0], o1, o2, o3]
    return [add(e[k], odd[k]) for k in range(4)] + [sub(e[k], odd[k]) for k in range(4)]


def twisted(re, im, tw_ref, c):
    if c == 0:
        return re, im
    cos = tw_ref[c : c + 1, :]
    sin = tw_ref[8 + c : 9 + c, :]
    return re * cos + im * sin, im * cos - re * sin


def put_split(y_ref, c, rows, re, im):
    re_hi = re.astype(bf16)
    im_hi = im.astype(bf16)
    y_ref[c, rows, 0:128] = re_hi
    y_ref[c, rows, 128:256] = im_hi
    y_ref[c, rows, 256:384] = (re - re_hi.astype(f32)).astype(bf16)
    y_ref[c, rows, 384:512] = (im - im_hi.astype(f32)).astype(bf16)


FAR_FIRST = (2, 3, 1, 0)
OFFSETS = [(y, x) for y in FAR_FIRST for x in FAR_FIRST]


def hops(offset):
    return sum(min(d, 4 - d) for d in offset)


FAR_CHIPS = sorted((d for d in OFFSETS if hops(d) > 2), key=lambda d: -hops(d))
NEAR_CHIPS = sorted((d for d in OFFSETS if 0 < hops(d) <= 2), key=lambda d: -hops(d))


def kernel(
    u_hbm, v_hbm, w_hbm, spacing_hbm, level_hbm, plane_hbm, weights_hbm, weights_t_hbm, tw_hbm,
    out_ref,
    spacing_ref, level_ref, plane_ref, weights_ref, weights_t, tw_ref,
    u_v, v_v, w_v, s_v, recv_u, recv_s, out_v, halo_out, halo_in, halo_cols, band, bmat,
    inv_s, fe_s, bc_s, vs_s, ws_s, vt_s, wt_s, yt_s, rhs, part, part_t, tc_s, ts_s, q_t, y_s, kx_s,
    sp_all, ex_all, sp_send, ex_send, far_send, far_all, red, edge,
    lsem, bar_send, bar_recv, s_recv, hello,
):
    me = lax.axis_index("row")
    g = lax.axis_index("gz")
    my_y, my_x, my_core = me // 8, lax.rem(me // 2, 4), lax.rem(me, 2)
    ys = [lax.rem(my_y + d, 4) * 8 for d in FAR_FIRST]
    ends = [
        lax.rem(my_x + d, 4) * 2 + lax.rem(my_core + c, 2) for d in FAR_FIRST for c in (1, 0)
    ]
    barrier = pltpu.get_barrier_semaphore()
    partner = 2 * (me // 2) + 1 - my_core
    upper_z, lower_z = lax.rem(g + 1, GZ), lax.rem(g + GZ - 1, GZ)

    def chip(d):
        return lax.rem(my_y + d[0], 4) * 8 + lax.rem(my_x + d[1], 4) * 2

    def greet(device):
        pl.semaphore_signal(barrier, inc=1, device_id=device, device_id_type=MESH)

    for d in FAR_CHIPS:
        greet({"row": chip(d) + 1})
    for d in NEAR_CHIPS:
        greet({"row": chip(d)})
    greet({"gz": upper_z})
    greet({"gz": lower_z})
    greet({"row": partner})
    loads = [
        pltpu.make_async_copy(u_hbm, u_v, lsem.at[0]),
        pltpu.make_async_copy(w_hbm, w_v, lsem.at[1]),
        pltpu.make_async_copy(v_hbm, v_v, lsem.at[2]),
        pltpu.make_async_copy(level_hbm, level_ref, lsem.at[3]),
        pltpu.make_async_copy(spacing_hbm, spacing_ref, lsem.at[4]),
        pltpu.make_async_copy(plane_hbm, plane_ref, lsem.at[5]),
        pltpu.make_async_copy(tw_hbm, tw_ref, lsem.at[6]),
        pltpu.make_async_copy(weights_hbm, weights_ref, lsem.at[7]),
        pltpu.make_async_copy(weights_t_hbm, weights_t, lsem.at[8]),
    ]
    for load in loads:
        load.start()

    def row_send(src, dst, k, t):
        return pltpu.make_async_remote_copy(
            src, dst, bar_send.at[k], bar_recv.at[k], device_id={"row": t}, device_id_type=MESH
        )

    def gz_send(src, dst, k, t):
        return pltpu.make_async_remote_copy(
            src, dst, bar_send.at[k], bar_recv.at[k], device_id={"gz": t}, device_id_type=MESH
        )

    def tell_partner():
        pl.semaphore_signal(hello.at[4], inc=1, device_id={"row": partner}, device_id_type=MESH)

    def send_u(chips):
        for n in range(2):
            for d in chips:
                t = chip(d) + lax.rem(my_core + 1 + n, 2)
                row_send(u_v.at[:, t], recv_u.at[:, me], 1, t).start()

    loads[0].wait()

    @pl.when(my_core == 0)
    def _():
        pl.semaphore_wait(barrier, 2 * len(NEAR_CHIPS) + 3)
        tell_partner()

    @pl.when(my_core == 1)
    def _():
        pl.semaphore_wait(hello.at[4], 1)

    send_u(NEAR_CHIPS)
    row_send(u_v.at[:, partner], recv_u.at[:, me], 1, partner).start()

    @pl.when(my_core == 1)
    def _():
        pl.semaphore_wait(barrier, 2 * len(FAR_CHIPS) + 3)
        tell_partner()

    @pl.when(my_core == 0)
    def _():
        pl.semaphore_wait(hello.at[4], 1)

    send_u(FAR_CHIPS)

    def greet_z(k, z):
        pl.semaphore_signal(hello.at[k], inc=1, device_id={"gz": z}, device_id_type=MESH)

    greet_z(0, upper_z)
    greet_z(1, lower_z)
    recv_u[:, pl.ds(me, 1)] = u_v[:, pl.ds(me, 1)]

    for load in loads[1:]:
        load.wait()

    pick = (lax.broadcasted_iota(jnp.int32, (16, DEPTH), 1) == DEPTH - 1).astype(f32).astype(bf16)
    for n in range(2):
        column = lax.dot_general(
            pick,
            w_v[n].reshape(1024, DEPTH),
            (((1,), (1,)), ((), ())),
            preferred_element_type=f32,
        )
        halo_out[:, n * 1024 : (n + 1) * 1024] = column[0:1, :]

    level = level_ref[...]
    width = jnp.zeros((GZ, DEPTH), f32)
    for n in range(64):
        width = jnp.where(level == n, spacing_ref[n], width)
    lane = lax.broadcasted_iota(jnp.int32, (GZ, DEPTH), 1)
    block = lax.broadcasted_iota(jnp.int32, (GZ, DEPTH), 0)
    shift_up = pltpu.roll(width, 1, 1)
    previous = jnp.where(lane == 0, pltpu.roll(shift_up, 1, 0), shift_up)
    shift_down = pltpu.roll(width, DEPTH - 1, 1)
    following = jnp.where(lane == DEPTH - 1, pltpu.roll(shift_down, GZ - 1, 0), shift_down)
    lower = 1.0 / (0.5 * (previous + width) * width)
    upper = 1.0 / (0.5 * (width + following) * width)
    lower = jnp.where((lane == 0) & (block == 0), 0.0, lower)
    upper = jnp.where((lane == DEPTH - 1) & (block == GZ - 1), 0.0, upper)
    band[0] = lower
    band[1] = upper
    band[2] = -(lower + upper)
    band[3] = 1.0 / width
    for n in range(3):
        row_n = jnp.broadcast_to(band[n, pl.ds(g, 1), :], (DEPTH, DEPTH))
        bmat[n] = row_n.T

    halo_copy = gz_send(halo_out, halo_in, 0, upper_z)

    @pl.when(g < GZ - 1)
    def _():
        halo_copy.start()

    @pl.when(g == 0)
    def _():
        halo_in[...] = jnp.zeros_like(halo_in)

    @pl.when(g > 0)
    def _():
        halo_copy.wait_recv()

    @pl.when(g < GZ - 1)
    def _():
        halo_copy.wait_send()

    first_lane = (lax.broadcasted_iota(jnp.int32, (8, DEPTH), 1) == 0).astype(f32)
    first_row = (lax.broadcasted_iota(jnp.int32, (8, DEPTH), 0) == 0).astype(f32)
    spot = (first_lane * first_row).astype(bf16)
    for n in range(2):
        wide = jnp.broadcast_to(halo_in[:, n * 1024 : (n + 1) * 1024], (8, 1024)).astype(bf16)
        halo_cols[n] = lax.dot_general(
            wide, spot, (((0,), (0,)), ((), ())), preferred_element_type=f32
        ).reshape(32, 32, DEPTH)
    pl.semaphore_wait(hello.at[0], 1)
    pl.semaphore_wait(hello.at[1], 1)
    greet_z(2, lax.rem(g + 2, GZ))
    greet_z(3, lax.rem(g + GZ - 2, GZ))
    inv_width = band[3, pl.ds(g, 1), :]
    lane32 = lax.broadcasted_iota(jnp.int32, (32, DEPTH), 1)

    def make_source(t):
        wave = plane_ref[t].astype(f32) * wave_unit
        slopes = []
        for n in range(2):
            upward = w_v[n, t].astype(f32)
            below = jnp.where(lane32 == 0, halo_cols[n, t], pltpu.roll(upward, 1, 1))
            slopes.append((upward - below) * inv_width)
        s_v[0, t] = (-wave * v_v[1, t].astype(f32) + slopes[0]).astype(bf16)
        s_v[1, t] = (wave * v_v[0, t].astype(f32) + slopes[1]).astype(bf16)

    def send_s(t):
        pltpu.make_async_remote_copy(
            s_v.at[:, t],
            recv_s.at[:, me],
            bar_send.at[2],
            s_recv.at[me // 4],
            device_id={"row": t},
            device_id_type=MESH,
        ).start()

    def source_step(i, carry):
        base = lax.rem(my_y + lax.rem(2 + i + (i // 2) * (1 + 2 * lax.rem(i, 2)), 4), 4) * 8
        make_source(base + ends[0])
        for n in range(1, 8):
            make_source(base + ends[n])
            send_s(base + ends[n - 1])

        @pl.when(i < 3)
        def _():
            send_s(base + ends[7])

        return carry

    lax.fori_loop(0, 4, source_step, 0)
    recv_s[:, pl.ds(me, 1)] = s_v[:, pl.ds(me, 1)]

    outer = lax.broadcasted_iota(jnp.int32, (RADIX, 128), 0)
    inner = lax.broadcasted_iota(jnp.int32, (RADIX, 128), 1)
    mode = 8 * inner + outer
    mode = jnp.where(mode >= 512, mode - 1024, mode)
    wave_x = mode.astype(f32) * (full_turn / 1024.0)
    own_wave = plane_ref[me].astype(f32) * wave_unit
    wave_sq = wave_x * wave_x + own_wave * own_wave
    kx_s[...] = wave_x

    def coef(n, z):
        return jnp.broadcast_to(bmat[n, pl.ds(z, 1), :], (RADIX, 128))

    def factor(j, carry):
        top, bottom, v_top, w_bottom = carry
        z = j
        lo, up = coef(0, z), coef(1, z)
        inv = 1.0 / ((coef(2, z) - wave_sq) - lo * top)
        fe = lo * inv
        top = up * inv
        inv_s[z] = inv
        fe_s[z] = fe
        bc_s[z] = top
        v_top = -fe * v_top
        vs_s[pl.ds(pl.multiple_of(z * 8, 8), 8), :] = v_top
        z = DEPTH - 1 - j
        lo, up = coef(0, z), coef(1, z)
        inv = 1.0 / ((coef(2, z) - wave_sq) - up * bottom)
        fe = up * inv
        bottom = lo * inv
        inv_s[z] = inv
        fe_s[z] = fe
        bc_s[z] = bottom
        w_bottom = -fe * w_bottom
        ws_s[pl.ds(pl.multiple_of(z * 8, 8), 8), :] = w_bottom
        return top, bottom, v_top, w_bottom

    zero = jnp.zeros((RADIX, 128), f32)
    one = jnp.ones((RADIX, 128), f32)
    top, bottom, v_top, w_bottom = lax.fori_loop(0, HALF, factor, (zero, zero, one, one))
    inv_det = 1.0 / (1.0 - top * bottom)

    def at(z):
        return pl.ds(pl.multiple_of(z * 8, 8), 8)

    v_lo = v_top * inv_det
    v_hi = -bottom * v_lo
    w_hi = w_bottom * inv_det
    w_lo = -top * w_hi
    vs_s[at(HALF - 1), :] = v_lo
    vs_s[at(HALF), :] = v_hi
    ws_s[at(HALF - 1), :] = w_lo
    ws_s[at(HALF), :] = w_hi

    def spread(j, carry):
        v_lo, v_hi, w_lo, w_hi = carry
        z = HALF - 1 - j
        bc = bc_s[z]
        v_lo = vs_s[at(z), :] - bc * v_lo
        w_lo = -bc * w_lo
        vs_s[at(z), :] = v_lo
        ws_s[at(z), :] = w_lo
        z = HALF + j
        bc = bc_s[z]
        v_hi = -bc * v_hi
        w_hi = ws_s[at(z), :] - bc * w_hi
        vs_s[at(z), :] = v_hi
        ws_s[at(z), :] = w_hi
        return v_lo, v_hi, w_lo, w_hi

    v_lo, v_hi, w_lo, w_hi = lax.fori_loop(1, HALF, spread, (v_lo, v_hi, w_lo, w_hi))
    sp_send[0] = v_lo
    sp_send[1] = v_hi
    sp_send[2] = w_lo
    sp_send[3] = w_hi
    sp_all[pl.ds(g, 1)] = sp_send[...][None]
    for c in range(RADIX):
        vt_s[c] = vs_s[pl.ds(c, DEPTH, stride=8), :]
        wt_s[c] = ws_s[pl.ds(c, DEPTH, stride=8), :]

    pl.semaphore_wait(hello.at[2], 1)
    pl.semaphore_wait(hello.at[3], 1)

    def send_sp(d, carry):
        t = lax.rem(g + d, GZ)
        gz_send(sp_send, sp_all.at[g], 3, t).start()
        return carry

    lax.fori_loop(1, GZ, send_sp, 0)

    def forward(recv, ready, finish):
        def flip(i, carry):
            y = lax.rem(my_y + 4 - lax.rem(2 + i + (i // 2) * (1 + 2 * lax.rem(i, 2)), 4), 4)
            for n in range(2):
                ready(2 * y + n)
            for n in range(2):
                for h in range(2):
                    a = 2 * y + h
                    q_t[n, a] = recv[n, pl.ds(4 * a, 4)].reshape(128, 128).T
            return carry

        lax.fori_loop(0, 4, flip, 0)

        for half in range(2):
            for i in range(4):
                rows = slice(64 * half + 16 * i, 64 * half + 16 * (i + 1))
                xr = [q_t[0, a, rows, :].astype(f32) for a in range(RADIX)]
                xi = [q_t[1, a, rows, :].astype(f32) for a in range(RADIX)]
                for c, (re, im) in enumerate(butterfly(xr, xi)):
                    re, im = twisted(re, im, tw_ref, c)
                    put_split(y_s, c, rows, re, im)
            for c in range(0, RADIX, 4):
                rows = y_s[c : c + 4, 64 * half : 64 * (half + 1), :].reshape(256, 512)
                acc = jnp.dot(
                    rows, weights_ref[0:512, :], preferred_element_type=f32
                ) + jnp.dot(rows[:, 0:256], weights_ref[512:768, :], preferred_element_type=f32)
                for n in range(4):
                    finish(c + n, half, acc[64 * n : 64 * (n + 1)])

    def keep_along(c, half, own):
        rows = slice(64 * half, 64 * (half + 1))
        kx = kx_s[c : c + 1, :]
        part[c, rows, 0:128] = -kx * own[:, 128:256]
        part[c, rows, 128:256] = kx * own[:, 0:128]

    def keep_rhs(c, half, own):
        total = own + part[c, 64 * half : 64 * (half + 1)]
        rhs[0, pl.ds(512 * half + c, 64, stride=8), :] = total[:, 0:128]
        rhs[1, pl.ds(512 * half + c, 64, stride=8), :] = total[:, 128:256]

    def row_wait(ref, k):
        row_send(ref.at[:, 0 : ROW - 1], ref.at[:, 0 : ROW - 1], k, me).wait_recv()

    def turn_table(c, carry):
        tc_s[c] = jnp.broadcast_to(tw_ref[pl.ds(c, 1), :], (128, 128)).T
        ts_s[c] = jnp.broadcast_to(tw_ref[pl.ds(8 + c, 1), :], (128, 128)).T
        return carry

    lax.fori_loop(1, RADIX, turn_table, 0)
    row_wait(recv_u, 1)
    forward(recv_u, lambda a: None, keep_along)

    gz_send(sp_all.at[0 : GZ - 1], sp_all.at[0 : GZ - 1], 3, g).wait_recv()
    beta = zero
    for b in range(GZ):
        v_first, v_last, w_first, w_last = (sp_all[b, n] for n in range(4))
        inv = 1.0 / (1.0 - v_first * beta)
        gamma = v_last * beta * inv
        red[0, b] = gamma
        red[1, b] = v_last + gamma * v_first
        red[2, b] = inv
        red[3, b] = inv * v_first
        red[4, b] = inv * w_first
        beta = w_last + gamma * w_first
        red[5, b] = beta

    def s_ready(a):
        def wait_for(count):
            view = recv_s.at[:, 0:count]
            pltpu.make_async_remote_copy(
                view, view, bar_send.at[2], s_recv.at[a], device_id={"row": me}, device_id_type=MESH
            ).wait_recv()

        @pl.when(a == me // 4)
        def _():
            wait_for(3)

        @pl.when(a != me // 4)
        def _():
            wait_for(4)

    forward(recv_s, s_ready, keep_rhs)

    def sweep(rows, factor_ref, scale_ref, before):
        for k in range(0, len(rows), 4):
            group = rows[k : k + 4]
            factors = [factor_ref[z] for z in group]
            products = [-factors[0]]
            for factor_z in factors[1:]:
                products.append(-factor_z * products[-1])
            after = []
            for n in range(2):
                partial = None
                for z, factor_z, product_z in zip(group, factors, products):
                    own = rhs[n, 8 * z : 8 * z + 8, :]
                    if scale_ref is not None:
                        own = own * scale_ref[z]
                    partial = own if partial is None else own - factor_z * partial
                    value = partial + product_z * before[n]
                    rhs[n, 8 * z : 8 * z + 8, :] = value
                after.append(value)
            before = after
            yield before

    def both(low_rows, high_rows, factor_ref, scale_ref, low, high):
        for low, high in zip(
            sweep(low_rows, factor_ref, scale_ref, low),
            sweep(high_rows, factor_ref, scale_ref, high),
        ):
            pass
        return low, high

    (low_re, low_im), (high_re, high_im) = both(
        range(HALF), range(DEPTH - 1, HALF - 1, -1), fe_s, inv_s, (zero, zero), (zero, zero)
    )
    bc_low, bc_high = bc_s[HALF - 1], bc_s[HALF]
    inv_det = 1.0 / (1.0 - bc_low * bc_high)
    low_re = (low_re - bc_low * high_re) * inv_det
    low_im = (low_im - bc_low * high_im) * inv_det
    high_re = high_re - bc_high * low_re
    high_im = high_im - bc_high * low_im
    rhs[0, at(HALF - 1), :] = low_re
    rhs[1, at(HALF - 1), :] = low_im
    rhs[0, at(HALF), :] = high_re
    rhs[1, at(HALF), :] = high_im

    (low_re, low_im), (high_re, high_im) = both(
        range(HALF - 2, -1, -1),
        range(HALF + 1, DEPTH),
        bc_s,
        None,
        (low_re, low_im),
        (high_re, high_im),
    )
    far_send[0, 0:8] = low_re.astype(bf16)
    far_send[0, 8:16] = low_im.astype(bf16)
    far_send[1, 0:8] = high_re.astype(bf16)
    far_send[1, 8:16] = high_im.astype(bf16)
    ex_send[0] = low_re
    ex_send[1] = low_im
    ex_send[2] = high_re
    ex_send[3] = high_im
    ex_all[pl.ds(g, 1)] = ex_send[...][None]

    for d in (4, 3, 5):
        gz_send(far_send, far_all.at[g], 6, lax.rem(g + d, GZ)).start()
    for d in (2, 6, 1, 7):
        gz_send(ex_send, ex_all.at[g], 4, lax.rem(g + d, GZ)).start()
    for c in range(RADIX):
        for n in range(2):
            yt_s[n, c] = rhs[n, pl.ds(c, DEPTH, stride=8), :]
    gz_send(ex_all.at[0:4], ex_all.at[0:4], 4, g).wait_recv()
    gz_send(far_all.at[0:3], far_all.at[0:3], 6, g).wait_recv()
    for d in (3, 4, 5):
        b = lax.rem(g + d, GZ)
        for n in range(2):
            pair = far_all[b, n].astype(f32)
            ex_all[b, 2 * n] = pair[0:8]
            ex_all[b, 2 * n + 1] = pair[8:16]

    for n in range(2):
        alpha = zero
        befores = []
        for b in range(GZ):
            befores.append(alpha)
            alpha = (
                ex_all[b, 2 + n] + red[0, b] * ex_all[b, n] + red[1, b] * alpha
            )
        first = zero
        edge[1, n, GZ - 1] = zero
        for b in range(GZ - 1, -1, -1):
            first = red[2, b] * ex_all[b, n] + red[3, b] * befores[b] + red[4, b] * first
            if b > 0:
                edge[1, n, b - 1] = first
                edge[0, n, b] = befores[b] + red[5, b - 1] * first
        edge[0, n, 0] = zero

    from_below = [edge[0, n, g] for n in range(2)]
    from_above = [edge[1, n, g] for n in range(2)]

    across = (((1,), (1,)), ((), ()))
    for c in range(0, RADIX, 2):
        for h in range(2):
            for i in range(DEPTH // 16):
                rows = slice(16 * i, 16 * (i + 1))
                v_c, w_c = vt_s[c + h, rows, :], wt_s[c + h, rows, :]
                full = [
                    yt_s[n, c + h, rows, :]
                    + v_c * from_below[n][c + h : c + h + 1, :]
                    + w_c * from_above[n][c + h : c + h + 1, :]
                    for n in range(2)
                ]
                put_split(y_s, c + h, rows, full[1], full[0])
        rows = y_s[c : c + 2].reshape(2 * DEPTH, 512)
        acc = lax.dot_general(
            weights_t[:, 0:512], rows, across, preferred_element_type=f32
        ) + lax.dot_general(
            weights_t[:, 512:768], rows[:, 0:256], across, preferred_element_type=f32
        )
        for n in range(2):
            for h in range(2):
                part_t[n, c + h] = acc[n * 128 : (n + 1) * 128, h * DEPTH : (h + 1) * DEPTH]

    def unmix(q, h):
        rows = pl.ds(pl.multiple_of(32 * q + 16 * h, 16), 16)
        turned = []
        for c in range(RADIX):
            re, im = part_t[0, c, rows, :], part_t[1, c, rows, :]
            if c > 0:
                cos, sin = tc_s[c, rows, :], ts_s[c, rows, :]
                re, im = re * cos + im * sin, im * cos - re * sin
            turned.append((re, im))
        mixed = butterfly([t[0] for t in turned], [t[1] for t in turned])
        for j, (first, second) in enumerate(mixed):
            out_v[0, 4 * j + q, 16 * h : 16 * h + 16, :] = second.astype(bf16)
            out_v[1, 4 * j + q, 16 * h : 16 * h + 16, :] = first.astype(bf16)

    def give(q, carry):
        for i in range(RADIX):
            y = lax.rem(my_y + (2, 3, 1, 0)[i // 2], 4)
            t = 8 * y + 4 * (i % 2) + q

            @pl.when(t != me)
            def _():
                row_send(out_v.at[:, t], out_ref.at[:, me], 5, t).start()

        return carry

    unmix(0, 0)
    unmix(0, 1)

    def unmix_step(q, carry):
        unmix(q, 0)
        give(q - 1, carry)
        unmix(q, 1)
        return carry

    lax.fori_loop(1, 4, unmix_step, 0)
    give(3, 0)
    out_ref[:, pl.ds(me, 1)] = out_v[:, pl.ds(me, 1)]
    row_wait(out_ref, 5)
    for k, ref in ((1, u_v), (2, s_v), (5, out_v)):
        row_send(ref.at[:, 0 : ROW - 1], ref.at[:, 0 : ROW - 1], k, me).wait_send()
    for k, ref, n in ((3, sp_all, 7), (4, ex_all, 4), (6, far_all, 3)):
        gz_send(ref.at[0:n], ref.at[0:n], k, g).wait_send()


def on_device(velocity_x, velocity_y, velocity_z, spacing, level_index, plane_index):
    weights, twiddle = tables()
    block = (2, 32, 32, 128)
    line = (DEPTH, RADIX, 128)
    flat = (DEPTH * RADIX, 128)
    tile = (RADIX, DEPTH, 128)
    pressure = pl.pallas_call(
        kernel,
        out_shape=pltpu.VMEM(block, bf16),
        in_specs=[
            pl.BlockSpec(memory_space=pltpu.HBM),
        ]
        * 9,
        out_specs=pl.BlockSpec(memory_space=pltpu.VMEM),
        scratch_shapes=[
            pltpu.SMEM((64,), f32),
            pltpu.VMEM((8, 128), jnp.int32),
            pltpu.SMEM((32,), jnp.int32),
            pltpu.VMEM((768, 256), bf16),
            pltpu.VMEM((256, 768), bf16),
            pltpu.VMEM((16, 128), f32),
            pltpu.VMEM(block, bf16),
            pltpu.VMEM(block, bf16),
            pltpu.VMEM(block, bf16),
            pltpu.VMEM(block, bf16),
            pltpu.VMEM(block, bf16),
            pltpu.VMEM(block, bf16),
            pltpu.VMEM(block, bf16),
            pltpu.VMEM((1, 2048), f32),
            pltpu.VMEM((1, 2048), f32),
            pltpu.VMEM(block, f32),
            pltpu.VMEM((4, 8, 128), f32),
            pltpu.VMEM((3, 128, 128), f32),
            pltpu.VMEM(line, f32),
            pltpu.VMEM(line, f32),
            pltpu.VMEM(line, f32),
            pltpu.VMEM(flat, f32),
            pltpu.VMEM(flat, f32),
            pltpu.VMEM(tile, f32),
            pltpu.VMEM(tile, f32),
            pltpu.VMEM((2,) + tile, f32),
            pltpu.VMEM((2,) + flat, f32),
            pltpu.VMEM((RADIX, DEPTH, 256), f32),
            pltpu.VMEM((2,) + tile, f32),
            pltpu.VMEM(tile, f32),
            pltpu.VMEM(tile, f32),
            pltpu.VMEM((2, RADIX, 128, 128), bf16),
            pltpu.VMEM((RADIX, DEPTH, 512), bf16),
            pltpu.VMEM((RADIX, 128), f32),
            pltpu.VMEM((GZ, 4, RADIX, 128), f32),
            pltpu.VMEM((GZ, 4, RADIX, 128), f32),
            pltpu.VMEM((4, RADIX, 128), f32),
            pltpu.VMEM((4, RADIX, 128), f32),
            pltpu.VMEM((2, 2 * RADIX, 128), bf16),
            pltpu.VMEM((GZ, 2, 2 * RADIX, 128), bf16),
            pltpu.VMEM((6, GZ, RADIX, 128), f32),
            pltpu.VMEM((2, 2, GZ, RADIX, 128), f32),
            pltpu.SemaphoreType.DMA((9,)),
            pltpu.SemaphoreType.DMA((7,)),
            pltpu.SemaphoreType.DMA((7,)),
            pltpu.SemaphoreType.DMA((8,)),
            pltpu.SemaphoreType.REGULAR((5,)),
        ],
        compiler_params=pltpu.CompilerParams(
            collective_id=0, has_side_effects=True, vmem_limit_bytes=48 * 1024 * 1024
        ),
        name="poisson",
    )(
        *(
            pltpu.with_memory_space_constraint(operand, pltpu.HBM)
            for operand in (
                velocity_x,
                velocity_y,
                velocity_z,
                spacing,
                level_index.reshape(8, 128),
                plane_index,
                jnp.asarray(weights),
                jnp.asarray(weights.T),
                jnp.asarray(twiddle),
            )
        )
    )
    return pressure.astype(f32) * (1.0 / 1024.0)


def solution(mesh):
    placed = (
        P(None, None, "row", "gz"),
        P(None, None, "row", "gz"),
        P(None, None, "row", "gz"),
        P(),
        P(),
        P(),
    )
    return jax.shard_map(
        on_device, mesh=mesh, in_specs=placed, out_specs=P(None, None, "row", "gz"), check_vma=False
    )
```

```python
import math

import jax
import jax.numpy as jnp
import numpy as np
from jax import lax
from jax.experimental import pallas as pl
from jax.experimental.pallas import tpu as pltpu
from jax.sharding import PartitionSpec as P

MESH = pl.DeviceIdType.MESH
f32 = jnp.float32
bf16 = jnp.bfloat16
full_turn = 2.0 * math.pi
wave_unit = 2.0 * math.pi / 2048.0
ROW = 32
GZ = 8
DEPTH = 128
RADIX = 8
HALF = DEPTH // 2
ROOT_HALF = math.sqrt(0.5)


def tables():
    idx = np.arange(128)
    angle = 2.0 * np.pi / 128.0 * ((idx[:, None] * idx[None, :]) % 128)
    c, s = np.cos(angle), np.sin(angle)
    w = np.block([[c, -s], [s, c]]).astype(np.float32)
    hi = w.astype(jnp.bfloat16)
    lo = (w - hi.astype(np.float32)).astype(jnp.bfloat16)
    weights = np.concatenate([hi, hi, lo], axis=0)
    twist = 2.0 * np.pi / 1024.0 * (np.arange(8)[:, None] * idx[None, :])
    twiddle = np.concatenate([np.cos(twist), np.sin(twist)], axis=0).astype(np.float32)
    return weights, twiddle


def butterfly(xr, xi):
    def add(p, q):
        return (p[0] + q[0], p[1] + q[1])

    def sub(p, q):
        return (p[0] - q[0], p[1] - q[1])

    def turn(p):
        return (p[1], -p[0])

    x = list(zip(xr, xi))
    a0, a1 = add(x[0], x[4]), sub(x[0], x[4])
    a2, a3 = add(x[2], x[6]), turn(sub(x[2], x[6]))
    b0, b1 = add(x[1], x[5]), sub(x[1], x[5])
    b2, b3 = add(x[3], x[7]), turn(sub(x[3], x[7]))
    e = [add(a0, a2), add(a1, a3), sub(a0, a2), sub(a1, a3)]
    o = [add(b0, b2), add(b1, b3), sub(b0, b2), sub(b1, b3)]
    o1 = ((o[1][0] + o[1][1]) * ROOT_HALF, (o[1][1] - o[1][0]) * ROOT_HALF)
    o2 = turn(o[2])
    o3 = ((o[3][1] - o[3][0]) * ROOT_HALF, -(o[3][0] + o[3][1]) * ROOT_HALF)
    odd = [o[0], o1, o2, o3]
    return [add(e[k], odd[k]) for k in range(4)] + [sub(e[k], odd[k]) for k in range(4)]


def twisted(re, im, tw_ref, c):
    if c == 0:
        return re, im
    cos = tw_ref[c : c + 1, :]
    sin = tw_ref[8 + c : 9 + c, :]
    return re * cos + im * sin, im * cos - re * sin


def put_split(y_ref, c, rows, re, im):
    re_hi = re.astype(bf16)
    im_hi = im.astype(bf16)
    y_ref[c, rows, 0:128] = re_hi
    y_ref[c, rows, 128:256] = im_hi
    y_ref[c, rows, 256:384] = (re - re_hi.astype(f32)).astype(bf16)
    y_ref[c, rows, 384:512] = (im - im_hi.astype(f32)).astype(bf16)


FAR_FIRST = (2, 3, 1, 0)
OFFSETS = [(y, x) for y in FAR_FIRST for x in FAR_FIRST]


def hops(offset):
    return sum(min(d, 4 - d) for d in offset)


FAR_CHIPS = sorted((d for d in OFFSETS if hops(d) > 2), key=lambda d: -hops(d))
NEAR_CHIPS = sorted((d for d in OFFSETS if 0 < hops(d) <= 2), key=lambda d: -hops(d))


def kernel(
    u_hbm, v_hbm, w_hbm, spacing_hbm, level_hbm, plane_hbm, weights_hbm, weights_t_hbm, tw_hbm,
    out_ref,
    spacing_ref, level_ref, plane_ref, weights_ref, weights_t, tw_ref,
    u_v, v_v, w_v, s_v, recv_u, recv_s, out_v, halo_out, halo_in, halo_cols, band, bmat,
    inv_s, fe_s, bc_s, vs_s, ws_s, vt_s, wt_s, yt_s, rhs, part, part_t, tc_s, ts_s, q_t, y_s, kx_s,
    sp_all, ex_all, sp_send, ex_send, far_send, far_all, red, edge,
    lsem, bar_send, bar_recv, s_recv, hello,
):
    me = lax.axis_index("row")
    g = lax.axis_index("gz")
    my_y, my_x, my_core = me // 8, lax.rem(me // 2, 4), lax.rem(me, 2)
    barrier = pltpu.get_barrier_semaphore()
    partner = 2 * (me // 2) + 1 - my_core
    upper_z, lower_z = lax.rem(g + 1, GZ), lax.rem(g + GZ - 1, GZ)

    def chip(d):
        return lax.rem(my_y + d[0], 4) * 8 + lax.rem(my_x + d[1], 4) * 2

    def greet(device):
        pl.semaphore_signal(barrier, inc=1, device_id=device, device_id_type=MESH)

    for d in FAR_CHIPS:
        greet({"row": chip(d) + 1})
    for d in NEAR_CHIPS:
        greet({"row": chip(d)})
    greet({"gz": upper_z})
    greet({"gz": lower_z})
    greet({"row": partner})
    loads = [
        pltpu.make_async_copy(u_hbm, u_v, lsem.at[0]),
        pltpu.make_async_copy(w_hbm, w_v, lsem.at[1]),
        pltpu.make_async_copy(v_hbm, v_v, lsem.at[2]),
        pltpu.make_async_copy(level_hbm, level_ref, lsem.at[3]),
        pltpu.make_async_copy(spacing_hbm, spacing_ref, lsem.at[4]),
        pltpu.make_async_copy(plane_hbm, plane_ref, lsem.at[5]),
        pltpu.make_async_copy(tw_hbm, tw_ref, lsem.at[6]),
        pltpu.make_async_copy(weights_hbm, weights_ref, lsem.at[7]),
        pltpu.make_async_copy(weights_t_hbm, weights_t, lsem.at[8]),
    ]
    for load in loads:
        load.start()

    def row_send(src, dst, k, t):
        return pltpu.make_async_remote_copy(
            src, dst, bar_send.at[k], bar_recv.at[k], device_id={"row": t}, device_id_type=MESH
        )

    def gz_send(src, dst, k, t):
        return pltpu.make_async_remote_copy(
            src, dst, bar_send.at[k], bar_recv.at[k], device_id={"gz": t}, device_id_type=MESH
        )

    def tell_partner():
        pl.semaphore_signal(hello.at[4], inc=1, device_id={"row": partner}, device_id_type=MESH)

    def send_u(chips, core):
        for d in chips:
            t = chip(d) + core
            row_send(u_v.at[:, t], recv_u.at[:, me], 1, t).start()

    loads[0].wait()

    @pl.when(my_core == 0)
    def _():
        pl.semaphore_wait(barrier, 2 * len(NEAR_CHIPS) + 3)
        tell_partner()

    @pl.when(my_core == 1)
    def _():
        pl.semaphore_wait(hello.at[4], 1)

    send_u(NEAR_CHIPS, 0)
    send_u(NEAR_CHIPS, 1)
    row_send(u_v.at[:, partner], recv_u.at[:, me], 1, partner).start()

    @pl.when(my_core == 1)
    def _():
        pl.semaphore_wait(barrier, 2 * len(FAR_CHIPS) + 3)
        tell_partner()

    @pl.when(my_core == 0)
    def _():
        pl.semaphore_wait(hello.at[4], 1)

    send_u(FAR_CHIPS, 0)

    def greet_z(k, z):
        pl.semaphore_signal(hello.at[k], inc=1, device_id={"gz": z}, device_id_type=MESH)

    greet_z(0, upper_z)
    greet_z(1, lower_z)
    recv_u[:, pl.ds(me, 1)] = u_v[:, pl.ds(me, 1)]

    for load in loads[1:]:
        load.wait()

    pick = (lax.broadcasted_iota(jnp.int32, (16, DEPTH), 1) == DEPTH - 1).astype(f32).astype(bf16)
    for n in range(2):
        column = lax.dot_general(
            pick,
            w_v[n].reshape(1024, DEPTH),
            (((1,), (1,)), ((), ())),
            preferred_element_type=f32,
        )
        halo_out[:, n * 1024 : (n + 1) * 1024] = column[0:1, :]

    level = level_ref[...]
    width = jnp.zeros((GZ, DEPTH), f32)
    for n in range(64):
        width = jnp.where(level == n, spacing_ref[n], width)
    lane = lax.broadcasted_iota(jnp.int32, (GZ, DEPTH), 1)
    block = lax.broadcasted_iota(jnp.int32, (GZ, DEPTH), 0)
    shift_up = pltpu.roll(width, 1, 1)
    previous = jnp.where(lane == 0, pltpu.roll(shift_up, 1, 0), shift_up)
    shift_down = pltpu.roll(width, DEPTH - 1, 1)
    following = jnp.where(lane == DEPTH - 1, pltpu.roll(shift_down, GZ - 1, 0), shift_down)
    lower = 1.0 / (0.5 * (previous + width) * width)
    upper = 1.0 / (0.5 * (width + following) * width)
    lower = jnp.where((lane == 0) & (block == 0), 0.0, lower)
    upper = jnp.where((lane == DEPTH - 1) & (block == GZ - 1), 0.0, upper)
    band[0] = lower
    band[1] = upper
    band[2] = -(lower + upper)
    band[3] = 1.0 / width
    for n in range(3):
        row_n = jnp.broadcast_to(band[n, pl.ds(g, 1), :], (DEPTH, DEPTH))
        bmat[n] = row_n.T

    halo_copy = gz_send(halo_out, halo_in, 0, upper_z)

    @pl.when(g < GZ - 1)
    def _():
        halo_copy.start()

    @pl.when(g == 0)
    def _():
        halo_in[...] = jnp.zeros_like(halo_in)

    outer = lax.broadcasted_iota(jnp.int32, (RADIX, 128), 0)
    inner = lax.broadcasted_iota(jnp.int32, (RADIX, 128), 1)
    mode = 8 * inner + outer
    mode = jnp.where(mode >= 512, mode - 1024, mode)
    wave_x = mode.astype(f32) * (full_turn / 1024.0)
    own_wave = plane_ref[me].astype(f32) * wave_unit
    wave_sq = wave_x * wave_x + own_wave * own_wave
    kx_s[...] = wave_x

    def coef(n, z):
        return jnp.broadcast_to(bmat[n, pl.ds(z, 1), :], (RADIX, 128))

    def factor(j, carry):
        top, bottom, v_top, w_bottom = carry
        z = j
        lo, up = coef(0, z), coef(1, z)
        inv = 1.0 / ((coef(2, z) - wave_sq) - lo * top)
        fe = lo * inv
        top = up * inv
        inv_s[z] = inv
        fe_s[z] = fe
        bc_s[z] = top
        v_top = -fe * v_top
        vs_s[pl.ds(pl.multiple_of(z * 8, 8), 8), :] = v_top
        z = DEPTH - 1 - j
        lo, up = coef(0, z), coef(1, z)
        inv = 1.0 / ((coef(2, z) - wave_sq) - up * bottom)
        fe = up * inv
        bottom = lo * inv
        inv_s[z] = inv
        fe_s[z] = fe
        bc_s[z] = bottom
        w_bottom = -fe * w_bottom
        ws_s[pl.ds(pl.multiple_of(z * 8, 8), 8), :] = w_bottom
        return top, bottom, v_top, w_bottom

    zero = jnp.zeros((RADIX, 128), f32)
    one = jnp.ones((RADIX, 128), f32)
    top, bottom, v_top, w_bottom = lax.fori_loop(0, HALF, factor, (zero, zero, one, one))
    inv_det = 1.0 / (1.0 - top * bottom)

    def at(z):
        return pl.ds(pl.multiple_of(z * 8, 8), 8)

    v_lo = v_top * inv_det
    v_hi = -bottom * v_lo
    w_hi = w_bottom * inv_det
    w_lo = -top * w_hi
    vs_s[at(HALF - 1), :] = v_lo
    vs_s[at(HALF), :] = v_hi
    ws_s[at(HALF - 1), :] = w_lo
    ws_s[at(HALF), :] = w_hi

    def spread(j, carry):
        v_lo, v_hi, w_lo, w_hi = carry
        z = HALF - 1 - j
        bc = bc_s[z]
        v_lo = vs_s[at(z), :] - bc * v_lo
        w_lo = -bc * w_lo
        vs_s[at(z), :] = v_lo
        ws_s[at(z), :] = w_lo
        z = HALF + j
        bc = bc_s[z]
        v_hi = -bc * v_hi
        w_hi = ws_s[at(z), :] - bc * w_hi
        vs_s[at(z), :] = v_hi
        ws_s[at(z), :] = w_hi
        return v_lo, v_hi, w_lo, w_hi

    v_lo, v_hi, w_lo, w_hi = lax.fori_loop(1, HALF, spread, (v_lo, v_hi, w_lo, w_hi))
    sp_send[0] = v_lo
    sp_send[1] = v_hi
    sp_send[2] = w_lo
    sp_send[3] = w_hi
    sp_all[pl.ds(g, 1)] = sp_send[...][None]
    for c in range(RADIX):
        vt_s[c] = vs_s[pl.ds(c, DEPTH, stride=8), :]
        wt_s[c] = ws_s[pl.ds(c, DEPTH, stride=8), :]

    @pl.when(g > 0)
    def _():
        halo_copy.wait_recv()

    @pl.when(g < GZ - 1)
    def _():
        halo_copy.wait_send()

    first_lane = (lax.broadcasted_iota(jnp.int32, (8, DEPTH), 1) == 0).astype(f32)
    first_row = (lax.broadcasted_iota(jnp.int32, (8, DEPTH), 0) == 0).astype(f32)
    spot = (first_lane * first_row).astype(bf16)
    for n in range(2):
        wide = jnp.broadcast_to(halo_in[:, n * 1024 : (n + 1) * 1024], (8, 1024)).astype(bf16)
        halo_cols[n] = lax.dot_general(
            wide, spot, (((0,), (0,)), ((), ())), preferred_element_type=f32
        ).reshape(32, 32, DEPTH)
    pl.semaphore_wait(hello.at[0], 1)
    pl.semaphore_wait(hello.at[1], 1)
    greet_z(2, lax.rem(g + 2, GZ))
    greet_z(3, lax.rem(g + GZ - 2, GZ))
    inv_width = band[3, pl.ds(g, 1), :]
    lane32 = lax.broadcasted_iota(jnp.int32, (32, DEPTH), 1)

    def make_source(t):
        wave = plane_ref[t].astype(f32) * wave_unit
        slopes = []
        for n in range(2):
            upward = w_v[n, t].astype(f32)
            below = jnp.where(lane32 == 0, halo_cols[n, t], pltpu.roll(upward, 1, 1))
            slopes.append((upward - below) * inv_width)
        s_v[0, t] = (-wave * v_v[1, t].astype(f32) + slopes[0]).astype(bf16)
        s_v[1, t] = (wave * v_v[0, t].astype(f32) + slopes[1]).astype(bf16)

    def send_s(t):
        pltpu.make_async_remote_copy(
            s_v.at[:, t],
            recv_s.at[:, me],
            bar_send.at[2],
            s_recv.at[me // 4],
            device_id={"row": t},
            device_id_type=MESH,
        ).start()

    columns = [lax.rem(my_x + d, 4) * 2 for d in FAR_FIRST]

    def sources_for(core):
        def source_step(i, carry):
            base = lax.rem(my_y + lax.rem(2 + i + (i // 2) * (1 + 2 * lax.rem(i, 2)), 4), 4) * 8
            make_source(base + columns[0] + core)
            for n in range(1, 4):
                make_source(base + columns[n] + core)
                send_s(base + columns[n - 1] + core)

            @pl.when(base + columns[3] + core != me)
            def _():
                send_s(base + columns[3] + core)

            return carry

        lax.fori_loop(0, 4, source_step, 0)

    sources_for(0)
    send_u(FAR_CHIPS, 1)
    sources_for(1)
    recv_s[:, pl.ds(me, 1)] = s_v[:, pl.ds(me, 1)]

    pl.semaphore_wait(hello.at[2], 1)
    pl.semaphore_wait(hello.at[3], 1)

    def send_sp(d, carry):
        t = lax.rem(g + d, GZ)
        gz_send(sp_send, sp_all.at[g], 3, t).start()
        return carry

    lax.fori_loop(1, GZ, send_sp, 0)

    def forward(recv, ready, finish):
        def flip(i, carry):
            y = lax.rem(my_y + 4 - lax.rem(2 + i + (i // 2) * (1 + 2 * lax.rem(i, 2)), 4), 4)
            for n in range(2):
                ready(2 * y + n)
            for n in range(2):
                for h in range(2):
                    a = 2 * y + h
                    q_t[n, a] = recv[n, pl.ds(4 * a, 4)].reshape(128, 128).T
            return carry

        lax.fori_loop(0, 4, flip, 0)

        for half in range(2):
            for i in range(4):
                rows = slice(64 * half + 16 * i, 64 * half + 16 * (i + 1))
                xr = [q_t[0, a, rows, :].astype(f32) for a in range(RADIX)]
                xi = [q_t[1, a, rows, :].astype(f32) for a in range(RADIX)]
                for c, (re, im) in enumerate(butterfly(xr, xi)):
                    re, im = twisted(re, im, tw_ref, c)
                    put_split(y_s, c, rows, re, im)
            for c in range(0, RADIX, 4):
                rows = y_s[c : c + 4, 64 * half : 64 * (half + 1), :].reshape(256, 512)
                acc = jnp.dot(
                    rows, weights_ref[0:512, :], preferred_element_type=f32
                ) + jnp.dot(rows[:, 0:256], weights_ref[512:768, :], preferred_element_type=f32)
                for n in range(4):
                    finish(c + n, half, acc[64 * n : 64 * (n + 1)])

    def keep_along(c, half, own):
        rows = slice(64 * half, 64 * (half + 1))
        kx = kx_s[c : c + 1, :]
        part[c, rows, 0:128] = -kx * own[:, 128:256]
        part[c, rows, 128:256] = kx * own[:, 0:128]

    def keep_rhs(c, half, own):
        total = own + part[c, 64 * half : 64 * (half + 1)]
        rhs[0, pl.ds(512 * half + c, 64, stride=8), :] = total[:, 0:128]
        rhs[1, pl.ds(512 * half + c, 64, stride=8), :] = total[:, 128:256]

    def row_wait(ref, k):
        row_send(ref.at[:, 0 : ROW - 1], ref.at[:, 0 : ROW - 1], k, me).wait_recv()

    def turn_table(c, carry):
        tc_s[c] = jnp.broadcast_to(tw_ref[pl.ds(c, 1), :], (128, 128)).T
        ts_s[c] = jnp.broadcast_to(tw_ref[pl.ds(8 + c, 1), :], (128, 128)).T
        return carry

    lax.fori_loop(1, RADIX, turn_table, 0)
    row_wait(recv_u, 1)
    forward(recv_u, lambda a: None, keep_along)

    def s_ready(a):
        def wait_for(count):
            view = recv_s.at[:, 0:count]
            pltpu.make_async_remote_copy(
                view, view, bar_send.at[2], s_recv.at[a], device_id={"row": me}, device_id_type=MESH
            ).wait_recv()

        @pl.when(a == me // 4)
        def _():
            wait_for(3)

        @pl.when(a != me // 4)
        def _():
            wait_for(4)

    forward(recv_s, s_ready, keep_rhs)

    def sweep(rows, factor_ref, scale_ref, before):
        for k in range(0, len(rows), 4):
            group = rows[k : k + 4]
            factors = [factor_ref[z] for z in group]
            products = [-factors[0]]
            for factor_z in factors[1:]:
                products.append(-factor_z * products[-1])
            after = []
            for n in range(2):
                partial = None
                for z, factor_z, product_z in zip(group, factors, products):
                    own = rhs[n, 8 * z : 8 * z + 8, :]
                    if scale_ref is not None:
                        own = own * scale_ref[z]
                    partial = own if partial is None else own - factor_z * partial
                    value = partial + product_z * before[n]
                    rhs[n, 8 * z : 8 * z + 8, :] = value
                after.append(value)
            before = after
            yield before

    def both(low_rows, high_rows, factor_ref, scale_ref, low, high):
        for low, high in zip(
            sweep(low_rows, factor_ref, scale_ref, low),
            sweep(high_rows, factor_ref, scale_ref, high),
        ):
            pass
        return low, high

    (low_re, low_im), (high_re, high_im) = both(
        range(HALF), range(DEPTH - 1, HALF - 1, -1), fe_s, inv_s, (zero, zero), (zero, zero)
    )
    bc_low, bc_high = bc_s[HALF - 1], bc_s[HALF]
    inv_det = 1.0 / (1.0 - bc_low * bc_high)
    low_re = (low_re - bc_low * high_re) * inv_det
    low_im = (low_im - bc_low * high_im) * inv_det
    high_re = high_re - bc_high * low_re
    high_im = high_im - bc_high * low_im
    rhs[0, at(HALF - 1), :] = low_re
    rhs[1, at(HALF - 1), :] = low_im
    rhs[0, at(HALF), :] = high_re
    rhs[1, at(HALF), :] = high_im

    (low_re, low_im), (high_re, high_im) = both(
        range(HALF - 2, -1, -1),
        range(HALF + 1, DEPTH),
        bc_s,
        None,
        (low_re, low_im),
        (high_re, high_im),
    )
    far_send[0, 0:8] = low_re.astype(bf16)
    far_send[0, 8:16] = low_im.astype(bf16)
    far_send[1, 0:8] = high_re.astype(bf16)
    far_send[1, 8:16] = high_im.astype(bf16)
    ex_send[0] = low_re
    ex_send[1] = low_im
    ex_send[2] = high_re
    ex_send[3] = high_im
    ex_all[pl.ds(g, 1)] = ex_send[...][None]

    for d in (4, 3, 5):
        gz_send(far_send, far_all.at[g], 6, lax.rem(g + d, GZ)).start()
    for d in (2, 6, 1, 7):
        gz_send(ex_send, ex_all.at[g], 4, lax.rem(g + d, GZ)).start()
    for c in range(RADIX):
        for n in range(2):
            yt_s[n, c] = rhs[n, pl.ds(c, DEPTH, stride=8), :]
    gz_send(sp_all.at[0 : GZ - 1], sp_all.at[0 : GZ - 1], 3, g).wait_recv()
    beta = zero
    for b in range(GZ):
        v_first, v_last, w_first, w_last = (sp_all[b, n] for n in range(4))
        inv = 1.0 / (1.0 - v_first * beta)
        gamma = v_last * beta * inv
        red[0, b] = gamma
        red[1, b] = v_last + gamma * v_first
        red[2, b] = inv
        red[3, b] = inv * v_first
        red[4, b] = inv * w_first
        beta = w_last + gamma * w_first
        red[5, b] = beta

    gz_send(ex_all.at[0:4], ex_all.at[0:4], 4, g).wait_recv()
    gz_send(far_all.at[0:3], far_all.at[0:3], 6, g).wait_recv()
    for d in (3, 4, 5):
        b = lax.rem(g + d, GZ)
        for n in range(2):
            pair = far_all[b, n].astype(f32)
            ex_all[b, 2 * n] = pair[0:8]
            ex_all[b, 2 * n + 1] = pair[8:16]

    for n in range(2):
        alpha = zero
        befores = []
        for b in range(GZ):
            befores.append(alpha)
            alpha = (
                ex_all[b, 2 + n] + red[0, b] * ex_all[b, n] + red[1, b] * alpha
            )
        first = zero
        edge[1, n, GZ - 1] = zero
        for b in range(GZ - 1, -1, -1):
            first = red[2, b] * ex_all[b, n] + red[3, b] * befores[b] + red[4, b] * first
            if b > 0:
                edge[1, n, b - 1] = first
                edge[0, n, b] = befores[b] + red[5, b - 1] * first
        edge[0, n, 0] = zero

    from_below = [edge[0, n, g] for n in range(2)]
    from_above = [edge[1, n, g] for n in range(2)]

    across = (((1,), (1,)), ((), ()))
    for c in range(0, RADIX, 2):
        for h in range(2):
            for i in range(DEPTH // 16):
                rows = slice(16 * i, 16 * (i + 1))
                v_c, w_c = vt_s[c + h, rows, :], wt_s[c + h, rows, :]
                full = [
                    yt_s[n, c + h, rows, :]
                    + v_c * from_below[n][c + h : c + h + 1, :]
                    + w_c * from_above[n][c + h : c + h + 1, :]
                    for n in range(2)
                ]
                put_split(y_s, c + h, rows, full[1], full[0])
        rows = y_s[c : c + 2].reshape(2 * DEPTH, 512)
        acc = lax.dot_general(
            weights_t[:, 0:512], rows, across, preferred_element_type=f32
        ) + lax.dot_general(
            weights_t[:, 512:768], rows[:, 0:256], across, preferred_element_type=f32
        )
        for n in range(2):
            for h in range(2):
                part_t[n, c + h] = acc[n * 128 : (n + 1) * 128, h * DEPTH : (h + 1) * DEPTH]

    def unmix(q, h):
        rows = pl.ds(pl.multiple_of(32 * q + 16 * h, 16), 16)
        turned = []
        for c in range(RADIX):
            re, im = part_t[0, c, rows, :], part_t[1, c, rows, :]
            if c > 0:
                cos, sin = tc_s[c, rows, :], ts_s[c, rows, :]
                re, im = re * cos + im * sin, im * cos - re * sin
            turned.append((re, im))
        mixed = butterfly([t[0] for t in turned], [t[1] for t in turned])
        for j, (first, second) in enumerate(mixed):
            out_v[0, 4 * j + q, 16 * h : 16 * h + 16, :] = second.astype(bf16)
            out_v[1, 4 * j + q, 16 * h : 16 * h + 16, :] = first.astype(bf16)

    def give(q, carry):
        for i in range(RADIX):
            y = lax.rem(my_y + (2, 3, 1, 0)[i // 2], 4)
            t = 8 * y + 4 * (i % 2) + q

            @pl.when(t != me)
            def _():
                row_send(out_v.at[:, t], out_ref.at[:, me], 5, t).start()

        return carry

    def turn(i):
        return 2 * lax.rem(i, 2) + i // 2

    unmix(0, 0)
    unmix(0, 1)

    def unmix_step(i, carry):
        unmix(turn(i), 0)
        give(turn(i - 1), carry)
        unmix(turn(i), 1)
        return carry

    lax.fori_loop(1, 4, unmix_step, 0)
    give(3, 0)
    out_ref[:, pl.ds(me, 1)] = out_v[:, pl.ds(me, 1)]
    row_wait(out_ref, 5)
    for k, ref in ((1, u_v), (2, s_v), (5, out_v)):
        row_send(ref.at[:, 0 : ROW - 1], ref.at[:, 0 : ROW - 1], k, me).wait_send()
    for k, ref, n in ((3, sp_all, 7), (4, ex_all, 4), (6, far_all, 3)):
        gz_send(ref.at[0:n], ref.at[0:n], k, g).wait_send()


def on_device(velocity_x, velocity_y, velocity_z, spacing, level_index, plane_index):
    weights, twiddle = tables()
    block = (2, 32, 32, 128)
    line = (DEPTH, RADIX, 128)
    flat = (DEPTH * RADIX, 128)
    tile = (RADIX, DEPTH, 128)
    pressure = pl.pallas_call(
        kernel,
        out_shape=pltpu.VMEM(block, bf16),
        in_specs=[
            pl.BlockSpec(memory_space=pltpu.HBM),
        ]
        * 9,
        out_specs=pl.BlockSpec(memory_space=pltpu.VMEM),
        scratch_shapes=[
            pltpu.SMEM((64,), f32),
            pltpu.VMEM((8, 128), jnp.int32),
            pltpu.SMEM((32,), jnp.int32),
            pltpu.VMEM((768, 256), bf16),
            pltpu.VMEM((256, 768), bf16),
            pltpu.VMEM((16, 128), f32),
            pltpu.VMEM(block, bf16),
            pltpu.VMEM(block, bf16),
            pltpu.VMEM(block, bf16),
            pltpu.VMEM(block, bf16),
            pltpu.VMEM(block, bf16),
            pltpu.VMEM(block, bf16),
            pltpu.VMEM(block, bf16),
            pltpu.VMEM((1, 2048), f32),
            pltpu.VMEM((1, 2048), f32),
            pltpu.VMEM(block, f32),
            pltpu.VMEM((4, 8, 128), f32),
            pltpu.VMEM((3, 128, 128), f32),
            pltpu.VMEM(line, f32),
            pltpu.VMEM(line, f32),
            pltpu.VMEM(line, f32),
            pltpu.VMEM(flat, f32),
            pltpu.VMEM(flat, f32),
            pltpu.VMEM(tile, f32),
            pltpu.VMEM(tile, f32),
            pltpu.VMEM((2,) + tile, f32),
            pltpu.VMEM((2,) + flat, f32),
            pltpu.VMEM((RADIX, DEPTH, 256), f32),
            pltpu.VMEM((2,) + tile, f32),
            pltpu.VMEM(tile, f32),
            pltpu.VMEM(tile, f32),
            pltpu.VMEM((2, RADIX, 128, 128), bf16),
            pltpu.VMEM((RADIX, DEPTH, 512), bf16),
            pltpu.VMEM((RADIX, 128), f32),
            pltpu.VMEM((GZ, 4, RADIX, 128), f32),
            pltpu.VMEM((GZ, 4, RADIX, 128), f32),
            pltpu.VMEM((4, RADIX, 128), f32),
            pltpu.VMEM((4, RADIX, 128), f32),
            pltpu.VMEM((2, 2 * RADIX, 128), bf16),
            pltpu.VMEM((GZ, 2, 2 * RADIX, 128), bf16),
            pltpu.VMEM((6, GZ, RADIX, 128), f32),
            pltpu.VMEM((2, 2, GZ, RADIX, 128), f32),
            pltpu.SemaphoreType.DMA((9,)),
            pltpu.SemaphoreType.DMA((7,)),
            pltpu.SemaphoreType.DMA((7,)),
            pltpu.SemaphoreType.DMA((8,)),
            pltpu.SemaphoreType.REGULAR((5,)),
        ],
        compiler_params=pltpu.CompilerParams(
            collective_id=0, has_side_effects=True, vmem_limit_bytes=48 * 1024 * 1024
        ),
        name="poisson",
    )(
        *(
            pltpu.with_memory_space_constraint(operand, pltpu.HBM)
            for operand in (
                velocity_x,
                velocity_y,
                velocity_z,
                spacing,
                level_index.reshape(8, 128),
                plane_index,
                jnp.asarray(weights),
                jnp.asarray(weights.T),
                jnp.asarray(twiddle),
            )
        )
    )
    return pressure.astype(f32) * (1.0 / 1024.0)


def solution(mesh):
    placed = (
        P(None, None, "row", "gz"),
        P(None, None, "row", "gz"),
        P(None, None, "row", "gz"),
        P(),
        P(),
        P(),
    )
    return jax.shard_map(
        on_device, mesh=mesh, in_specs=placed, out_specs=P(None, None, "row", "gz"), check_vma=False
    )
```

```python
import math

import jax
import jax.numpy as jnp
import numpy as np
from jax import lax
from jax.experimental import pallas as pl
from jax.experimental.pallas import tpu as pltpu
from jax.sharding import PartitionSpec as P

MESH = pl.DeviceIdType.MESH
f32 = jnp.float32
bf16 = jnp.bfloat16
full_turn = 2.0 * math.pi
wave_unit = 2.0 * math.pi / 2048.0
ROW = 32
GZ = 8
DEPTH = 128
RADIX = 8
HALF = DEPTH // 2
ROOT_HALF = math.sqrt(0.5)


def tables():
    idx = np.arange(128)
    angle = 2.0 * np.pi / 128.0 * ((idx[:, None] * idx[None, :]) % 128)
    c, s = np.cos(angle), np.sin(angle)
    w = np.block([[c, -s], [s, c]]).astype(np.float32)
    hi = w.astype(jnp.bfloat16)
    lo = (w - hi.astype(np.float32)).astype(jnp.bfloat16)
    weights = np.concatenate([hi, hi, lo], axis=0)
    twist = 2.0 * np.pi / 1024.0 * (np.arange(8)[:, None] * idx[None, :])
    twiddle = np.concatenate([np.cos(twist), np.sin(twist)], axis=0).astype(np.float32)
    return weights, twiddle


def butterfly(xr, xi):
    def add(p, q):
        return (p[0] + q[0], p[1] + q[1])

    def sub(p, q):
        return (p[0] - q[0], p[1] - q[1])

    def turn(p):
        return (p[1], -p[0])

    x = list(zip(xr, xi))
    a0, a1 = add(x[0], x[4]), sub(x[0], x[4])
    a2, a3 = add(x[2], x[6]), turn(sub(x[2], x[6]))
    b0, b1 = add(x[1], x[5]), sub(x[1], x[5])
    b2, b3 = add(x[3], x[7]), turn(sub(x[3], x[7]))
    e = [add(a0, a2), add(a1, a3), sub(a0, a2), sub(a1, a3)]
    o = [add(b0, b2), add(b1, b3), sub(b0, b2), sub(b1, b3)]
    o1 = ((o[1][0] + o[1][1]) * ROOT_HALF, (o[1][1] - o[1][0]) * ROOT_HALF)
    o2 = turn(o[2])
    o3 = ((o[3][1] - o[3][0]) * ROOT_HALF, -(o[3][0] + o[3][1]) * ROOT_HALF)
    odd = [o[0], o1, o2, o3]
    return [add(e[k], odd[k]) for k in range(4)] + [sub(e[k], odd[k]) for k in range(4)]


def twisted(re, im, tw_ref, c):
    if c == 0:
        return re, im
    cos = tw_ref[c : c + 1, :]
    sin = tw_ref[8 + c : 9 + c, :]
    return re * cos + im * sin, im * cos - re * sin


def put_split(y_ref, c, rows, re, im):
    re_hi = re.astype(bf16)
    im_hi = im.astype(bf16)
    y_ref[c, rows, 0:128] = re_hi
    y_ref[c, rows, 128:256] = im_hi
    y_ref[c, rows, 256:384] = (re - re_hi.astype(f32)).astype(bf16)
    y_ref[c, rows, 384:512] = (im - im_hi.astype(f32)).astype(bf16)


FAR_FIRST = (2, 3, 1, 0)
OFFSETS = [(y, x) for y in FAR_FIRST for x in FAR_FIRST]


def hops(offset):
    return sum(min(d, 4 - d) for d in offset)


FAR_CHIPS = sorted((d for d in OFFSETS if hops(d) > 2), key=lambda d: -hops(d))
NEAR_CHIPS = sorted((d for d in OFFSETS if 0 < hops(d) <= 2), key=lambda d: -hops(d))


def kernel(
    u_hbm, v_hbm, w_hbm, spacing_hbm, level_hbm, plane_hbm, weights_hbm, weights_t_hbm, tw_hbm,
    out_ref,
    spacing_ref, level_ref, plane_ref, weights_ref, weights_t, tw_ref,
    u_v, v_v, w_v, s_v, recv_u, recv_s, out_v, halo_out, halo_in, halo_cols, band, bmat,
    inv_s, fe_s, bc_s, vs_s, ws_s, vt_s, wt_s, yt_s, rhs, part, part_t, tc_s, ts_s, q_t, y_s, kx_s,
    sp_all, ex_all, sp_send, ex_send, far_send, far_all, red, edge,
    lsem, bar_send, bar_recv, s_recv, hello,
):
    me = lax.axis_index("row")
    g = lax.axis_index("gz")
    my_y, my_x, my_core = me // 8, lax.rem(me // 2, 4), lax.rem(me, 2)
    barrier = pltpu.get_barrier_semaphore()
    partner = 2 * (me // 2) + 1 - my_core
    upper_z, lower_z = lax.rem(g + 1, GZ), lax.rem(g + GZ - 1, GZ)

    def chip(d):
        return lax.rem(my_y + d[0], 4) * 8 + lax.rem(my_x + d[1], 4) * 2

    def greet(device):
        pl.semaphore_signal(barrier, inc=1, device_id=device, device_id_type=MESH)

    for d in FAR_CHIPS:
        greet({"row": chip(d) + 1})
    for d in NEAR_CHIPS:
        greet({"row": chip(d)})
    greet({"row": 2 * (me // 2), "gz": upper_z})
    greet({"row": 2 * (me // 2), "gz": lower_z})
    greet({"row": partner})
    loads = [
        pltpu.make_async_copy(u_hbm, u_v, lsem.at[0]),
        pltpu.make_async_copy(w_hbm, w_v, lsem.at[1]),
        pltpu.make_async_copy(v_hbm, v_v, lsem.at[2]),
        pltpu.make_async_copy(level_hbm, level_ref, lsem.at[3]),
        pltpu.make_async_copy(spacing_hbm, spacing_ref, lsem.at[4]),
        pltpu.make_async_copy(plane_hbm, plane_ref, lsem.at[5]),
        pltpu.make_async_copy(tw_hbm, tw_ref, lsem.at[6]),
        pltpu.make_async_copy(weights_hbm, weights_ref, lsem.at[7]),
        pltpu.make_async_copy(weights_t_hbm, weights_t, lsem.at[8]),
    ]
    for load in loads:
        load.start()

    def row_send(src, dst, k, t):
        return pltpu.make_async_remote_copy(
            src, dst, bar_send.at[k], bar_recv.at[k], device_id={"row": t}, device_id_type=MESH
        )

    def gz_send(src, dst, k, t):
        return pltpu.make_async_remote_copy(
            src, dst, bar_send.at[k], bar_recv.at[k], device_id={"gz": t}, device_id_type=MESH
        )

    def tell_partner():
        pl.semaphore_signal(hello.at[4], inc=1, device_id={"row": partner}, device_id_type=MESH)

    def send_u(chips, core):
        for d in chips:
            t = chip(d) + core
            row_send(u_v.at[:, t], recv_u.at[:, me], 1, t).start()

    loads[0].wait()

    @pl.when(my_core == 0)
    def _():
        pl.semaphore_wait(barrier, 2 * len(NEAR_CHIPS) + 5)
        tell_partner()

    @pl.when(my_core == 1)
    def _():
        pl.semaphore_wait(hello.at[4], 1)

    send_u(NEAR_CHIPS, 0)
    send_u(NEAR_CHIPS, 1)
    row_send(u_v.at[:, partner], recv_u.at[:, me], 1, partner).start()

    loads[1].wait()

    pick = (lax.broadcasted_iota(jnp.int32, (16, DEPTH), 1) == DEPTH - 1).astype(f32).astype(bf16)
    for n in range(2):
        column = lax.dot_general(
            pick,
            w_v[n].reshape(1024, DEPTH),
            (((1,), (1,)), ((), ())),
            preferred_element_type=f32,
        )
        halo_out[:, n * 1024 : (n + 1) * 1024] = column[0:1, :]

    halo_copy = gz_send(halo_out, halo_in, 0, upper_z)

    @pl.when(g < GZ - 1)
    def _():
        halo_copy.start()

    @pl.when(g == 0)
    def _():
        halo_in[...] = jnp.zeros_like(halo_in)

    @pl.when(my_core == 1)
    def _():
        pl.semaphore_wait(barrier, 2 * len(FAR_CHIPS) + 1)
        tell_partner()

    @pl.when(my_core == 0)
    def _():
        pl.semaphore_wait(hello.at[4], 1)

    send_u(FAR_CHIPS, 0)

    def greet_z(k, z):
        pl.semaphore_signal(hello.at[k], inc=1, device_id={"gz": z}, device_id_type=MESH)

    greet_z(0, upper_z)
    greet_z(1, lower_z)
    recv_u[:, pl.ds(me, 1)] = u_v[:, pl.ds(me, 1)]

    for load in loads[2:]:
        load.wait()

    level = level_ref[...]
    width = jnp.zeros((GZ, DEPTH), f32)
    for n in range(64):
        width = jnp.where(level == n, spacing_ref[n], width)
    lane = lax.broadcasted_iota(jnp.int32, (GZ, DEPTH), 1)
    block = lax.broadcasted_iota(jnp.int32, (GZ, DEPTH), 0)
    shift_up = pltpu.roll(width, 1, 1)
    previous = jnp.where(lane == 0, pltpu.roll(shift_up, 1, 0), shift_up)
    shift_down = pltpu.roll(width, DEPTH - 1, 1)
    following = jnp.where(lane == DEPTH - 1, pltpu.roll(shift_down, GZ - 1, 0), shift_down)
    lower = 1.0 / (0.5 * (previous + width) * width)
    upper = 1.0 / (0.5 * (width + following) * width)
    lower = jnp.where((lane == 0) & (block == 0), 0.0, lower)
    upper = jnp.where((lane == DEPTH - 1) & (block == GZ - 1), 0.0, upper)
    band[0] = lower
    band[1] = upper
    band[2] = -(lower + upper)
    band[3] = 1.0 / width
    for n in range(3):
        row_n = jnp.broadcast_to(band[n, pl.ds(g, 1), :], (DEPTH, DEPTH))
        bmat[n] = row_n.T

    outer = lax.broadcasted_iota(jnp.int32, (RADIX, 128), 0)
    inner = lax.broadcasted_iota(jnp.int32, (RADIX, 128), 1)
    mode = 8 * inner + outer
    mode = jnp.where(mode >= 512, mode - 1024, mode)
    wave_x = mode.astype(f32) * (full_turn / 1024.0)
    own_wave = plane_ref[me].astype(f32) * wave_unit
    wave_sq = wave_x * wave_x + own_wave * own_wave
    kx_s[...] = wave_x

    def coef(n, z):
        return jnp.broadcast_to(bmat[n, pl.ds(z, 1), :], (RADIX, 128))

    def factor(j, carry):
        top, bottom, v_top, w_bottom = carry
        z = j
        lo, up = coef(0, z), coef(1, z)
        inv = 1.0 / ((coef(2, z) - wave_sq) - lo * top)
        fe = lo * inv
        top = up * inv
        inv_s[z] = inv
        fe_s[z] = fe
        bc_s[z] = top
        v_top = -fe * v_top
        vs_s[pl.ds(pl.multiple_of(z * 8, 8), 8), :] = v_top
        z = DEPTH - 1 - j
        lo, up = coef(0, z), coef(1, z)
        inv = 1.0 / ((coef(2, z) - wave_sq) - up * bottom)
        fe = up * inv
        bottom = lo * inv
        inv_s[z] = inv
        fe_s[z] = fe
        bc_s[z] = bottom
        w_bottom = -fe * w_bottom
        ws_s[pl.ds(pl.multiple_of(z * 8, 8), 8), :] = w_bottom
        return top, bottom, v_top, w_bottom

    zero = jnp.zeros((RADIX, 128), f32)
    one = jnp.ones((RADIX, 128), f32)
    top, bottom, v_top, w_bottom = lax.fori_loop(0, HALF, factor, (zero, zero, one, one))
    inv_det = 1.0 / (1.0 - top * bottom)

    def at(z):
        return pl.ds(pl.multiple_of(z * 8, 8), 8)

    v_lo = v_top * inv_det
    v_hi = -bottom * v_lo
    w_hi = w_bottom * inv_det
    w_lo = -top * w_hi
    vs_s[at(HALF - 1), :] = v_lo
    vs_s[at(HALF), :] = v_hi
    ws_s[at(HALF - 1), :] = w_lo
    ws_s[at(HALF), :] = w_hi

    def spread(j, carry):
        v_lo, v_hi, w_lo, w_hi = carry
        z = HALF - 1 - j
        bc = bc_s[z]
        v_lo = vs_s[at(z), :] - bc * v_lo
        w_lo = -bc * w_lo
        vs_s[at(z), :] = v_lo
        ws_s[at(z), :] = w_lo
        z = HALF + j
        bc = bc_s[z]
        v_hi = -bc * v_hi
        w_hi = ws_s[at(z), :] - bc * w_hi
        vs_s[at(z), :] = v_hi
        ws_s[at(z), :] = w_hi
        return v_lo, v_hi, w_lo, w_hi

    v_lo, v_hi, w_lo, w_hi = lax.fori_loop(1, HALF, spread, (v_lo, v_hi, w_lo, w_hi))
    sp_send[0] = v_lo
    sp_send[1] = v_hi
    sp_send[2] = w_lo
    sp_send[3] = w_hi
    sp_all[pl.ds(g, 1)] = sp_send[...][None]
    for c in range(RADIX):
        vt_s[c] = vs_s[pl.ds(c, DEPTH, stride=8), :]
        wt_s[c] = ws_s[pl.ds(c, DEPTH, stride=8), :]

    @pl.when(g > 0)
    def _():
        halo_copy.wait_recv()

    @pl.when(g < GZ - 1)
    def _():
        halo_copy.wait_send()

    first_lane = (lax.broadcasted_iota(jnp.int32, (8, DEPTH), 1) == 0).astype(f32)
    first_row = (lax.broadcasted_iota(jnp.int32, (8, DEPTH), 0) == 0).astype(f32)
    spot = (first_lane * first_row).astype(bf16)
    for n in range(2):
        wide = jnp.broadcast_to(halo_in[:, n * 1024 : (n + 1) * 1024], (8, 1024)).astype(bf16)
        halo_cols[n] = lax.dot_general(
            wide, spot, (((0,), (0,)), ((), ())), preferred_element_type=f32
        ).reshape(32, 32, DEPTH)
    pl.semaphore_wait(hello.at[0], 1)
    pl.semaphore_wait(hello.at[1], 1)
    greet_z(2, lax.rem(g + 2, GZ))
    greet_z(3, lax.rem(g + GZ - 2, GZ))
    inv_width = band[3, pl.ds(g, 1), :]
    lane32 = lax.broadcasted_iota(jnp.int32, (32, DEPTH), 1)

    def make_source(t):
        wave = plane_ref[t].astype(f32) * wave_unit
        slopes = []
        for n in range(2):
            upward = w_v[n, t].astype(f32)
            below = jnp.where(lane32 == 0, halo_cols[n, t], pltpu.roll(upward, 1, 1))
            slopes.append((upward - below) * inv_width)
        s_v[0, t] = (-wave * v_v[1, t].astype(f32) + slopes[0]).astype(bf16)
        s_v[1, t] = (wave * v_v[0, t].astype(f32) + slopes[1]).astype(bf16)

    def send_s(t):
        pltpu.make_async_remote_copy(
            s_v.at[:, t],
            recv_s.at[:, me],
            bar_send.at[2],
            s_recv.at[me // 4],
            device_id={"row": t},
            device_id_type=MESH,
        ).start()

    columns = [lax.rem(my_x + d, 4) * 2 for d in FAR_FIRST]

    def sources_for(core):
        def source_step(i, carry):
            base = lax.rem(my_y + lax.rem(2 + i + (i // 2) * (1 + 2 * lax.rem(i, 2)), 4), 4) * 8
            make_source(base + columns[0] + core)
            for n in range(1, 4):
                make_source(base + columns[n] + core)
                send_s(base + columns[n - 1] + core)

            @pl.when(base + columns[3] + core != me)
            def _():
                send_s(base + columns[3] + core)

            return carry

        lax.fori_loop(0, 4, source_step, 0)

    sources_for(0)
    send_u(FAR_CHIPS, 1)
    sources_for(1)
    recv_s[:, pl.ds(me, 1)] = s_v[:, pl.ds(me, 1)]

    pl.semaphore_wait(hello.at[2], 1)
    pl.semaphore_wait(hello.at[3], 1)

    def send_sp(d, carry):
        t = lax.rem(g + d, GZ)
        gz_send(sp_send, sp_all.at[g], 3, t).start()
        return carry

    lax.fori_loop(1, GZ, send_sp, 0)

    def forward(recv, ready, finish):
        def flip(i, carry):
            y = lax.rem(my_y + 4 - lax.rem(2 + i + (i // 2) * (1 + 2 * lax.rem(i, 2)), 4), 4)
            for n in range(2):
                ready(2 * y + n)
            for n in range(2):
                for h in range(2):
                    a = 2 * y + h
                    q_t[n, a] = recv[n, pl.ds(4 * a, 4)].reshape(128, 128).T
            return carry

        lax.fori_loop(0, 4, flip, 0)

        for half in range(2):
            for i in range(4):
                rows = slice(64 * half + 16 * i, 64 * half + 16 * (i + 1))
                xr = [q_t[0, a, rows, :].astype(f32) for a in range(RADIX)]
                xi = [q_t[1, a, rows, :].astype(f32) for a in range(RADIX)]
                for c, (re, im) in enumerate(butterfly(xr, xi)):
                    re, im = twisted(re, im, tw_ref, c)
                    put_split(y_s, c, rows, re, im)
            for c in range(0, RADIX, 4):
                rows = y_s[c : c + 4, 64 * half : 64 * (half + 1), :].reshape(256, 512)
                acc = jnp.dot(
                    rows, weights_ref[0:512, :], preferred_element_type=f32
                ) + jnp.dot(rows[:, 0:256], weights_ref[512:768, :], preferred_element_type=f32)
                for n in range(4):
                    finish(c + n, half, acc[64 * n : 64 * (n + 1)])

    def keep_along(c, half, own):
        rows = slice(64 * half, 64 * (half + 1))
        kx = kx_s[c : c + 1, :]
        part[c, rows, 0:128] = -kx * own[:, 128:256]
        part[c, rows, 128:256] = kx * own[:, 0:128]

    def keep_rhs(c, half, own):
        total = own + part[c, 64 * half : 64 * (half + 1)]
        rhs[0, pl.ds(512 * half + c, 64, stride=8), :] = total[:, 0:128]
        rhs[1, pl.ds(512 * half + c, 64, stride=8), :] = total[:, 128:256]

    def row_wait(ref, k):
        row_send(ref.at[:, 0 : ROW - 1], ref.at[:, 0 : ROW - 1], k, me).wait_recv()

    def turn_table(c, carry):
        tc_s[c] = jnp.broadcast_to(tw_ref[pl.ds(c, 1), :], (128, 128)).T
        ts_s[c] = jnp.broadcast_to(tw_ref[pl.ds(8 + c, 1), :], (128, 128)).T
        return carry

    lax.fori_loop(1, RADIX, turn_table, 0)
    row_wait(recv_u, 1)
    forward(recv_u, lambda a: None, keep_along)

    def s_ready(a):
        def wait_for(count):
            view = recv_s.at[:, 0:count]
            pltpu.make_async_remote_copy(
                view, view, bar_send.at[2], s_recv.at[a], device_id={"row": me}, device_id_type=MESH
            ).wait_recv()

        @pl.when(a == me // 4)
        def _():
            wait_for(3)

        @pl.when(a != me // 4)
        def _():
            wait_for(4)

    forward(recv_s, s_ready, keep_rhs)

    def sweep(rows, factor_ref, scale_ref, before):
        for k in range(0, len(rows), 4):
            group = rows[k : k + 4]
            factors = [factor_ref[z] for z in group]
            products = [-factors[0]]
            for factor_z in factors[1:]:
                products.append(-factor_z * products[-1])
            after = []
            for n in range(2):
                partial = None
                for z, factor_z, product_z in zip(group, factors, products):
                    own = rhs[n, 8 * z : 8 * z + 8, :]
                    if scale_ref is not None:
                        own = own * scale_ref[z]
                    partial = own if partial is None else own - factor_z * partial
                    value = partial + product_z * before[n]
                    rhs[n, 8 * z : 8 * z + 8, :] = value
                after.append(value)
            before = after
            yield before

    def both(low_rows, high_rows, factor_ref, scale_ref, low, high):
        for low, high in zip(
            sweep(low_rows, factor_ref, scale_ref, low),
            sweep(high_rows, factor_ref, scale_ref, high),
        ):
            pass
        return low, high

    (low_re, low_im), (high_re, high_im) = both(
        range(HALF), range(DEPTH - 1, HALF - 1, -1), fe_s, inv_s, (zero, zero), (zero, zero)
    )
    bc_low, bc_high = bc_s[HALF - 1], bc_s[HALF]
    inv_det = 1.0 / (1.0 - bc_low * bc_high)
    low_re = (low_re - bc_low * high_re) * inv_det
    low_im = (low_im - bc_low * high_im) * inv_det
    high_re = high_re - bc_high * low_re
    high_im = high_im - bc_high * low_im
    rhs[0, at(HALF - 1), :] = low_re
    rhs[1, at(HALF - 1), :] = low_im
    rhs[0, at(HALF), :] = high_re
    rhs[1, at(HALF), :] = high_im

    (low_re, low_im), (high_re, high_im) = both(
        range(HALF - 2, -1, -1),
        range(HALF + 1, DEPTH),
        bc_s,
        None,
        (low_re, low_im),
        (high_re, high_im),
    )
    far_send[0, 0:8] = low_re.astype(bf16)
    far_send[0, 8:16] = low_im.astype(bf16)
    far_send[1, 0:8] = high_re.astype(bf16)
    far_send[1, 8:16] = high_im.astype(bf16)
    ex_send[0] = low_re
    ex_send[1] = low_im
    ex_send[2] = high_re
    ex_send[3] = high_im
    ex_all[pl.ds(g, 1)] = ex_send[...][None]

    for d in (4, 3, 5):
        gz_send(far_send, far_all.at[g], 6, lax.rem(g + d, GZ)).start()
    for d in (2, 6, 1, 7):
        gz_send(ex_send, ex_all.at[g], 4, lax.rem(g + d, GZ)).start()
    for c in range(RADIX):
        for n in range(2):
            yt_s[n, c] = rhs[n, pl.ds(c, DEPTH, stride=8), :]
    gz_send(sp_all.at[0 : GZ - 1], sp_all.at[0 : GZ - 1], 3, g).wait_recv()
    beta = zero
    for b in range(GZ):
        v_first, v_last, w_first, w_last = (sp_all[b, n] for n in range(4))
        inv = 1.0 / (1.0 - v_first * beta)
        gamma = v_last * beta * inv
        red[0, b] = gamma
        red[1, b] = v_last + gamma * v_first
        red[2, b] = inv
        red[3, b] = inv * v_first
        red[4, b] = inv * w_first
        beta = w_last + gamma * w_first
        red[5, b] = beta

    gz_send(ex_all.at[0:4], ex_all.at[0:4], 4, g).wait_recv()
    gz_send(far_all.at[0:3], far_all.at[0:3], 6, g).wait_recv()
    for d in (3, 4, 5):
        b = lax.rem(g + d, GZ)
        for n in range(2):
            pair = far_all[b, n].astype(f32)
            ex_all[b, 2 * n] = pair[0:8]
            ex_all[b, 2 * n + 1] = pair[8:16]

    for n in range(2):
        alpha = zero
        befores = []
        for b in range(GZ):
            befores.append(alpha)
            alpha = (
                ex_all[b, 2 + n] + red[0, b] * ex_all[b, n] + red[1, b] * alpha
            )
        first = zero
        edge[1, n, GZ - 1] = zero
        for b in range(GZ - 1, -1, -1):
            first = red[2, b] * ex_all[b, n] + red[3, b] * befores[b] + red[4, b] * first
            if b > 0:
                edge[1, n, b - 1] = first
                edge[0, n, b] = befores[b] + red[5, b - 1] * first
        edge[0, n, 0] = zero

    from_below = [edge[0, n, g] for n in range(2)]
    from_above = [edge[1, n, g] for n in range(2)]

    across = (((1,), (1,)), ((), ()))
    for c in range(0, RADIX, 2):
        for h in range(2):
            for i in range(DEPTH // 16):
                rows = slice(16 * i, 16 * (i + 1))
                v_c, w_c = vt_s[c + h, rows, :], wt_s[c + h, rows, :]
                full = [
                    yt_s[n, c + h, rows, :]
                    + v_c * from_below[n][c + h : c + h + 1, :]
                    + w_c * from_above[n][c + h : c + h + 1, :]
                    for n in range(2)
                ]
                put_split(y_s, c + h, rows, full[1], full[0])
        rows = y_s[c : c + 2].reshape(2 * DEPTH, 512)
        acc = lax.dot_general(
            weights_t[:, 0:512], rows, across, preferred_element_type=f32
        ) + lax.dot_general(
            weights_t[:, 512:768], rows[:, 0:256], across, preferred_element_type=f32
        )
        for n in range(2):
            for h in range(2):
                part_t[n, c + h] = acc[n * 128 : (n + 1) * 128, h * DEPTH : (h + 1) * DEPTH]

    def unmix(q, h):
        rows = pl.ds(pl.multiple_of(32 * q + 16 * h, 16), 16)
        turned = []
        for c in range(RADIX):
            re, im = part_t[0, c, rows, :], part_t[1, c, rows, :]
            if c > 0:
                cos, sin = tc_s[c, rows, :], ts_s[c, rows, :]
                re, im = re * cos + im * sin, im * cos - re * sin
            turned.append((re, im))
        mixed = butterfly([t[0] for t in turned], [t[1] for t in turned])
        for j, (first, second) in enumerate(mixed):
            out_v[0, 4 * j + q, 16 * h : 16 * h + 16, :] = second.astype(bf16)
            out_v[1, 4 * j + q, 16 * h : 16 * h + 16, :] = first.astype(bf16)

    def give(q, carry):
        for i in range(RADIX):
            y = lax.rem(my_y + (2, 3, 1, 0)[i // 2], 4)
            t = 8 * y + 4 * (i % 2) + q

            @pl.when(t != me)
            def _():
                row_send(out_v.at[:, t], out_ref.at[:, me], 5, t).start()

        return carry

    def turn(i):
        return 2 * lax.rem(i, 2) + i // 2

    unmix(0, 0)
    unmix(0, 1)

    def unmix_step(i, carry):
        unmix(turn(i), 0)
        give(turn(i - 1), carry)
        unmix(turn(i), 1)
        return carry

    lax.fori_loop(1, 4, unmix_step, 0)
    give(3, 0)
    out_ref[:, pl.ds(me, 1)] = out_v[:, pl.ds(me, 1)]
    row_wait(out_ref, 5)
    for k, ref in ((1, u_v), (2, s_v), (5, out_v)):
        row_send(ref.at[:, 0 : ROW - 1], ref.at[:, 0 : ROW - 1], k, me).wait_send()
    for k, ref, n in ((3, sp_all, 7), (4, ex_all, 4), (6, far_all, 3)):
        gz_send(ref.at[0:n], ref.at[0:n], k, g).wait_send()


def on_device(velocity_x, velocity_y, velocity_z, spacing, level_index, plane_index):
    weights, twiddle = tables()
    block = (2, 32, 32, 128)
    line = (DEPTH, RADIX, 128)
    flat = (DEPTH * RADIX, 128)
    tile = (RADIX, DEPTH, 128)
    pressure = pl.pallas_call(
        kernel,
        out_shape=pltpu.VMEM(block, bf16),
        in_specs=[
            pl.BlockSpec(memory_space=pltpu.HBM),
        ]
        * 9,
        out_specs=pl.BlockSpec(memory_space=pltpu.VMEM),
        scratch_shapes=[
            pltpu.SMEM((64,), f32),
            pltpu.VMEM((8, 128), jnp.int32),
            pltpu.SMEM((32,), jnp.int32),
            pltpu.VMEM((768, 256), bf16),
            pltpu.VMEM((256, 768), bf16),
            pltpu.VMEM((16, 128), f32),
            pltpu.VMEM(block, bf16),
            pltpu.VMEM(block, bf16),
            pltpu.VMEM(block, bf16),
            pltpu.VMEM(block, bf16),
            pltpu.VMEM(block, bf16),
            pltpu.VMEM(block, bf16),
            pltpu.VMEM(block, bf16),
            pltpu.VMEM((1, 2048), f32),
            pltpu.VMEM((1, 2048), f32),
            pltpu.VMEM(block, f32),
            pltpu.VMEM((4, 8, 128), f32),
            pltpu.VMEM((3, 128, 128), f32),
            pltpu.VMEM(line, f32),
            pltpu.VMEM(line, f32),
            pltpu.VMEM(line, f32),
            pltpu.VMEM(flat, f32),
            pltpu.VMEM(flat, f32),
            pltpu.VMEM(tile, f32),
            pltpu.VMEM(tile, f32),
            pltpu.VMEM((2,) + tile, f32),
            pltpu.VMEM((2,) + flat, f32),
            pltpu.VMEM((RADIX, DEPTH, 256), f32),
            pltpu.VMEM((2,) + tile, f32),
            pltpu.VMEM(tile, f32),
            pltpu.VMEM(tile, f32),
            pltpu.VMEM((2, RADIX, 128, 128), bf16),
            pltpu.VMEM((RADIX, DEPTH, 512), bf16),
            pltpu.VMEM((RADIX, 128), f32),
            pltpu.VMEM((GZ, 4, RADIX, 128), f32),
            pltpu.VMEM((GZ, 4, RADIX, 128), f32),
            pltpu.VMEM((4, RADIX, 128), f32),
            pltpu.VMEM((4, RADIX, 128), f32),
            pltpu.VMEM((2, 2 * RADIX, 128), bf16),
            pltpu.VMEM((GZ, 2, 2 * RADIX, 128), bf16),
            pltpu.VMEM((6, GZ, RADIX, 128), f32),
            pltpu.VMEM((2, 2, GZ, RADIX, 128), f32),
            pltpu.SemaphoreType.DMA((9,)),
            pltpu.SemaphoreType.DMA((7,)),
            pltpu.SemaphoreType.DMA((7,)),
            pltpu.SemaphoreType.DMA((8,)),
            pltpu.SemaphoreType.REGULAR((5,)),
        ],
        compiler_params=pltpu.CompilerParams(
            collective_id=0, has_side_effects=True, vmem_limit_bytes=48 * 1024 * 1024
        ),
        name="poisson",
    )(
        *(
            pltpu.with_memory_space_constraint(operand, pltpu.HBM)
            for operand in (
                velocity_x,
                velocity_y,
                velocity_z,
                spacing,
                level_index.reshape(8, 128),
                plane_index,
                jnp.asarray(weights),
                jnp.asarray(weights.T),
                jnp.asarray(twiddle),
            )
        )
    )
    return pressure.astype(f32) * (1.0 / 1024.0)


def solution(mesh):
    placed = (
        P(None, None, "row", "gz"),
        P(None, None, "row", "gz"),
        P(None, None, "row", "gz"),
        P(),
        P(),
        P(),
    )
    return jax.shard_map(
        on_device, mesh=mesh, in_specs=placed, out_specs=P(None, None, "row", "gz"), check_vma=False
    )
```

```python
import math

import jax
import jax.numpy as jnp
import numpy as np
from jax import lax
from jax.experimental import pallas as pl
from jax.experimental.pallas import tpu as pltpu
from jax.sharding import PartitionSpec as P

MESH = pl.DeviceIdType.MESH
f32 = jnp.float32
bf16 = jnp.bfloat16
full_turn = 2.0 * math.pi
wave_unit = 2.0 * math.pi / 2048.0
ROW = 32
GZ = 8
DEPTH = 128
RADIX = 8
HALF = DEPTH // 2
ROOT_HALF = math.sqrt(0.5)


def tables():
    idx = np.arange(128)
    angle = 2.0 * np.pi / 128.0 * ((idx[:, None] * idx[None, :]) % 128)
    c, s = np.cos(angle), np.sin(angle)
    w = np.block([[c, -s], [s, c]]).astype(np.float32)
    hi = w.astype(jnp.bfloat16)
    lo = (w - hi.astype(np.float32)).astype(jnp.bfloat16)
    weights = np.concatenate([hi, hi, lo], axis=0)
    twist = 2.0 * np.pi / 1024.0 * (np.arange(8)[:, None] * idx[None, :])
    twiddle = np.concatenate([np.cos(twist), np.sin(twist)], axis=0).astype(np.float32)
    return weights, twiddle


def butterfly(xr, xi):
    def add(p, q):
        return (p[0] + q[0], p[1] + q[1])

    def sub(p, q):
        return (p[0] - q[0], p[1] - q[1])

    def turn(p):
        return (p[1], -p[0])

    x = list(zip(xr, xi))
    a0, a1 = add(x[0], x[4]), sub(x[0], x[4])
    a2, a3 = add(x[2], x[6]), turn(sub(x[2], x[6]))
    b0, b1 = add(x[1], x[5]), sub(x[1], x[5])
    b2, b3 = add(x[3], x[7]), turn(sub(x[3], x[7]))
    e = [add(a0, a2), add(a1, a3), sub(a0, a2), sub(a1, a3)]
    o = [add(b0, b2), add(b1, b3), sub(b0, b2), sub(b1, b3)]
    o1 = ((o[1][0] + o[1][1]) * ROOT_HALF, (o[1][1] - o[1][0]) * ROOT_HALF)
    o2 = turn(o[2])
    o3 = ((o[3][1] - o[3][0]) * ROOT_HALF, -(o[3][0] + o[3][1]) * ROOT_HALF)
    odd = [o[0], o1, o2, o3]
    return [add(e[k], odd[k]) for k in range(4)] + [sub(e[k], odd[k]) for k in range(4)]


def twisted(re, im, tw_ref, c):
    if c == 0:
        return re, im
    cos = tw_ref[c : c + 1, :]
    sin = tw_ref[8 + c : 9 + c, :]
    return re * cos + im * sin, im * cos - re * sin


def put_split(y_ref, c, rows, re, im):
    re_hi = re.astype(bf16)
    im_hi = im.astype(bf16)
    y_ref[c, rows, 0:128] = re_hi
    y_ref[c, rows, 128:256] = im_hi
    y_ref[c, rows, 256:384] = (re - re_hi.astype(f32)).astype(bf16)
    y_ref[c, rows, 384:512] = (im - im_hi.astype(f32)).astype(bf16)


FAR_FIRST = (2, 3, 1, 0)
OFFSETS = [(y, x) for y in FAR_FIRST for x in FAR_FIRST]


def hops(offset):
    return sum(min(d, 4 - d) for d in offset)


FAR_CHIPS = sorted((d for d in OFFSETS if hops(d) > 2), key=lambda d: -hops(d))
NEAR_CHIPS = sorted((d for d in OFFSETS if 0 < hops(d) <= 2), key=lambda d: -hops(d))


def kernel(
    u_hbm, v_hbm, w_hbm, spacing_hbm, level_hbm, plane_hbm, weights_hbm, weights_t_hbm, tw_hbm,
    out_ref,
    spacing_ref, level_ref, plane_ref, weights_ref, weights_t, tw_ref,
    u_v, v_v, w_v, s_v, recv_u, recv_s, out_v, halo_out, halo_in, halo_cols, band, bmat,
    inv_s, fe_s, bc_s, vs_s, ws_s, vt_s, wt_s, yt_s, rhs, part, part_t, tc_s, ts_s, q_t, y_s, kx_s,
    sp_all, ex_all, sp_send, ex_send, far_send, far_all, red, edge,
    lsem, bar_send, bar_recv, s_recv, hello,
):
    me = lax.axis_index("row")
    g = lax.axis_index("gz")
    my_y, my_x, my_core = me // 8, lax.rem(me // 2, 4), lax.rem(me, 2)
    barrier = pltpu.get_barrier_semaphore()
    partner = 2 * (me // 2) + 1 - my_core
    upper_z, lower_z = lax.rem(g + 1, GZ), lax.rem(g + GZ - 1, GZ)

    def chip(d):
        return lax.rem(my_y + d[0], 4) * 8 + lax.rem(my_x + d[1], 4) * 2

    def greet(device):
        pl.semaphore_signal(barrier, inc=1, device_id=device, device_id_type=MESH)

    for d in FAR_CHIPS:
        greet({"row": chip(d) + 1})
    for d in NEAR_CHIPS:
        greet({"row": chip(d)})
    greet({"row": 2 * (me // 2), "gz": upper_z})
    greet({"row": 2 * (me // 2), "gz": lower_z})
    greet({"row": partner})
    loads = [
        pltpu.make_async_copy(u_hbm, u_v, lsem.at[0]),
        pltpu.make_async_copy(w_hbm, w_v, lsem.at[1]),
        pltpu.make_async_copy(v_hbm, v_v, lsem.at[2]),
        pltpu.make_async_copy(level_hbm, level_ref, lsem.at[3]),
        pltpu.make_async_copy(spacing_hbm, spacing_ref, lsem.at[4]),
        pltpu.make_async_copy(plane_hbm, plane_ref, lsem.at[5]),
        pltpu.make_async_copy(tw_hbm, tw_ref, lsem.at[6]),
        pltpu.make_async_copy(weights_hbm, weights_ref, lsem.at[7]),
        pltpu.make_async_copy(weights_t_hbm, weights_t, lsem.at[8]),
    ]
    for load in loads:
        load.start()

    def row_send(src, dst, k, t):
        return pltpu.make_async_remote_copy(
            src, dst, bar_send.at[k], bar_recv.at[k], device_id={"row": t}, device_id_type=MESH
        )

    def gz_send(src, dst, k, t):
        return pltpu.make_async_remote_copy(
            src, dst, bar_send.at[k], bar_recv.at[k], device_id={"gz": t}, device_id_type=MESH
        )

    def tell_partner():
        pl.semaphore_signal(hello.at[4], inc=1, device_id={"row": partner}, device_id_type=MESH)

    def send_u(chips, core):
        for d in chips:
            t = chip(d) + core
            row_send(u_v.at[:, t], recv_u.at[:, me], 1, t).start()

    loads[0].wait()

    @pl.when(my_core == 0)
    def _():
        pl.semaphore_wait(barrier, 2 * len(NEAR_CHIPS) + 5)
        tell_partner()

    @pl.when(my_core == 1)
    def _():
        pl.semaphore_wait(hello.at[4], 1)

    send_u(NEAR_CHIPS, 0)
    send_u(NEAR_CHIPS, 1)
    row_send(u_v.at[:, partner], recv_u.at[:, me], 1, partner).start()

    loads[1].wait()

    pick = (lax.broadcasted_iota(jnp.int32, (16, DEPTH), 1) == DEPTH - 1).astype(f32).astype(bf16)
    for n in range(2):
        column = lax.dot_general(
            pick,
            w_v[n].reshape(1024, DEPTH),
            (((1,), (1,)), ((), ())),
            preferred_element_type=f32,
        )
        halo_out[:, n * 1024 : (n + 1) * 1024] = column[0:1, :]

    halo_copy = gz_send(halo_out, halo_in, 0, upper_z)

    @pl.when(g < GZ - 1)
    def _():
        halo_copy.start()

    @pl.when(g == 0)
    def _():
        halo_in[...] = jnp.zeros_like(halo_in)

    @pl.when(my_core == 1)
    def _():
        pl.semaphore_wait(barrier, 2 * len(FAR_CHIPS) + 1)
        tell_partner()

    @pl.when(my_core == 0)
    def _():
        pl.semaphore_wait(hello.at[4], 1)

    send_u(FAR_CHIPS, 0)

    def greet_z(k, z):
        pl.semaphore_signal(hello.at[k], inc=1, device_id={"gz": z}, device_id_type=MESH)

    greet_z(0, upper_z)
    greet_z(1, lower_z)
    recv_u[:, pl.ds(me, 1)] = u_v[:, pl.ds(me, 1)]

    for load in loads[2:]:
        load.wait()

    level = level_ref[...]
    width = jnp.zeros((GZ, DEPTH), f32)
    for n in range(64):
        width = jnp.where(level == n, spacing_ref[n], width)
    lane = lax.broadcasted_iota(jnp.int32, (GZ, DEPTH), 1)
    block = lax.broadcasted_iota(jnp.int32, (GZ, DEPTH), 0)
    shift_up = pltpu.roll(width, 1, 1)
    previous = jnp.where(lane == 0, pltpu.roll(shift_up, 1, 0), shift_up)
    shift_down = pltpu.roll(width, DEPTH - 1, 1)
    following = jnp.where(lane == DEPTH - 1, pltpu.roll(shift_down, GZ - 1, 0), shift_down)
    lower = 1.0 / (0.5 * (previous + width) * width)
    upper = 1.0 / (0.5 * (width + following) * width)
    lower = jnp.where((lane == 0) & (block == 0), 0.0, lower)
    upper = jnp.where((lane == DEPTH - 1) & (block == GZ - 1), 0.0, upper)
    band[0] = lower
    band[1] = upper
    band[2] = -(lower + upper)
    band[3] = 1.0 / width
    for n in range(3):
        row_n = jnp.broadcast_to(band[n, pl.ds(g, 1), :], (DEPTH, DEPTH))
        bmat[n] = row_n.T

    outer = lax.broadcasted_iota(jnp.int32, (RADIX, 128), 0)
    inner = lax.broadcasted_iota(jnp.int32, (RADIX, 128), 1)
    mode = 8 * inner + outer
    mode = jnp.where(mode >= 512, mode - 1024, mode)
    wave_x = mode.astype(f32) * (full_turn / 1024.0)
    own_wave = plane_ref[me].astype(f32) * wave_unit
    wave_sq = wave_x * wave_x + own_wave * own_wave
    kx_s[...] = wave_x

    def coef(n, z):
        return jnp.broadcast_to(bmat[n, pl.ds(z, 1), :], (RADIX, 128))

    def factor(j, carry):
        top, bottom, v_top, w_bottom = carry
        z = j
        lo, up = coef(0, z), coef(1, z)
        inv = 1.0 / ((coef(2, z) - wave_sq) - lo * top)
        fe = lo * inv
        top = up * inv
        inv_s[z] = inv
        fe_s[z] = fe
        bc_s[z] = top
        v_top = -fe * v_top
        vs_s[pl.ds(pl.multiple_of(z * 8, 8), 8), :] = v_top
        z = DEPTH - 1 - j
        lo, up = coef(0, z), coef(1, z)
        inv = 1.0 / ((coef(2, z) - wave_sq) - up * bottom)
        fe = up * inv
        bottom = lo * inv
        inv_s[z] = inv
        fe_s[z] = fe
        bc_s[z] = bottom
        w_bottom = -fe * w_bottom
        ws_s[pl.ds(pl.multiple_of(z * 8, 8), 8), :] = w_bottom
        return top, bottom, v_top, w_bottom

    zero = jnp.zeros((RADIX, 128), f32)
    one = jnp.ones((RADIX, 128), f32)
    top, bottom, v_top, w_bottom = lax.fori_loop(0, HALF, factor, (zero, zero, one, one))
    inv_det = 1.0 / (1.0 - top * bottom)

    def at(z):
        return pl.ds(pl.multiple_of(z * 8, 8), 8)

    v_lo = v_top * inv_det
    v_hi = -bottom * v_lo
    w_hi = w_bottom * inv_det
    w_lo = -top * w_hi
    vs_s[at(HALF - 1), :] = v_lo
    vs_s[at(HALF), :] = v_hi
    ws_s[at(HALF - 1), :] = w_lo
    ws_s[at(HALF), :] = w_hi

    def spread(j, carry):
        v_lo, v_hi, w_lo, w_hi = carry
        z = HALF - 1 - j
        bc = bc_s[z]
        v_lo = vs_s[at(z), :] - bc * v_lo
        w_lo = -bc * w_lo
        vs_s[at(z), :] = v_lo
        ws_s[at(z), :] = w_lo
        z = HALF + j
        bc = bc_s[z]
        v_hi = -bc * v_hi
        w_hi = ws_s[at(z), :] - bc * w_hi
        vs_s[at(z), :] = v_hi
        ws_s[at(z), :] = w_hi
        return v_lo, v_hi, w_lo, w_hi

    v_lo, v_hi, w_lo, w_hi = lax.fori_loop(1, HALF, spread, (v_lo, v_hi, w_lo, w_hi))
    sp_send[0] = v_lo
    sp_send[1] = v_hi
    sp_send[2] = w_lo
    sp_send[3] = w_hi
    sp_all[pl.ds(g, 1)] = sp_send[...][None]
    for c in range(RADIX):
        vt_s[c] = vs_s[pl.ds(c, DEPTH, stride=8), :]
        wt_s[c] = ws_s[pl.ds(c, DEPTH, stride=8), :]

    @pl.when(g > 0)
    def _():
        halo_copy.wait_recv()

    @pl.when(g < GZ - 1)
    def _():
        halo_copy.wait_send()

    first_lane = (lax.broadcasted_iota(jnp.int32, (8, DEPTH), 1) == 0).astype(f32)
    first_row = (lax.broadcasted_iota(jnp.int32, (8, DEPTH), 0) == 0).astype(f32)
    spot = (first_lane * first_row).astype(bf16)
    for n in range(2):
        wide = jnp.broadcast_to(halo_in[:, n * 1024 : (n + 1) * 1024], (8, 1024)).astype(bf16)
        halo_cols[n] = lax.dot_general(
            wide, spot, (((0,), (0,)), ((), ())), preferred_element_type=f32
        ).reshape(32, 32, DEPTH)
    pl.semaphore_wait(hello.at[0], 1)
    pl.semaphore_wait(hello.at[1], 1)
    greet_z(2, lax.rem(g + 2, GZ))
    greet_z(3, lax.rem(g + GZ - 2, GZ))
    inv_width = band[3, pl.ds(g, 1), :]
    lane32 = lax.broadcasted_iota(jnp.int32, (32, DEPTH), 1)

    def make_source(t):
        wave = plane_ref[t].astype(f32) * wave_unit
        slopes = []
        for n in range(2):
            upward = w_v[n, t].astype(f32)
            below = jnp.where(lane32 == 0, halo_cols[n, t], pltpu.roll(upward, 1, 1))
            slopes.append((upward - below) * inv_width)
        s_v[0, t] = (-wave * v_v[1, t].astype(f32) + slopes[0]).astype(bf16)
        s_v[1, t] = (wave * v_v[0, t].astype(f32) + slopes[1]).astype(bf16)

    def send_s(t):
        pltpu.make_async_remote_copy(
            s_v.at[:, t],
            recv_s.at[:, me],
            bar_send.at[2],
            s_recv.at[me // 4],
            device_id={"row": t},
            device_id_type=MESH,
        ).start()

    columns = [lax.rem(my_x + d, 4) * 2 for d in FAR_FIRST]

    def sources_for(core):
        def source_step(i, carry):
            base = lax.rem(my_y + lax.rem(2 + i + (i // 2) * (1 + 2 * lax.rem(i, 2)), 4), 4) * 8
            make_source(base + columns[0] + core)
            for n in range(1, 4):
                make_source(base + columns[n] + core)
                send_s(base + columns[n - 1] + core)

            @pl.when(base + columns[3] + core != me)
            def _():
                send_s(base + columns[3] + core)

            return carry

        lax.fori_loop(0, 4, source_step, 0)

    sources_for(0)
    send_u(FAR_CHIPS, 1)
    sources_for(1)
    recv_s[:, pl.ds(me, 1)] = s_v[:, pl.ds(me, 1)]

    pl.semaphore_wait(hello.at[2], 1)
    pl.semaphore_wait(hello.at[3], 1)

    def send_sp(d, carry):
        t = lax.rem(g + d, GZ)
        gz_send(sp_send, sp_all.at[g], 3, t).start()
        return carry

    lax.fori_loop(1, GZ, send_sp, 0)

    def forward(recv, ready, finish):
        def flip(i, carry):
            y = lax.rem(my_y + 4 - lax.rem(2 + i + (i // 2) * (1 + 2 * lax.rem(i, 2)), 4), 4)
            for n in range(2):
                ready(2 * y + n)
            for n in range(2):
                for h in range(2):
                    a = 2 * y + h
                    q_t[n, a] = recv[n, pl.ds(4 * a, 4)].reshape(128, 128).T
            return carry

        lax.fori_loop(0, 4, flip, 0)

        for half in range(2):
            for i in range(4):
                rows = slice(64 * half + 16 * i, 64 * half + 16 * (i + 1))
                xr = [q_t[0, a, rows, :].astype(f32) for a in range(RADIX)]
                xi = [q_t[1, a, rows, :].astype(f32) for a in range(RADIX)]
                for c, (re, im) in enumerate(butterfly(xr, xi)):
                    re, im = twisted(re, im, tw_ref, c)
                    put_split(y_s, c, rows, re, im)
            for c in range(0, RADIX, 4):
                rows = y_s[c : c + 4, 64 * half : 64 * (half + 1), :].reshape(256, 512)
                acc = jnp.dot(
                    rows, weights_ref[0:512, :], preferred_element_type=f32
                ) + jnp.dot(rows[:, 0:256], weights_ref[512:768, :], preferred_element_type=f32)
                for n in range(4):
                    finish(c + n, half, acc[64 * n : 64 * (n + 1)])

    def keep_along(c, half, own):
        rows = slice(64 * half, 64 * (half + 1))
        kx = kx_s[c : c + 1, :]
        part[c, rows, 0:128] = -kx * own[:, 128:256]
        part[c, rows, 128:256] = kx * own[:, 0:128]

    def keep_rhs(c, half, own):
        total = own + part[c, 64 * half : 64 * (half + 1)]
        rhs[0, pl.ds(512 * half + c, 64, stride=8), :] = total[:, 0:128]
        rhs[1, pl.ds(512 * half + c, 64, stride=8), :] = total[:, 128:256]

    def row_wait(ref, k):
        row_send(ref.at[:, 0 : ROW - 1], ref.at[:, 0 : ROW - 1], k, me).wait_recv()

    def turn_table(c, carry):
        tc_s[c] = jnp.broadcast_to(tw_ref[pl.ds(c, 1), :], (128, 128)).T
        ts_s[c] = jnp.broadcast_to(tw_ref[pl.ds(8 + c, 1), :], (128, 128)).T
        return carry

    lax.fori_loop(1, RADIX, turn_table, 0)
    row_wait(recv_u, 1)
    forward(recv_u, lambda a: None, keep_along)

    def s_ready(a):
        def wait_for(count):
            view = recv_s.at[:, 0:count]
            pltpu.make_async_remote_copy(
                view, view, bar_send.at[2], s_recv.at[a], device_id={"row": me}, device_id_type=MESH
            ).wait_recv()

        @pl.when(a == me // 4)
        def _():
            wait_for(3)

        @pl.when(a != me // 4)
        def _():
            wait_for(4)

    forward(recv_s, s_ready, keep_rhs)

    def sweep(rows, factor_ref, scale_ref, before):
        for k in range(0, len(rows), 4):
            group = rows[k : k + 4]
            factors = [factor_ref[z] for z in group]
            products = [-factors[0]]
            for factor_z in factors[1:]:
                products.append(-factor_z * products[-1])
            after = []
            for n in range(2):
                partial = None
                for z, factor_z, product_z in zip(group, factors, products):
                    own = rhs[n, 8 * z : 8 * z + 8, :]
                    if scale_ref is not None:
                        own = own * scale_ref[z]
                    partial = own if partial is None else own - factor_z * partial
                    value = partial + product_z * before[n]
                    rhs[n, 8 * z : 8 * z + 8, :] = value
                after.append(value)
            before = after
            yield before

    def both(low_rows, high_rows, factor_ref, scale_ref, low, high):
        for low, high in zip(
            sweep(low_rows, factor_ref, scale_ref, low),
            sweep(high_rows, factor_ref, scale_ref, high),
        ):
            pass
        return low, high

    (low_re, low_im), (high_re, high_im) = both(
        range(HALF), range(DEPTH - 1, HALF - 1, -1), fe_s, inv_s, (zero, zero), (zero, zero)
    )
    bc_low, bc_high = bc_s[HALF - 1], bc_s[HALF]
    inv_det = 1.0 / (1.0 - bc_low * bc_high)
    low_re = (low_re - bc_low * high_re) * inv_det
    low_im = (low_im - bc_low * high_im) * inv_det
    high_re = high_re - bc_high * low_re
    high_im = high_im - bc_high * low_im
    rhs[0, at(HALF - 1), :] = low_re
    rhs[1, at(HALF - 1), :] = low_im
    rhs[0, at(HALF), :] = high_re
    rhs[1, at(HALF), :] = high_im

    (low_re, low_im), (high_re, high_im) = both(
        range(HALF - 2, -1, -1),
        range(HALF + 1, DEPTH),
        bc_s,
        None,
        (low_re, low_im),
        (high_re, high_im),
    )
    far_send[0, 0:8] = low_re.astype(bf16)
    far_send[0, 8:16] = low_im.astype(bf16)
    far_send[1, 0:8] = high_re.astype(bf16)
    far_send[1, 8:16] = high_im.astype(bf16)
    ex_send[0] = low_re
    ex_send[1] = low_im
    ex_send[2] = high_re
    ex_send[3] = high_im
    ex_all[pl.ds(g, 1)] = ex_send[...][None]

    for d in (4, 3, 5):
        gz_send(far_send, far_all.at[g], 6, lax.rem(g + d, GZ)).start()
    for d in (2, 6, 1, 7):
        gz_send(ex_send, ex_all.at[g], 4, lax.rem(g + d, GZ)).start()
    for c in range(RADIX):
        for n in range(2):
            yt_s[n, c] = rhs[n, pl.ds(c, DEPTH, stride=8), :]
    gz_send(sp_all.at[0 : GZ - 1], sp_all.at[0 : GZ - 1], 3, g).wait_recv()
    beta = zero
    for b in range(GZ):
        v_first, v_last, w_first, w_last = (sp_all[b, n] for n in range(4))
        inv = 1.0 / (1.0 - v_first * beta)
        gamma = v_last * beta * inv
        red[0, b] = gamma
        red[1, b] = v_last + gamma * v_first
        red[2, b] = inv
        red[3, b] = inv * v_first
        red[4, b] = inv * w_first
        beta = w_last + gamma * w_first
        red[5, b] = beta

    gz_send(ex_all.at[0:4], ex_all.at[0:4], 4, g).wait_recv()
    gz_send(far_all.at[0:3], far_all.at[0:3], 6, g).wait_recv()
    for d in (3, 4, 5):
        b = lax.rem(g + d, GZ)
        for n in range(2):
            pair = far_all[b, n].astype(f32)
            ex_all[b, 2 * n] = pair[0:8]
            ex_all[b, 2 * n + 1] = pair[8:16]

    for n in range(2):
        alpha = zero
        befores = []
        for b in range(GZ):
            befores.append(alpha)
            alpha = (
                ex_all[b, 2 + n] + red[0, b] * ex_all[b, n] + red[1, b] * alpha
            )
        first = zero
        edge[1, n, GZ - 1] = zero
        for b in range(GZ - 1, -1, -1):
            first = red[2, b] * ex_all[b, n] + red[3, b] * befores[b] + red[4, b] * first
            if b > 0:
                edge[1, n, b - 1] = first
                edge[0, n, b] = befores[b] + red[5, b - 1] * first
        edge[0, n, 0] = zero

    from_below = [edge[0, n, g] for n in range(2)]
    from_above = [edge[1, n, g] for n in range(2)]

    across = (((1,), (1,)), ((), ()))
    for c in range(0, RADIX, 2):
        for h in range(2):
            for i in range(DEPTH // 16):
                rows = slice(16 * i, 16 * (i + 1))
                v_c, w_c = vt_s[c + h, rows, :], wt_s[c + h, rows, :]
                full = [
                    yt_s[n, c + h, rows, :]
                    + v_c * from_below[n][c + h : c + h + 1, :]
                    + w_c * from_above[n][c + h : c + h + 1, :]
                    for n in range(2)
                ]
                put_split(y_s, c + h, rows, full[1], full[0])
        rows = y_s[c : c + 2].reshape(2 * DEPTH, 512)
        acc = lax.dot_general(
            weights_t[:, 0:512], rows, across, preferred_element_type=f32
        ) + lax.dot_general(
            weights_t[:, 512:768], rows[:, 0:256], across, preferred_element_type=f32
        )
        for n in range(2):
            for h in range(2):
                part_t[n, c + h] = acc[n * 128 : (n + 1) * 128, h * DEPTH : (h + 1) * DEPTH]

    def unmix(q, h):
        rows = pl.ds(pl.multiple_of(32 * q + 16 * h, 16), 16)
        turned = []
        for c in range(RADIX):
            re, im = part_t[0, c, rows, :], part_t[1, c, rows, :]
            if c > 0:
                cos, sin = tc_s[c, rows, :], ts_s[c, rows, :]
                re, im = re * cos + im * sin, im * cos - re * sin
            turned.append((re, im))
        mixed = butterfly([t[0] for t in turned], [t[1] for t in turned])
        for j, (first, second) in enumerate(mixed):
            out_v[0, 4 * j + q, 16 * h : 16 * h + 16, :] = second.astype(bf16)
            out_v[1, 4 * j + q, 16 * h : 16 * h + 16, :] = first.astype(bf16)

    def give(q, carry):
        for i in range(RADIX):
            y = lax.rem(my_y + (2, 3, 1, 0)[i // 2], 4)
            t = 8 * y + 4 * (i % 2) + q

            @pl.when(t != me)
            def _():
                row_send(out_v.at[:, t], out_ref.at[:, me], 5, t).start()

        return carry

    def turn(i):
        return lax.rem(i, 2) * 2 + 1 - i // 2

    unmix(turn(0), 0)
    unmix(turn(0), 1)

    def unmix_step(i, carry):
        unmix(turn(i), 0)
        give(turn(i - 1), carry)
        unmix(turn(i), 1)
        return carry

    lax.fori_loop(1, 4, unmix_step, 0)
    give(turn(3), 0)
    out_ref[:, pl.ds(me, 1)] = out_v[:, pl.ds(me, 1)]
    row_wait(out_ref, 5)
    for k, ref in ((1, u_v), (2, s_v), (5, out_v)):
        row_send(ref.at[:, 0 : ROW - 1], ref.at[:, 0 : ROW - 1], k, me).wait_send()
    for k, ref, n in ((3, sp_all, 7), (4, ex_all, 4), (6, far_all, 3)):
        gz_send(ref.at[0:n], ref.at[0:n], k, g).wait_send()


def on_device(velocity_x, velocity_y, velocity_z, spacing, level_index, plane_index):
    weights, twiddle = tables()
    block = (2, 32, 32, 128)
    line = (DEPTH, RADIX, 128)
    flat = (DEPTH * RADIX, 128)
    tile = (RADIX, DEPTH, 128)
    pressure = pl.pallas_call(
        kernel,
        out_shape=pltpu.VMEM(block, bf16),
        in_specs=[
            pl.BlockSpec(memory_space=pltpu.HBM),
        ]
        * 9,
        out_specs=pl.BlockSpec(memory_space=pltpu.VMEM),
        scratch_shapes=[
            pltpu.SMEM((64,), f32),
            pltpu.VMEM((8, 128), jnp.int32),
            pltpu.SMEM((32,), jnp.int32),
            pltpu.VMEM((768, 256), bf16),
            pltpu.VMEM((256, 768), bf16),
            pltpu.VMEM((16, 128), f32),
            pltpu.VMEM(block, bf16),
            pltpu.VMEM(block, bf16),
            pltpu.VMEM(block, bf16),
            pltpu.VMEM(block, bf16),
            pltpu.VMEM(block, bf16),
            pltpu.VMEM(block, bf16),
            pltpu.VMEM(block, bf16),
            pltpu.VMEM((1, 2048), f32),
            pltpu.VMEM((1, 2048), f32),
            pltpu.VMEM(block, f32),
            pltpu.VMEM((4, 8, 128), f32),
            pltpu.VMEM((3, 128, 128), f32),
            pltpu.VMEM(line, f32),
            pltpu.VMEM(line, f32),
            pltpu.VMEM(line, f32),
            pltpu.VMEM(flat, f32),
            pltpu.VMEM(flat, f32),
            pltpu.VMEM(tile, f32),
            pltpu.VMEM(tile, f32),
            pltpu.VMEM((2,) + tile, f32),
            pltpu.VMEM((2,) + flat, f32),
            pltpu.VMEM((RADIX, DEPTH, 256), f32),
            pltpu.VMEM((2,) + tile, f32),
            pltpu.VMEM(tile, f32),
            pltpu.VMEM(tile, f32),
            pltpu.VMEM((2, RADIX, 128, 128), bf16),
            pltpu.VMEM((RADIX, DEPTH, 512), bf16),
            pltpu.VMEM((RADIX, 128), f32),
            pltpu.VMEM((GZ, 4, RADIX, 128), f32),
            pltpu.VMEM((GZ, 4, RADIX, 128), f32),
            pltpu.VMEM((4, RADIX, 128), f32),
            pltpu.VMEM((4, RADIX, 128), f32),
            pltpu.VMEM((2, 2 * RADIX, 128), bf16),
            pltpu.VMEM((GZ, 2, 2 * RADIX, 128), bf16),
            pltpu.VMEM((6, GZ, RADIX, 128), f32),
            pltpu.VMEM((2, 2, GZ, RADIX, 128), f32),
            pltpu.SemaphoreType.DMA((9,)),
            pltpu.SemaphoreType.DMA((7,)),
            pltpu.SemaphoreType.DMA((7,)),
            pltpu.SemaphoreType.DMA((8,)),
            pltpu.SemaphoreType.REGULAR((5,)),
        ],
        compiler_params=pltpu.CompilerParams(
            collective_id=0, has_side_effects=True, vmem_limit_bytes=48 * 1024 * 1024
        ),
        name="poisson",
    )(
        *(
            pltpu.with_memory_space_constraint(operand, pltpu.HBM)
            for operand in (
                velocity_x,
                velocity_y,
                velocity_z,
                spacing,
                level_index.reshape(8, 128),
                plane_index,
                jnp.asarray(weights),
                jnp.asarray(weights.T),
                jnp.asarray(twiddle),
            )
        )
    )
    return pressure.astype(f32) * (1.0 / 1024.0)


def solution(mesh):
    placed = (
        P(None, None, "row", "gz"),
        P(None, None, "row", "gz"),
        P(None, None, "row", "gz"),
        P(),
        P(),
        P(),
    )
    return jax.shard_map(
        on_device, mesh=mesh, in_specs=placed, out_specs=P(None, None, "row", "gz"), check_vma=False
    )
```

```python
import math

import jax
import jax.numpy as jnp
import numpy as np
from jax import lax
from jax.experimental import pallas as pl
from jax.experimental.pallas import tpu as pltpu
from jax.sharding import PartitionSpec as P

MESH = pl.DeviceIdType.MESH
f32 = jnp.float32
bf16 = jnp.bfloat16
full_turn = 2.0 * math.pi
wave_unit = 2.0 * math.pi / 2048.0
ROW = 32
GZ = 8
DEPTH = 128
RADIX = 8
HALF = DEPTH // 2
ROOT_HALF = math.sqrt(0.5)


def tables():
    idx = np.arange(128)
    angle = 2.0 * np.pi / 128.0 * ((idx[:, None] * idx[None, :]) % 128)
    c, s = np.cos(angle), np.sin(angle)
    w = np.block([[c, -s], [s, c]]).astype(np.float32)
    hi = w.astype(jnp.bfloat16)
    lo = (w - hi.astype(np.float32)).astype(jnp.bfloat16)
    weights = np.concatenate([hi, hi, lo], axis=0)
    twist = 2.0 * np.pi / 1024.0 * (np.arange(8)[:, None] * idx[None, :])
    twiddle = np.concatenate([np.cos(twist), np.sin(twist)], axis=0).astype(np.float32)
    return weights, twiddle


def butterfly(xr, xi):
    def add(p, q):
        return (p[0] + q[0], p[1] + q[1])

    def sub(p, q):
        return (p[0] - q[0], p[1] - q[1])

    def turn(p):
        return (p[1], -p[0])

    x = list(zip(xr, xi))
    a0, a1 = add(x[0], x[4]), sub(x[0], x[4])
    a2, a3 = add(x[2], x[6]), turn(sub(x[2], x[6]))
    b0, b1 = add(x[1], x[5]), sub(x[1], x[5])
    b2, b3 = add(x[3], x[7]), turn(sub(x[3], x[7]))
    e = [add(a0, a2), add(a1, a3), sub(a0, a2), sub(a1, a3)]
    o = [add(b0, b2), add(b1, b3), sub(b0, b2), sub(b1, b3)]
    o1 = ((o[1][0] + o[1][1]) * ROOT_HALF, (o[1][1] - o[1][0]) * ROOT_HALF)
    o2 = turn(o[2])
    o3 = ((o[3][1] - o[3][0]) * ROOT_HALF, -(o[3][0] + o[3][1]) * ROOT_HALF)
    odd = [o[0], o1, o2, o3]
    return [add(e[k], odd[k]) for k in range(4)] + [sub(e[k], odd[k]) for k in range(4)]


def twisted(re, im, tw_ref, c):
    if c == 0:
        return re, im
    cos = tw_ref[c : c + 1, :]
    sin = tw_ref[8 + c : 9 + c, :]
    return re * cos + im * sin, im * cos - re * sin


def put_split(y_ref, c, rows, re, im):
    re_hi = re.astype(bf16)
    im_hi = im.astype(bf16)
    y_ref[c, rows, 0:128] = re_hi
    y_ref[c, rows, 128:256] = im_hi
    y_ref[c, rows, 256:384] = (re - re_hi.astype(f32)).astype(bf16)
    y_ref[c, rows, 384:512] = (im - im_hi.astype(f32)).astype(bf16)


FAR_FIRST = (2, 3, 1, 0)
OFFSETS = [(y, x) for y in FAR_FIRST for x in FAR_FIRST]


def hops(offset):
    return sum(min(d, 4 - d) for d in offset)


FAR_CHIPS = sorted((d for d in OFFSETS if hops(d) > 2), key=lambda d: -hops(d))
NEAR_CHIPS = sorted((d for d in OFFSETS if 0 < hops(d) <= 2), key=lambda d: -hops(d))


def kernel(
    u_hbm, v_hbm, w_hbm, spacing_hbm, level_hbm, plane_hbm, weights_hbm, weights_t_hbm, tw_hbm,
    out_ref,
    spacing_ref, level_ref, plane_ref, weights_ref, weights_t, tw_ref,
    u_v, v_v, w_v, s_v, recv_u, recv_s, out_v, halo_out, halo_in, halo_cols, band, bmat,
    inv_s, fe_s, bc_s, vs_s, ws_s, vt_s, wt_s, yt_s, rhs, part, part_t, tc_s, ts_s, q_t, y_s, kx_s,
    sp_all, ex_all, sp_send, ex_send, far_send, far_all, red, edge,
    lsem, bar_send, bar_recv, s_recv, hello,
):
    me = lax.axis_index("row")
    g = lax.axis_index("gz")
    my_y, my_x, my_core = me // 8, lax.rem(me // 2, 4), lax.rem(me, 2)
    barrier = pltpu.get_barrier_semaphore()
    partner = 2 * (me // 2) + 1 - my_core
    upper_z, lower_z = lax.rem(g + 1, GZ), lax.rem(g + GZ - 1, GZ)

    def chip(d):
        return lax.rem(my_y + d[0], 4) * 8 + lax.rem(my_x + d[1], 4) * 2

    def greet(device):
        pl.semaphore_signal(barrier, inc=1, device_id=device, device_id_type=MESH)

    for d in FAR_CHIPS:
        greet({"row": chip(d) + 1})
    for d in NEAR_CHIPS:
        greet({"row": chip(d)})
    greet({"row": 2 * (me // 2), "gz": upper_z})
    greet({"row": 2 * (me // 2), "gz": lower_z})
    greet({"row": partner})
    loads = [
        pltpu.make_async_copy(u_hbm, u_v, lsem.at[0]),
        pltpu.make_async_copy(w_hbm, w_v, lsem.at[1]),
        pltpu.make_async_copy(v_hbm, v_v, lsem.at[2]),
        pltpu.make_async_copy(level_hbm, level_ref, lsem.at[3]),
        pltpu.make_async_copy(spacing_hbm, spacing_ref, lsem.at[4]),
        pltpu.make_async_copy(plane_hbm, plane_ref, lsem.at[5]),
        pltpu.make_async_copy(tw_hbm, tw_ref, lsem.at[6]),
        pltpu.make_async_copy(weights_hbm, weights_ref, lsem.at[7]),
        pltpu.make_async_copy(weights_t_hbm, weights_t, lsem.at[8]),
    ]
    for load in loads:
        load.start()

    def row_send(src, dst, k, t):
        return pltpu.make_async_remote_copy(
            src, dst, bar_send.at[k], bar_recv.at[k], device_id={"row": t}, device_id_type=MESH
        )

    def gz_send(src, dst, k, t):
        return pltpu.make_async_remote_copy(
            src, dst, bar_send.at[k], bar_recv.at[k], device_id={"gz": t}, device_id_type=MESH
        )

    def tell_partner():
        pl.semaphore_signal(hello.at[4], inc=1, device_id={"row": partner}, device_id_type=MESH)

    def send_u(chips, core):
        for d in chips:
            t = chip(d) + core
            row_send(u_v.at[:, t], recv_u.at[:, me], 1, t).start()

    loads[0].wait()

    @pl.when(my_core == 0)
    def _():
        pl.semaphore_wait(barrier, 2 * len(NEAR_CHIPS) + 5)
        tell_partner()

    @pl.when(my_core == 1)
    def _():
        pl.semaphore_wait(hello.at[4], 1)

    send_u(NEAR_CHIPS, 0)
    send_u(NEAR_CHIPS, 1)
    row_send(u_v.at[:, partner], recv_u.at[:, me], 1, partner).start()

    loads[1].wait()

    pick = (lax.broadcasted_iota(jnp.int32, (16, DEPTH), 1) == DEPTH - 1).astype(f32).astype(bf16)
    for n in range(2):
        column = lax.dot_general(
            pick,
            w_v[n].reshape(1024, DEPTH),
            (((1,), (1,)), ((), ())),
            preferred_element_type=f32,
        )
        halo_out[:, n * 1024 : (n + 1) * 1024] = column[0:1, :]

    halo_copy = gz_send(halo_out, halo_in, 0, upper_z)

    @pl.when(g < GZ - 1)
    def _():
        halo_copy.start()

    @pl.when(g == 0)
    def _():
        halo_in[...] = jnp.zeros_like(halo_in)

    @pl.when(my_core == 1)
    def _():
        pl.semaphore_wait(barrier, 2 * len(FAR_CHIPS) + 1)
        tell_partner()

    @pl.when(my_core == 0)
    def _():
        pl.semaphore_wait(hello.at[4], 1)

    send_u(FAR_CHIPS, 0)

    def greet_z(k, z):
        pl.semaphore_signal(hello.at[k], inc=1, device_id={"gz": z}, device_id_type=MESH)

    greet_z(0, upper_z)
    greet_z(1, lower_z)
    recv_u[:, pl.ds(me, 1)] = u_v[:, pl.ds(me, 1)]

    for load in loads[2:]:
        load.wait()

    level = level_ref[...]
    width = jnp.zeros((GZ, DEPTH), f32)
    for n in range(64):
        width = jnp.where(level == n, spacing_ref[n], width)
    lane = lax.broadcasted_iota(jnp.int32, (GZ, DEPTH), 1)
    block = lax.broadcasted_iota(jnp.int32, (GZ, DEPTH), 0)
    shift_up = pltpu.roll(width, 1, 1)
    previous = jnp.where(lane == 0, pltpu.roll(shift_up, 1, 0), shift_up)
    shift_down = pltpu.roll(width, DEPTH - 1, 1)
    following = jnp.where(lane == DEPTH - 1, pltpu.roll(shift_down, GZ - 1, 0), shift_down)
    lower = 1.0 / (0.5 * (previous + width) * width)
    upper = 1.0 / (0.5 * (width + following) * width)
    lower = jnp.where((lane == 0) & (block == 0), 0.0, lower)
    upper = jnp.where((lane == DEPTH - 1) & (block == GZ - 1), 0.0, upper)
    band[0] = lower
    band[1] = upper
    band[2] = -(lower + upper)
    band[3] = 1.0 / width
    for n in range(3):
        row_n = jnp.broadcast_to(band[n, pl.ds(g, 1), :], (DEPTH, DEPTH))
        bmat[n] = row_n.T

    outer = lax.broadcasted_iota(jnp.int32, (RADIX, 128), 0)
    inner = lax.broadcasted_iota(jnp.int32, (RADIX, 128), 1)
    mode = 8 * inner + outer
    mode = jnp.where(mode >= 512, mode - 1024, mode)
    wave_x = mode.astype(f32) * (full_turn / 1024.0)
    own_wave = plane_ref[me].astype(f32) * wave_unit
    wave_sq = wave_x * wave_x + own_wave * own_wave
    kx_s[...] = wave_x

    def coef(n, z):
        return jnp.broadcast_to(bmat[n, pl.ds(z, 1), :], (RADIX, 128))

    def factor(j, carry):
        top, bottom, v_top, w_bottom = carry
        z = j
        lo, up = coef(0, z), coef(1, z)
        inv = 1.0 / ((coef(2, z) - wave_sq) - lo * top)
        fe = lo * inv
        top = up * inv
        inv_s[z] = inv
        fe_s[z] = fe
        bc_s[z] = top
        v_top = -fe * v_top
        vs_s[pl.ds(pl.multiple_of(z * 8, 8), 8), :] = v_top
        z = DEPTH - 1 - j
        lo, up = coef(0, z), coef(1, z)
        inv = 1.0 / ((coef(2, z) - wave_sq) - up * bottom)
        fe = up * inv
        bottom = lo * inv
        inv_s[z] = inv
        fe_s[z] = fe
        bc_s[z] = bottom
        w_bottom = -fe * w_bottom
        ws_s[pl.ds(pl.multiple_of(z * 8, 8), 8), :] = w_bottom
        return top, bottom, v_top, w_bottom

    zero = jnp.zeros((RADIX, 128), f32)
    one = jnp.ones((RADIX, 128), f32)
    top, bottom, v_top, w_bottom = lax.fori_loop(0, HALF, factor, (zero, zero, one, one))
    inv_det = 1.0 / (1.0 - top * bottom)

    def at(z):
        return pl.ds(pl.multiple_of(z * 8, 8), 8)

    v_lo = v_top * inv_det
    v_hi = -bottom * v_lo
    w_hi = w_bottom * inv_det
    w_lo = -top * w_hi
    vs_s[at(HALF - 1), :] = v_lo
    vs_s[at(HALF), :] = v_hi
    ws_s[at(HALF - 1), :] = w_lo
    ws_s[at(HALF), :] = w_hi

    def spread(j, carry):
        v_lo, v_hi, w_lo, w_hi = carry
        z = HALF - 1 - j
        bc = bc_s[z]
        v_lo = vs_s[at(z), :] - bc * v_lo
        w_lo = -bc * w_lo
        vs_s[at(z), :] = v_lo
        ws_s[at(z), :] = w_lo
        z = HALF + j
        bc = bc_s[z]
        v_hi = -bc * v_hi
        w_hi = ws_s[at(z), :] - bc * w_hi
        vs_s[at(z), :] = v_hi
        ws_s[at(z), :] = w_hi
        return v_lo, v_hi, w_lo, w_hi

    v_lo, v_hi, w_lo, w_hi = lax.fori_loop(1, HALF, spread, (v_lo, v_hi, w_lo, w_hi))
    sp_send[0] = v_lo
    sp_send[1] = v_hi
    sp_send[2] = w_lo
    sp_send[3] = w_hi
    sp_all[pl.ds(g, 1)] = sp_send[...][None]
    for c in range(RADIX):
        vt_s[c] = vs_s[pl.ds(c, DEPTH, stride=8), :]
        wt_s[c] = ws_s[pl.ds(c, DEPTH, stride=8), :]

    @pl.when(g > 0)
    def _():
        halo_copy.wait_recv()

    @pl.when(g < GZ - 1)
    def _():
        halo_copy.wait_send()

    first_lane = (lax.broadcasted_iota(jnp.int32, (8, DEPTH), 1) == 0).astype(f32)
    first_row = (lax.broadcasted_iota(jnp.int32, (8, DEPTH), 0) == 0).astype(f32)
    spot = (first_lane * first_row).astype(bf16)
    for n in range(2):
        wide = jnp.broadcast_to(halo_in[:, n * 1024 : (n + 1) * 1024], (8, 1024)).astype(bf16)
        halo_cols[n] = lax.dot_general(
            wide, spot, (((0,), (0,)), ((), ())), preferred_element_type=f32
        ).reshape(32, 32, DEPTH)
    pl.semaphore_wait(hello.at[0], 1)
    pl.semaphore_wait(hello.at[1], 1)
    greet_z(2, lax.rem(g + 2, GZ))
    greet_z(3, lax.rem(g + GZ - 2, GZ))
    inv_width = band[3, pl.ds(g, 1), :]
    lane32 = lax.broadcasted_iota(jnp.int32, (32, DEPTH), 1)

    def make_source(t):
        wave = plane_ref[t].astype(f32) * wave_unit
        slopes = []
        for n in range(2):
            upward = w_v[n, t].astype(f32)
            below = jnp.where(lane32 == 0, halo_cols[n, t], pltpu.roll(upward, 1, 1))
            slopes.append((upward - below) * inv_width)
        s_v[0, t] = (-wave * v_v[1, t].astype(f32) + slopes[0]).astype(bf16)
        s_v[1, t] = (wave * v_v[0, t].astype(f32) + slopes[1]).astype(bf16)

    def send_s(t, core):
        pltpu.make_async_remote_copy(
            s_v.at[:, t],
            recv_s.at[:, me],
            bar_send.at[2 + 5 * core],
            s_recv.at[me // 4],
            device_id={"row": t},
            device_id_type=MESH,
        ).start()

    columns = [lax.rem(my_x + d, 4) * 2 for d in FAR_FIRST]

    def sources_for(core, with_sends):
        def source_step(i, carry):
            base = lax.rem(my_y + lax.rem(2 + i + (i // 2) * (1 + 2 * lax.rem(i, 2)), 4), 4) * 8
            for n in range(4):
                if with_sends:
                    make_source(base + columns[n] + core)
                if n > 0:
                    send_s(base + columns[n - 1] + core, core)

            @pl.when(base + columns[3] + core != me)
            def _():
                send_s(base + columns[3] + core, core)

            return carry

        lax.fori_loop(0, 4, source_step, 0)

    def s_sent(k, count):
        row_send(s_v.at[:, 0:count], recv_s.at[:, 0:count], k, me).wait_send()

    sources_for(0, True)
    def source_ahead(i, carry):
        make_source(2 * i + 1)
        return carry

    lax.fori_loop(0, 16, source_ahead, 0)
    for core in range(2):

        @pl.when(my_core == core)
        def _():
            s_sent(2, 15 + core)

    send_u(FAR_CHIPS, 1)
    sources_for(1, False)
    recv_s[:, pl.ds(me, 1)] = s_v[:, pl.ds(me, 1)]

    pl.semaphore_wait(hello.at[2], 1)
    pl.semaphore_wait(hello.at[3], 1)

    def send_sp(d, carry):
        t = lax.rem(g + d, GZ)
        gz_send(sp_send, sp_all.at[g], 3, t).start()
        return carry

    lax.fori_loop(1, GZ, send_sp, 0)

    def forward(recv, ready, finish):
        def flip(i, carry):
            y = lax.rem(my_y + 4 - lax.rem(2 + i + (i // 2) * (1 + 2 * lax.rem(i, 2)), 4), 4)
            for n in range(2):
                ready(2 * y + n)
            for n in range(2):
                for h in range(2):
                    a = 2 * y + h
                    q_t[n, a] = recv[n, pl.ds(4 * a, 4)].reshape(128, 128).T
            return carry

        lax.fori_loop(0, 4, flip, 0)

        for half in range(2):
            for i in range(4):
                rows = slice(64 * half + 16 * i, 64 * half + 16 * (i + 1))
                xr = [q_t[0, a, rows, :].astype(f32) for a in range(RADIX)]
                xi = [q_t[1, a, rows, :].astype(f32) for a in range(RADIX)]
                for c, (re, im) in enumerate(butterfly(xr, xi)):
                    re, im = twisted(re, im, tw_ref, c)
                    put_split(y_s, c, rows, re, im)
            for c in range(0, RADIX, 4):
                rows = y_s[c : c + 4, 64 * half : 64 * (half + 1), :].reshape(256, 512)
                acc = jnp.dot(
                    rows, weights_ref[0:512, :], preferred_element_type=f32
                ) + jnp.dot(rows[:, 0:256], weights_ref[512:768, :], preferred_element_type=f32)
                for n in range(4):
                    finish(c + n, half, acc[64 * n : 64 * (n + 1)])

    def keep_along(c, half, own):
        rows = slice(64 * half, 64 * (half + 1))
        kx = kx_s[c : c + 1, :]
        part[c, rows, 0:128] = -kx * own[:, 128:256]
        part[c, rows, 128:256] = kx * own[:, 0:128]

    def keep_rhs(c, half, own):
        total = own + part[c, 64 * half : 64 * (half + 1)]
        rhs[0, pl.ds(512 * half + c, 64, stride=8), :] = total[:, 0:128]
        rhs[1, pl.ds(512 * half + c, 64, stride=8), :] = total[:, 128:256]

    def row_wait(ref, k):
        row_send(ref.at[:, 0 : ROW - 1], ref.at[:, 0 : ROW - 1], k, me).wait_recv()

    def turn_table(c, carry):
        tc_s[c] = jnp.broadcast_to(tw_ref[pl.ds(c, 1), :], (128, 128)).T
        ts_s[c] = jnp.broadcast_to(tw_ref[pl.ds(8 + c, 1), :], (128, 128)).T
        return carry

    lax.fori_loop(1, RADIX, turn_table, 0)
    row_wait(recv_u, 1)
    forward(recv_u, lambda a: None, keep_along)

    def s_ready(a):
        def wait_for(count):
            view = recv_s.at[:, 0:count]
            pltpu.make_async_remote_copy(
                view, view, bar_send.at[2], s_recv.at[a], device_id={"row": me}, device_id_type=MESH
            ).wait_recv()

        @pl.when(a == me // 4)
        def _():
            wait_for(3)

        @pl.when(a != me // 4)
        def _():
            wait_for(4)

    forward(recv_s, s_ready, keep_rhs)

    def sweep(rows, factor_ref, scale_ref, before):
        for k in range(0, len(rows), 4):
            group = rows[k : k + 4]
            factors = [factor_ref[z] for z in group]
            products = [-factors[0]]
            for factor_z in factors[1:]:
                products.append(-factor_z * products[-1])
            after = []
            for n in range(2):
                partial = None
                for z, factor_z, product_z in zip(group, factors, products):
                    own = rhs[n, 8 * z : 8 * z + 8, :]
                    if scale_ref is not None:
                        own = own * scale_ref[z]
                    partial = own if partial is None else own - factor_z * partial
                    value = partial + product_z * before[n]
                    rhs[n, 8 * z : 8 * z + 8, :] = value
                after.append(value)
            before = after
            yield before

    def both(low_rows, high_rows, factor_ref, scale_ref, low, high):
        for low, high in zip(
            sweep(low_rows, factor_ref, scale_ref, low),
            sweep(high_rows, factor_ref, scale_ref, high),
        ):
            pass
        return low, high

    (low_re, low_im), (high_re, high_im) = both(
        range(HALF), range(DEPTH - 1, HALF - 1, -1), fe_s, inv_s, (zero, zero), (zero, zero)
    )
    bc_low, bc_high = bc_s[HALF - 1], bc_s[HALF]
    inv_det = 1.0 / (1.0 - bc_low * bc_high)
    low_re = (low_re - bc_low * high_re) * inv_det
    low_im = (low_im - bc_low * high_im) * inv_det
    high_re = high_re - bc_high * low_re
    high_im = high_im - bc_high * low_im
    rhs[0, at(HALF - 1), :] = low_re
    rhs[1, at(HALF - 1), :] = low_im
    rhs[0, at(HALF), :] = high_re
    rhs[1, at(HALF), :] = high_im

    (low_re, low_im), (high_re, high_im) = both(
        range(HALF - 2, -1, -1),
        range(HALF + 1, DEPTH),
        bc_s,
        None,
        (low_re, low_im),
        (high_re, high_im),
    )
    far_send[0, 0:8] = low_re.astype(bf16)
    far_send[0, 8:16] = low_im.astype(bf16)
    far_send[1, 0:8] = high_re.astype(bf16)
    far_send[1, 8:16] = high_im.astype(bf16)
    ex_send[0] = low_re
    ex_send[1] = low_im
    ex_send[2] = high_re
    ex_send[3] = high_im
    ex_all[pl.ds(g, 1)] = ex_send[...][None]

    for d in (4, 3, 5):
        gz_send(far_send, far_all.at[g], 6, lax.rem(g + d, GZ)).start()
    for d in (2, 6, 1, 7):
        gz_send(ex_send, ex_all.at[g], 4, lax.rem(g + d, GZ)).start()
    for c in range(RADIX):
        for n in range(2):
            yt_s[n, c] = rhs[n, pl.ds(c, DEPTH, stride=8), :]
    gz_send(sp_all.at[0 : GZ - 1], sp_all.at[0 : GZ - 1], 3, g).wait_recv()
    beta = zero
    for b in range(GZ):
        v_first, v_last, w_first, w_last = (sp_all[b, n] for n in range(4))
        inv = 1.0 / (1.0 - v_first * beta)
        gamma = v_last * beta * inv
        red[0, b] = gamma
        red[1, b] = v_last + gamma * v_first
        red[2, b] = inv
        red[3, b] = inv * v_first
        red[4, b] = inv * w_first
        beta = w_last + gamma * w_first
        red[5, b] = beta

    gz_send(ex_all.at[0:4], ex_all.at[0:4], 4, g).wait_recv()
    gz_send(far_all.at[0:3], far_all.at[0:3], 6, g).wait_recv()
    for d in (3, 4, 5):
        b = lax.rem(g + d, GZ)
        for n in range(2):
            pair = far_all[b, n].astype(f32)
            ex_all[b, 2 * n] = pair[0:8]
            ex_all[b, 2 * n + 1] = pair[8:16]

    for n in range(2):
        alpha = zero
        befores = []
        for b in range(GZ):
            befores.append(alpha)
            alpha = (
                ex_all[b, 2 + n] + red[0, b] * ex_all[b, n] + red[1, b] * alpha
            )
        first = zero
        edge[1, n, GZ - 1] = zero
        for b in range(GZ - 1, -1, -1):
            first = red[2, b] * ex_all[b, n] + red[3, b] * befores[b] + red[4, b] * first
            if b > 0:
                edge[1, n, b - 1] = first
                edge[0, n, b] = befores[b] + red[5, b - 1] * first
        edge[0, n, 0] = zero

    from_below = [edge[0, n, g] for n in range(2)]
    from_above = [edge[1, n, g] for n in range(2)]

    across = (((1,), (1,)), ((), ()))
    for c in range(0, RADIX, 2):
        for h in range(2):
            for i in range(DEPTH // 16):
                rows = slice(16 * i, 16 * (i + 1))
                v_c, w_c = vt_s[c + h, rows, :], wt_s[c + h, rows, :]
                full = [
                    yt_s[n, c + h, rows, :]
                    + v_c * from_below[n][c + h : c + h + 1, :]
                    + w_c * from_above[n][c + h : c + h + 1, :]
                    for n in range(2)
                ]
                put_split(y_s, c + h, rows, full[1], full[0])
        rows = y_s[c : c + 2].reshape(2 * DEPTH, 512)
        acc = lax.dot_general(
            weights_t[:, 0:512], rows, across, preferred_element_type=f32
        ) + lax.dot_general(
            weights_t[:, 512:768], rows[:, 0:256], across, preferred_element_type=f32
        )
        for n in range(2):
            for h in range(2):
                part_t[n, c + h] = acc[n * 128 : (n + 1) * 128, h * DEPTH : (h + 1) * DEPTH]

    def unmix(q, h):
        rows = pl.ds(pl.multiple_of(32 * q + 16 * h, 16), 16)
        turned = []
        for c in range(RADIX):
            re, im = part_t[0, c, rows, :], part_t[1, c, rows, :]
            if c > 0:
                cos, sin = tc_s[c, rows, :], ts_s[c, rows, :]
                re, im = re * cos + im * sin, im * cos - re * sin
            turned.append((re, im))
        mixed = butterfly([t[0] for t in turned], [t[1] for t in turned])
        for j, (first, second) in enumerate(mixed):
            out_v[0, 4 * j + q, 16 * h : 16 * h + 16, :] = second.astype(bf16)
            out_v[1, 4 * j + q, 16 * h : 16 * h + 16, :] = first.astype(bf16)

    def give(q, carry):
        for i in range(RADIX):
            y = lax.rem(my_y + (2, 3, 1, 0)[i // 2], 4)
            t = 8 * y + 4 * (i % 2) + q

            @pl.when(t != me)
            def _():
                row_send(out_v.at[:, t], out_ref.at[:, me], 5, t).start()

        return carry

    def turn(i):
        return lax.rem(i, 2) * 2 + 1 - i // 2

    unmix(turn(0), 0)
    unmix(turn(0), 1)

    def unmix_step(i, carry):
        unmix(turn(i), 0)
        give(turn(i - 1), carry)
        unmix(turn(i), 1)
        return carry

    lax.fori_loop(1, 4, unmix_step, 0)
    give(turn(3), 0)
    out_ref[:, pl.ds(me, 1)] = out_v[:, pl.ds(me, 1)]
    row_wait(out_ref, 5)
    for core in range(2):

        @pl.when(my_core == core)
        def _():
            s_sent(7, 16 - core)

    for k, ref in ((1, u_v), (5, out_v)):
        row_send(ref.at[:, 0 : ROW - 1], ref.at[:, 0 : ROW - 1], k, me).wait_send()
    for k, ref, n in ((3, sp_all, 7), (4, ex_all, 4), (6, far_all, 3)):
        gz_send(ref.at[0:n], ref.at[0:n], k, g).wait_send()


def on_device(velocity_x, velocity_y, velocity_z, spacing, level_index, plane_index):
    weights, twiddle = tables()
    block = (2, 32, 32, 128)
    line = (DEPTH, RADIX, 128)
    flat = (DEPTH * RADIX, 128)
    tile = (RADIX, DEPTH, 128)
    pressure = pl.pallas_call(
        kernel,
        out_shape=pltpu.VMEM(block, bf16),
        in_specs=[
            pl.BlockSpec(memory_space=pltpu.HBM),
        ]
        * 9,
        out_specs=pl.BlockSpec(memory_space=pltpu.VMEM),
        scratch_shapes=[
            pltpu.SMEM((64,), f32),
            pltpu.VMEM((8, 128), jnp.int32),
            pltpu.SMEM((32,), jnp.int32),
            pltpu.VMEM((768, 256), bf16),
            pltpu.VMEM((256, 768), bf16),
            pltpu.VMEM((16, 128), f32),
            pltpu.VMEM(block, bf16),
            pltpu.VMEM(block, bf16),
            pltpu.VMEM(block, bf16),
            pltpu.VMEM(block, bf16),
            pltpu.VMEM(block, bf16),
            pltpu.VMEM(block, bf16),
            pltpu.VMEM(block, bf16),
            pltpu.VMEM((1, 2048), f32),
            pltpu.VMEM((1, 2048), f32),
            pltpu.VMEM(block, f32),
            pltpu.VMEM((4, 8, 128), f32),
            pltpu.VMEM((3, 128, 128), f32),
            pltpu.VMEM(line, f32),
            pltpu.VMEM(line, f32),
            pltpu.VMEM(line, f32),
            pltpu.VMEM(flat, f32),
            pltpu.VMEM(flat, f32),
            pltpu.VMEM(tile, f32),
            pltpu.VMEM(tile, f32),
            pltpu.VMEM((2,) + tile, f32),
            pltpu.VMEM((2,) + flat, f32),
            pltpu.VMEM((RADIX, DEPTH, 256), f32),
            pltpu.VMEM((2,) + tile, f32),
            pltpu.VMEM(tile, f32),
            pltpu.VMEM(tile, f32),
            pltpu.VMEM((2, RADIX, 128, 128), bf16),
            pltpu.VMEM((RADIX, DEPTH, 512), bf16),
            pltpu.VMEM((RADIX, 128), f32),
            pltpu.VMEM((GZ, 4, RADIX, 128), f32),
            pltpu.VMEM((GZ, 4, RADIX, 128), f32),
            pltpu.VMEM((4, RADIX, 128), f32),
            pltpu.VMEM((4, RADIX, 128), f32),
            pltpu.VMEM((2, 2 * RADIX, 128), bf16),
            pltpu.VMEM((GZ, 2, 2 * RADIX, 128), bf16),
            pltpu.VMEM((6, GZ, RADIX, 128), f32),
            pltpu.VMEM((2, 2, GZ, RADIX, 128), f32),
            pltpu.SemaphoreType.DMA((9,)),
            pltpu.SemaphoreType.DMA((8,)),
            pltpu.SemaphoreType.DMA((8,)),
            pltpu.SemaphoreType.DMA((8,)),
            pltpu.SemaphoreType.REGULAR((5,)),
        ],
        compiler_params=pltpu.CompilerParams(
            collective_id=0, has_side_effects=True, vmem_limit_bytes=48 * 1024 * 1024
        ),
        name="poisson",
    )(
        *(
            pltpu.with_memory_space_constraint(operand, pltpu.HBM)
            for operand in (
                velocity_x,
                velocity_y,
                velocity_z,
                spacing,
                level_index.reshape(8, 128),
                plane_index,
                jnp.asarray(weights),
                jnp.asarray(weights.T),
                jnp.asarray(twiddle),
            )
        )
    )
    return pressure.astype(f32) * (1.0 / 1024.0)


def solution(mesh):
    placed = (
        P(None, None, "row", "gz"),
        P(None, None, "row", "gz"),
        P(None, None, "row", "gz"),
        P(),
        P(),
        P(),
    )
    return jax.shard_map(
        on_device, mesh=mesh, in_specs=placed, out_specs=P(None, None, "row", "gz"), check_vma=False
    )
```

```python
import math

import jax
import jax.numpy as jnp
import numpy as np
from jax import lax
from jax.experimental import pallas as pl
from jax.experimental.pallas import tpu as pltpu
from jax.sharding import PartitionSpec as P

MESH = pl.DeviceIdType.MESH
f32 = jnp.float32
bf16 = jnp.bfloat16
full_turn = 2.0 * math.pi
wave_unit = 2.0 * math.pi / 2048.0
ROW = 32
GZ = 8
DEPTH = 128
RADIX = 8
HALF = DEPTH // 2
ROOT_HALF = math.sqrt(0.5)


def tables():
    idx = np.arange(128)
    angle = 2.0 * np.pi / 128.0 * ((idx[:, None] * idx[None, :]) % 128)
    c, s = np.cos(angle), np.sin(angle)
    w = np.block([[c, -s], [s, c]]).astype(np.float32)
    hi = w.astype(jnp.bfloat16)
    lo = (w - hi.astype(np.float32)).astype(jnp.bfloat16)
    weights = np.concatenate([hi, hi, lo], axis=0)
    twist = 2.0 * np.pi / 1024.0 * (np.arange(8)[:, None] * idx[None, :])
    twiddle = np.concatenate([np.cos(twist), np.sin(twist)], axis=0).astype(np.float32)
    return weights, twiddle


def butterfly(xr, xi):
    def add(p, q):
        return (p[0] + q[0], p[1] + q[1])

    def sub(p, q):
        return (p[0] - q[0], p[1] - q[1])

    def turn(p):
        return (p[1], -p[0])

    x = list(zip(xr, xi))
    a0, a1 = add(x[0], x[4]), sub(x[0], x[4])
    a2, a3 = add(x[2], x[6]), turn(sub(x[2], x[6]))
    b0, b1 = add(x[1], x[5]), sub(x[1], x[5])
    b2, b3 = add(x[3], x[7]), turn(sub(x[3], x[7]))
    e = [add(a0, a2), add(a1, a3), sub(a0, a2), sub(a1, a3)]
    o = [add(b0, b2), add(b1, b3), sub(b0, b2), sub(b1, b3)]
    o1 = ((o[1][0] + o[1][1]) * ROOT_HALF, (o[1][1] - o[1][0]) * ROOT_HALF)
    o2 = turn(o[2])
    o3 = ((o[3][1] - o[3][0]) * ROOT_HALF, -(o[3][0] + o[3][1]) * ROOT_HALF)
    odd = [o[0], o1, o2, o3]
    return [add(e[k], odd[k]) for k in range(4)] + [sub(e[k], odd[k]) for k in range(4)]


def twisted(re, im, tw_ref, c):
    if c == 0:
        return re, im
    cos = tw_ref[c : c + 1, :]
    sin = tw_ref[8 + c : 9 + c, :]
    return re * cos + im * sin, im * cos - re * sin


def put_split(y_ref, c, rows, re, im):
    re_hi = re.astype(bf16)
    im_hi = im.astype(bf16)
    y_ref[c, rows, 0:128] = re_hi
    y_ref[c, rows, 128:256] = im_hi
    y_ref[c, rows, 256:384] = (re - re_hi.astype(f32)).astype(bf16)
    y_ref[c, rows, 384:512] = (im - im_hi.astype(f32)).astype(bf16)


FAR_FIRST = (2, 3, 1, 0)
OFFSETS = [(y, x) for y in FAR_FIRST for x in FAR_FIRST]


def hops(offset):
    return sum(min(d, 4 - d) for d in offset)


FAR_CHIPS = sorted((d for d in OFFSETS if hops(d) > 2), key=lambda d: -hops(d))
NEAR_CHIPS = sorted((d for d in OFFSETS if 0 < hops(d) <= 2), key=lambda d: -hops(d))


def kernel(
    u_hbm, v_hbm, w_hbm, spacing_hbm, level_hbm, plane_hbm, weights_hbm, weights_t_hbm, tw_hbm,
    out_ref,
    spacing_ref, level_ref, plane_ref, weights_ref, weights_t, tw_ref,
    u_v, v_v, w_v, s_v, recv_u, recv_s, out_v, halo_out, halo_in, halo_cols, band, bmat,
    inv_s, fe_s, bc_s, vs_s, ws_s, vt_s, wt_s, yt_s, rhs, part, part_t, tc_s, ts_s, q_t, y_s, kx_s,
    sp_all, ex_all, sp_send, ex_send, far_send, far_all, red, edge,
    lsem, bar_send, bar_recv, s_recv, hello,
):
    me = lax.axis_index("row")
    g = lax.axis_index("gz")
    my_y, my_x, my_core = me // 8, lax.rem(me // 2, 4), lax.rem(me, 2)
    barrier = pltpu.get_barrier_semaphore()
    partner = 2 * (me // 2) + 1 - my_core
    upper_z, lower_z = lax.rem(g + 1, GZ), lax.rem(g + GZ - 1, GZ)

    def chip(d):
        return lax.rem(my_y + d[0], 4) * 8 + lax.rem(my_x + d[1], 4) * 2

    def greet(device):
        pl.semaphore_signal(barrier, inc=1, device_id=device, device_id_type=MESH)

    for d in FAR_CHIPS:
        greet({"row": chip(d) + 1})
    for d in NEAR_CHIPS:
        greet({"row": chip(d)})
    greet({"row": 2 * (me // 2), "gz": upper_z})
    greet({"row": 2 * (me // 2), "gz": lower_z})
    greet({"row": partner})
    loads = [
        pltpu.make_async_copy(u_hbm, u_v, lsem.at[0]),
        pltpu.make_async_copy(w_hbm, w_v, lsem.at[1]),
        pltpu.make_async_copy(v_hbm, v_v, lsem.at[2]),
        pltpu.make_async_copy(level_hbm, level_ref, lsem.at[3]),
        pltpu.make_async_copy(spacing_hbm, spacing_ref, lsem.at[4]),
        pltpu.make_async_copy(plane_hbm, plane_ref, lsem.at[5]),
        pltpu.make_async_copy(tw_hbm, tw_ref, lsem.at[6]),
        pltpu.make_async_copy(weights_hbm, weights_ref, lsem.at[7]),
        pltpu.make_async_copy(weights_t_hbm, weights_t, lsem.at[8]),
    ]
    for load in loads:
        load.start()

    def row_send(src, dst, k, t):
        return pltpu.make_async_remote_copy(
            src, dst, bar_send.at[k], bar_recv.at[k], device_id={"row": t}, device_id_type=MESH
        )

    def gz_send(src, dst, k, t):
        return pltpu.make_async_remote_copy(
            src, dst, bar_send.at[k], bar_recv.at[k], device_id={"gz": t}, device_id_type=MESH
        )

    def tell_partner():
        pl.semaphore_signal(hello.at[4], inc=1, device_id={"row": partner}, device_id_type=MESH)

    def send_u(chips, core):
        for d in chips:
            t = chip(d) + core
            row_send(u_v.at[:, t], recv_u.at[:, me], 1, t).start()

    loads[0].wait()

    @pl.when(my_core == 0)
    def _():
        pl.semaphore_wait(barrier, 2 * len(NEAR_CHIPS) + 5)
        tell_partner()

    @pl.when(my_core == 1)
    def _():
        pl.semaphore_wait(hello.at[4], 1)

    send_u(NEAR_CHIPS, 0)
    send_u(NEAR_CHIPS, 1)
    row_send(u_v.at[:, partner], recv_u.at[:, me], 1, partner).start()

    loads[1].wait()

    pick = (lax.broadcasted_iota(jnp.int32, (16, DEPTH), 1) == DEPTH - 1).astype(f32).astype(bf16)
    for n in range(2):
        column = lax.dot_general(
            pick,
            w_v[n].reshape(1024, DEPTH),
            (((1,), (1,)), ((), ())),
            preferred_element_type=f32,
        )
        halo_out[:, n * 1024 : (n + 1) * 1024] = column[0:1, :]

    halo_copy = gz_send(halo_out, halo_in, 0, upper_z)

    @pl.when(g < GZ - 1)
    def _():
        halo_copy.start()

    @pl.when(g == 0)
    def _():
        halo_in[...] = jnp.zeros_like(halo_in)

    @pl.when(my_core == 1)
    def _():
        pl.semaphore_wait(barrier, 2 * len(FAR_CHIPS) + 1)
        tell_partner()

    @pl.when(my_core == 0)
    def _():
        pl.semaphore_wait(hello.at[4], 1)

    send_u(FAR_CHIPS, 0)

    def greet_z(k, z):
        pl.semaphore_signal(hello.at[k], inc=1, device_id={"gz": z}, device_id_type=MESH)

    greet_z(0, upper_z)
    greet_z(1, lower_z)
    recv_u[:, pl.ds(me, 1)] = u_v[:, pl.ds(me, 1)]

    for load in loads[2:]:
        load.wait()

    level = level_ref[...]
    width = jnp.zeros((GZ, DEPTH), f32)
    for n in range(64):
        width = jnp.where(level == n, spacing_ref[n], width)
    lane = lax.broadcasted_iota(jnp.int32, (GZ, DEPTH), 1)
    block = lax.broadcasted_iota(jnp.int32, (GZ, DEPTH), 0)
    shift_up = pltpu.roll(width, 1, 1)
    previous = jnp.where(lane == 0, pltpu.roll(shift_up, 1, 0), shift_up)
    shift_down = pltpu.roll(width, DEPTH - 1, 1)
    following = jnp.where(lane == DEPTH - 1, pltpu.roll(shift_down, GZ - 1, 0), shift_down)
    lower = 1.0 / (0.5 * (previous + width) * width)
    upper = 1.0 / (0.5 * (width + following) * width)
    lower = jnp.where((lane == 0) & (block == 0), 0.0, lower)
    upper = jnp.where((lane == DEPTH - 1) & (block == GZ - 1), 0.0, upper)
    band[0] = lower
    band[1] = upper
    band[2] = -(lower + upper)
    band[3] = 1.0 / width
    for n in range(3):
        row_n = jnp.broadcast_to(band[n, pl.ds(g, 1), :], (DEPTH, DEPTH))
        bmat[n] = row_n.T

    outer = lax.broadcasted_iota(jnp.int32, (RADIX, 128), 0)
    inner = lax.broadcasted_iota(jnp.int32, (RADIX, 128), 1)
    mode = 8 * inner + outer
    mode = jnp.where(mode >= 512, mode - 1024, mode)
    wave_x = mode.astype(f32) * (full_turn / 1024.0)
    own_wave = plane_ref[me].astype(f32) * wave_unit
    wave_sq = wave_x * wave_x + own_wave * own_wave
    kx_s[...] = wave_x

    def coef(n, z):
        return jnp.broadcast_to(bmat[n, pl.ds(z, 1), :], (RADIX, 128))

    def factor(j, carry):
        top, bottom, v_top, w_bottom = carry
        z = j
        lo, up = coef(0, z), coef(1, z)
        inv = 1.0 / ((coef(2, z) - wave_sq) - lo * top)
        fe = lo * inv
        top = up * inv
        inv_s[z] = inv
        fe_s[z] = fe
        bc_s[z] = top
        v_top = -fe * v_top
        vs_s[pl.ds(pl.multiple_of(z * 8, 8), 8), :] = v_top
        z = DEPTH - 1 - j
        lo, up = coef(0, z), coef(1, z)
        inv = 1.0 / ((coef(2, z) - wave_sq) - up * bottom)
        fe = up * inv
        bottom = lo * inv
        inv_s[z] = inv
        fe_s[z] = fe
        bc_s[z] = bottom
        w_bottom = -fe * w_bottom
        ws_s[pl.ds(pl.multiple_of(z * 8, 8), 8), :] = w_bottom
        return top, bottom, v_top, w_bottom

    zero = jnp.zeros((RADIX, 128), f32)
    one = jnp.ones((RADIX, 128), f32)
    top, bottom, v_top, w_bottom = lax.fori_loop(0, HALF, factor, (zero, zero, one, one))
    inv_det = 1.0 / (1.0 - top * bottom)

    def at(z):
        return pl.ds(pl.multiple_of(z * 8, 8), 8)

    v_lo = v_top * inv_det
    v_hi = -bottom * v_lo
    w_hi = w_bottom * inv_det
    w_lo = -top * w_hi
    vs_s[at(HALF - 1), :] = v_lo
    vs_s[at(HALF), :] = v_hi
    ws_s[at(HALF - 1), :] = w_lo
    ws_s[at(HALF), :] = w_hi

    def spread(j, carry):
        v_lo, v_hi, w_lo, w_hi = carry
        z = HALF - 1 - j
        bc = bc_s[z]
        v_lo = vs_s[at(z), :] - bc * v_lo
        w_lo = -bc * w_lo
        vs_s[at(z), :] = v_lo
        ws_s[at(z), :] = w_lo
        z = HALF + j
        bc = bc_s[z]
        v_hi = -bc * v_hi
        w_hi = ws_s[at(z), :] - bc * w_hi
        vs_s[at(z), :] = v_hi
        ws_s[at(z), :] = w_hi
        return v_lo, v_hi, w_lo, w_hi

    v_lo, v_hi, w_lo, w_hi = lax.fori_loop(1, HALF, spread, (v_lo, v_hi, w_lo, w_hi))
    sp_send[0] = v_lo
    sp_send[1] = v_hi
    sp_send[2] = w_lo
    sp_send[3] = w_hi
    sp_all[pl.ds(g, 1)] = sp_send[...][None]
    for c in range(RADIX):
        vt_s[c] = vs_s[pl.ds(c, DEPTH, stride=8), :]
        wt_s[c] = ws_s[pl.ds(c, DEPTH, stride=8), :]

    @pl.when(g > 0)
    def _():
        halo_copy.wait_recv()

    @pl.when(g < GZ - 1)
    def _():
        halo_copy.wait_send()

    first_lane = (lax.broadcasted_iota(jnp.int32, (8, DEPTH), 1) == 0).astype(f32)
    first_row = (lax.broadcasted_iota(jnp.int32, (8, DEPTH), 0) == 0).astype(f32)
    spot = (first_lane * first_row).astype(bf16)
    for n in range(2):
        wide = jnp.broadcast_to(halo_in[:, n * 1024 : (n + 1) * 1024], (8, 1024)).astype(bf16)
        halo_cols[n] = lax.dot_general(
            wide, spot, (((0,), (0,)), ((), ())), preferred_element_type=f32
        ).reshape(32, 32, DEPTH)
    pl.semaphore_wait(hello.at[0], 1)
    pl.semaphore_wait(hello.at[1], 1)
    greet_z(2, lax.rem(g + 2, GZ))
    greet_z(3, lax.rem(g + GZ - 2, GZ))
    inv_width = band[3, pl.ds(g, 1), :]
    lane32 = lax.broadcasted_iota(jnp.int32, (32, DEPTH), 1)

    def make_source(t):
        wave = plane_ref[t].astype(f32) * wave_unit
        slopes = []
        for n in range(2):
            upward = w_v[n, t].astype(f32)
            below = jnp.where(lane32 == 0, halo_cols[n, t], pltpu.roll(upward, 1, 1))
            slopes.append((upward - below) * inv_width)
        s_v[0, t] = (-wave * v_v[1, t].astype(f32) + slopes[0]).astype(bf16)
        s_v[1, t] = (wave * v_v[0, t].astype(f32) + slopes[1]).astype(bf16)

    def send_s(t, core):
        pltpu.make_async_remote_copy(
            s_v.at[:, t],
            recv_s.at[:, me],
            bar_send.at[2 + 5 * core],
            s_recv.at[me // 4],
            device_id={"row": t},
            device_id_type=MESH,
        ).start()

    columns = [lax.rem(my_x + d, 4) * 2 for d in FAR_FIRST]

    def plane_row(i):
        return lax.rem(my_y + lax.rem(2 + i + (i // 2) * (1 + 2 * lax.rem(i, 2)), 4), 4) * 8

    def sources_for(core, with_sends):
        def source_step(i, carry):
            base = plane_row(i)
            for n in range(4):
                if with_sends:
                    make_source(base + columns[n] + core)
                if n > 0:
                    send_s(base + columns[n - 1] + core, core)
                else:

                    @pl.when(i > 0)
                    def _():
                        send_s(plane_row(i - 1) + columns[3] + core, core)

            return carry

        lax.fori_loop(0, 4, source_step, 0)

        @pl.when(my_core != core)
        def _():
            send_s(partner, core)

    def s_sent(k, count):
        row_send(s_v.at[:, 0:count], recv_s.at[:, 0:count], k, me).wait_send()

    sources_for(0, True)
    def source_ahead(i, carry):
        make_source(2 * i + 1)
        return carry

    lax.fori_loop(0, 16, source_ahead, 0)
    for core in range(2):

        @pl.when(my_core == core)
        def _():
            s_sent(2, 15 + core)

    send_u(FAR_CHIPS, 1)
    sources_for(1, False)
    recv_s[:, pl.ds(me, 1)] = s_v[:, pl.ds(me, 1)]

    pl.semaphore_wait(hello.at[2], 1)
    pl.semaphore_wait(hello.at[3], 1)

    def send_sp(d, carry):
        t = lax.rem(g + d, GZ)
        gz_send(sp_send, sp_all.at[g], 3, t).start()
        return carry

    lax.fori_loop(1, GZ, send_sp, 0)

    def forward(recv, ready, finish):
        def flip(i, carry):
            y = lax.rem(my_y + 4 - lax.rem(2 + i + (i // 2) * (1 + 2 * lax.rem(i, 2)), 4), 4)
            for n in range(2):
                ready(2 * y + n)
            for n in range(2):
                for h in range(2):
                    a = 2 * y + h
                    q_t[n, a] = recv[n, pl.ds(4 * a, 4)].reshape(128, 128).T
            return carry

        lax.fori_loop(0, 4, flip, 0)

        for half in range(2):
            for i in range(4):
                rows = slice(64 * half + 16 * i, 64 * half + 16 * (i + 1))
                xr = [q_t[0, a, rows, :].astype(f32) for a in range(RADIX)]
                xi = [q_t[1, a, rows, :].astype(f32) for a in range(RADIX)]
                for c, (re, im) in enumerate(butterfly(xr, xi)):
                    re, im = twisted(re, im, tw_ref, c)
                    put_split(y_s, c, rows, re, im)
            for c in range(0, RADIX, 4):
                rows = y_s[c : c + 4, 64 * half : 64 * (half + 1), :].reshape(256, 512)
                acc = jnp.dot(
                    rows, weights_ref[0:512, :], preferred_element_type=f32
                ) + jnp.dot(rows[:, 0:256], weights_ref[512:768, :], preferred_element_type=f32)
                for n in range(4):
                    finish(c + n, half, acc[64 * n : 64 * (n + 1)])

    def keep_along(c, half, own):
        rows = slice(64 * half, 64 * (half + 1))
        kx = kx_s[c : c + 1, :]
        part[c, rows, 0:128] = -kx * own[:, 128:256]
        part[c, rows, 128:256] = kx * own[:, 0:128]

    def keep_rhs(c, half, own):
        total = own + part[c, 64 * half : 64 * (half + 1)]
        rhs[0, pl.ds(512 * half + c, 64, stride=8), :] = total[:, 0:128]
        rhs[1, pl.ds(512 * half + c, 64, stride=8), :] = total[:, 128:256]

    def row_wait(ref, k):
        row_send(ref.at[:, 0 : ROW - 1], ref.at[:, 0 : ROW - 1], k, me).wait_recv()

    def turn_table(c, carry):
        tc_s[c] = jnp.broadcast_to(tw_ref[pl.ds(c, 1), :], (128, 128)).T
        ts_s[c] = jnp.broadcast_to(tw_ref[pl.ds(8 + c, 1), :], (128, 128)).T
        return carry

    lax.fori_loop(1, RADIX, turn_table, 0)
    row_wait(recv_u, 1)
    forward(recv_u, lambda a: None, keep_along)

    def s_ready(a):
        def wait_for(count):
            view = recv_s.at[:, 0:count]
            pltpu.make_async_remote_copy(
                view, view, bar_send.at[2], s_recv.at[a], device_id={"row": me}, device_id_type=MESH
            ).wait_recv()

        @pl.when(a == me // 4)
        def _():
            wait_for(3)

        @pl.when(a != me // 4)
        def _():
            wait_for(4)

    forward(recv_s, s_ready, keep_rhs)

    def sweep(rows, factor_ref, scale_ref, before):
        for k in range(0, len(rows), 4):
            group = rows[k : k + 4]
            factors = [factor_ref[z] for z in group]
            products = [-factors[0]]
            for factor_z in factors[1:]:
                products.append(-factor_z * products[-1])
            after = []
            for n in range(2):
                partial = None
                for z, factor_z, product_z in zip(group, factors, products):
                    own = rhs[n, 8 * z : 8 * z + 8, :]
                    if scale_ref is not None:
                        own = own * scale_ref[z]
                    partial = own if partial is None else own - factor_z * partial
                    value = partial + product_z * before[n]
                    rhs[n, 8 * z : 8 * z + 8, :] = value
                after.append(value)
            before = after
            yield before

    def both(low_rows, high_rows, factor_ref, scale_ref, low, high):
        for low, high in zip(
            sweep(low_rows, factor_ref, scale_ref, low),
            sweep(high_rows, factor_ref, scale_ref, high),
        ):
            pass
        return low, high

    (low_re, low_im), (high_re, high_im) = both(
        range(HALF), range(DEPTH - 1, HALF - 1, -1), fe_s, inv_s, (zero, zero), (zero, zero)
    )
    bc_low, bc_high = bc_s[HALF - 1], bc_s[HALF]
    inv_det = 1.0 / (1.0 - bc_low * bc_high)
    low_re = (low_re - bc_low * high_re) * inv_det
    low_im = (low_im - bc_low * high_im) * inv_det
    high_re = high_re - bc_high * low_re
    high_im = high_im - bc_high * low_im
    rhs[0, at(HALF - 1), :] = low_re
    rhs[1, at(HALF - 1), :] = low_im
    rhs[0, at(HALF), :] = high_re
    rhs[1, at(HALF), :] = high_im

    (low_re, low_im), (high_re, high_im) = both(
        range(HALF - 2, -1, -1),
        range(HALF + 1, DEPTH),
        bc_s,
        None,
        (low_re, low_im),
        (high_re, high_im),
    )
    far_send[0, 0:8] = low_re.astype(bf16)
    far_send[0, 8:16] = low_im.astype(bf16)
    far_send[1, 0:8] = high_re.astype(bf16)
    far_send[1, 8:16] = high_im.astype(bf16)
    ex_send[0] = low_re
    ex_send[1] = low_im
    ex_send[2] = high_re
    ex_send[3] = high_im
    ex_all[pl.ds(g, 1)] = ex_send[...][None]

    for d in (4, 3, 5):
        gz_send(far_send, far_all.at[g], 6, lax.rem(g + d, GZ)).start()
    for d in (2, 6, 1, 7):
        gz_send(ex_send, ex_all.at[g], 4, lax.rem(g + d, GZ)).start()
    for c in range(RADIX):
        for n in range(2):
            yt_s[n, c] = rhs[n, pl.ds(c, DEPTH, stride=8), :]
    gz_send(sp_all.at[0 : GZ - 1], sp_all.at[0 : GZ - 1], 3, g).wait_recv()
    beta = zero
    for b in range(GZ):
        v_first, v_last, w_first, w_last = (sp_all[b, n] for n in range(4))
        inv = 1.0 / (1.0 - v_first * beta)
        gamma = v_last * beta * inv
        red[0, b] = gamma
        red[1, b] = v_last + gamma * v_first
        red[2, b] = inv
        red[3, b] = inv * v_first
        red[4, b] = inv * w_first
        beta = w_last + gamma * w_first
        red[5, b] = beta

    gz_send(ex_all.at[0:4], ex_all.at[0:4], 4, g).wait_recv()
    gz_send(far_all.at[0:3], far_all.at[0:3], 6, g).wait_recv()
    for d in (3, 4, 5):
        b = lax.rem(g + d, GZ)
        for n in range(2):
            pair = far_all[b, n].astype(f32)
            ex_all[b, 2 * n] = pair[0:8]
            ex_all[b, 2 * n + 1] = pair[8:16]

    for n in range(2):
        alpha = zero
        befores = []
        for b in range(GZ):
            befores.append(alpha)
            alpha = (
                ex_all[b, 2 + n] + red[0, b] * ex_all[b, n] + red[1, b] * alpha
            )
        first = zero
        edge[1, n, GZ - 1] = zero
        for b in range(GZ - 1, -1, -1):
            first = red[2, b] * ex_all[b, n] + red[3, b] * befores[b] + red[4, b] * first
            if b > 0:
                edge[1, n, b - 1] = first
                edge[0, n, b] = befores[b] + red[5, b - 1] * first
        edge[0, n, 0] = zero

    from_below = [edge[0, n, g] for n in range(2)]
    from_above = [edge[1, n, g] for n in range(2)]

    across = (((1,), (1,)), ((), ()))
    for c in range(0, RADIX, 2):
        for h in range(2):
            for i in range(DEPTH // 16):
                rows = slice(16 * i, 16 * (i + 1))
                v_c, w_c = vt_s[c + h, rows, :], wt_s[c + h, rows, :]
                full = [
                    yt_s[n, c + h, rows, :]
                    + v_c * from_below[n][c + h : c + h + 1, :]
                    + w_c * from_above[n][c + h : c + h + 1, :]
                    for n in range(2)
                ]
                put_split(y_s, c + h, rows, full[1], full[0])
        rows = y_s[c : c + 2].reshape(2 * DEPTH, 512)
        acc = lax.dot_general(
            weights_t[:, 0:512], rows, across, preferred_element_type=f32
        ) + lax.dot_general(
            weights_t[:, 512:768], rows[:, 0:256], across, preferred_element_type=f32
        )
        for n in range(2):
            for h in range(2):
                part_t[n, c + h] = acc[n * 128 : (n + 1) * 128, h * DEPTH : (h + 1) * DEPTH]

    def unmix(q, h):
        rows = pl.ds(pl.multiple_of(32 * q + 16 * h, 16), 16)
        turned = []
        for c in range(RADIX):
            re, im = part_t[0, c, rows, :], part_t[1, c, rows, :]
            if c > 0:
                cos, sin = tc_s[c, rows, :], ts_s[c, rows, :]
                re, im = re * cos + im * sin, im * cos - re * sin
            turned.append((re, im))
        mixed = butterfly([t[0] for t in turned], [t[1] for t in turned])
        for j, (first, second) in enumerate(mixed):
            out_v[0, 4 * j + q, 16 * h : 16 * h + 16, :] = second.astype(bf16)
            out_v[1, 4 * j + q, 16 * h : 16 * h + 16, :] = first.astype(bf16)

    def give(q, carry):
        for i in range(RADIX):
            y = lax.rem(my_y + (2, 3, 1, 0)[i // 2], 4)
            t = 8 * y + 4 * (i % 2) + q

            @pl.when(t != me)
            def _():
                row_send(out_v.at[:, t], out_ref.at[:, me], 5, t).start()

        return carry

    def turn(i):
        return lax.rem(i, 2) * 2 + 1 - i // 2

    unmix(turn(0), 0)
    unmix(turn(0), 1)

    def unmix_step(i, carry):
        unmix(turn(i), 0)
        give(turn(i - 1), carry)
        unmix(turn(i), 1)
        return carry

    lax.fori_loop(1, 4, unmix_step, 0)
    give(turn(3), 0)
    out_ref[:, pl.ds(me, 1)] = out_v[:, pl.ds(me, 1)]
    row_wait(out_ref, 5)
    for core in range(2):

        @pl.when(my_core == core)
        def _():
            s_sent(7, 16 - core)

    for k, ref in ((1, u_v), (5, out_v)):
        row_send(ref.at[:, 0 : ROW - 1], ref.at[:, 0 : ROW - 1], k, me).wait_send()
    for k, ref, n in ((3, sp_all, 7), (4, ex_all, 4), (6, far_all, 3)):
        gz_send(ref.at[0:n], ref.at[0:n], k, g).wait_send()


def on_device(velocity_x, velocity_y, velocity_z, spacing, level_index, plane_index):
    weights, twiddle = tables()
    block = (2, 32, 32, 128)
    line = (DEPTH, RADIX, 128)
    flat = (DEPTH * RADIX, 128)
    tile = (RADIX, DEPTH, 128)
    pressure = pl.pallas_call(
        kernel,
        out_shape=pltpu.VMEM(block, bf16),
        in_specs=[
            pl.BlockSpec(memory_space=pltpu.HBM),
        ]
        * 9,
        out_specs=pl.BlockSpec(memory_space=pltpu.VMEM),
        scratch_shapes=[
            pltpu.SMEM((64,), f32),
            pltpu.VMEM((8, 128), jnp.int32),
            pltpu.SMEM((32,), jnp.int32),
            pltpu.VMEM((768, 256), bf16),
            pltpu.VMEM((256, 768), bf16),
            pltpu.VMEM((16, 128), f32),
            pltpu.VMEM(block, bf16),
            pltpu.VMEM(block, bf16),
            pltpu.VMEM(block, bf16),
            pltpu.VMEM(block, bf16),
            pltpu.VMEM(block, bf16),
            pltpu.VMEM(block, bf16),
            pltpu.VMEM(block, bf16),
            pltpu.VMEM((1, 2048), f32),
            pltpu.VMEM((1, 2048), f32),
            pltpu.VMEM(block, f32),
            pltpu.VMEM((4, 8, 128), f32),
            pltpu.VMEM((3, 128, 128), f32),
            pltpu.VMEM(line, f32),
            pltpu.VMEM(line, f32),
            pltpu.VMEM(line, f32),
            pltpu.VMEM(flat, f32),
            pltpu.VMEM(flat, f32),
            pltpu.VMEM(tile, f32),
            pltpu.VMEM(tile, f32),
            pltpu.VMEM((2,) + tile, f32),
            pltpu.VMEM((2,) + flat, f32),
            pltpu.VMEM((RADIX, DEPTH, 256), f32),
            pltpu.VMEM((2,) + tile, f32),
            pltpu.VMEM(tile, f32),
            pltpu.VMEM(tile, f32),
            pltpu.VMEM((2, RADIX, 128, 128), bf16),
            pltpu.VMEM((RADIX, DEPTH, 512), bf16),
            pltpu.VMEM((RADIX, 128), f32),
            pltpu.VMEM((GZ, 4, RADIX, 128), f32),
            pltpu.VMEM((GZ, 4, RADIX, 128), f32),
            pltpu.VMEM((4, RADIX, 128), f32),
            pltpu.VMEM((4, RADIX, 128), f32),
            pltpu.VMEM((2, 2 * RADIX, 128), bf16),
            pltpu.VMEM((GZ, 2, 2 * RADIX, 128), bf16),
            pltpu.VMEM((6, GZ, RADIX, 128), f32),
            pltpu.VMEM((2, 2, GZ, RADIX, 128), f32),
            pltpu.SemaphoreType.DMA((9,)),
            pltpu.SemaphoreType.DMA((8,)),
            pltpu.SemaphoreType.DMA((8,)),
            pltpu.SemaphoreType.DMA((8,)),
            pltpu.SemaphoreType.REGULAR((5,)),
        ],
        compiler_params=pltpu.CompilerParams(
            collective_id=0, has_side_effects=True, vmem_limit_bytes=48 * 1024 * 1024
        ),
        name="poisson",
    )(
        *(
            pltpu.with_memory_space_constraint(operand, pltpu.HBM)
            for operand in (
                velocity_x,
                velocity_y,
                velocity_z,
                spacing,
                level_index.reshape(8, 128),
                plane_index,
                jnp.asarray(weights),
                jnp.asarray(weights.T),
                jnp.asarray(twiddle),
            )
        )
    )
    return pressure.astype(f32) * (1.0 / 1024.0)


def solution(mesh):
    placed = (
        P(None, None, "row", "gz"),
        P(None, None, "row", "gz"),
        P(None, None, "row", "gz"),
        P(),
        P(),
        P(),
    )
    return jax.shard_map(
        on_device, mesh=mesh, in_specs=placed, out_specs=P(None, None, "row", "gz"), check_vma=False
    )
```
